32 devices in a mesh: tm: 8 (over z, y), space: 4 (over x, core).
Axes of the slice: x: 2, y: 2, z: 4, core: 2. Of those that a mesh axis runs over, the one named last changes fastest.
Arguments:
- amplitude: float32 [80, 96, 512], P('tm', 'space'), may hold values from 0.3 to 3
- phase: float32 [80, 96, 512], P('tm', 'space'), may hold values from -3.140625 to 3.140625
- validity: int32 [96, 512], P('space'), may hold values 0 or 1
- iterations: int32 [8], P('tm'), may hold values from 10 to 20, as said below
- reference_date: int32 [8], P('tm'), may hold values from 0 to 9
Outputs:
- linked: float32 [2, 80, 96, 512], P(None, 'tm', 'space')
The draws below stay inside these ranges and needn't reach their ends.
Inputs may be any that keep to these rules, and one draw needn't show every extreme that they name: Every ministack takes between 10 and 20 iterations, and some ministack takes exactly 20.
All inputs are finite; a program needn't handle non-finite values. No bound on the sum of `validity` on one device may be relied on, other than what follows from the above.
Results may differ from the reference program's by a relative error of at most 0.0003.
Values sent between devices are 32-bit elements; how exact they have to be, the bound alone decides.
No kernel may reach another device: no remote copies, remote signals or barrier semaphores. Data moves between devices by JAX's collectives and lax.ppermute only.
A program may use at most 64 MiB of HBM per device.

```python
import math
import jax
import jax.numpy as jnp
from jax import lax

DATES_MS = 10
WIN_ROWS = 11
WIN_COLS = 5
ITERS = 20
COLS = 512
MINISTACKS = 8
DATES = 80
ROWS = 96


def draw_iterations(key, part):
    first_key, second_key = jax.random.split(jax.random.fold_in(key, 7))
    counts = jax.random.randint(first_key, (MINISTACKS,), ITERS // 2, ITERS + 1)
    chosen = jax.random.randint(second_key, (), 0, MINISTACKS)
    return jnp.where(jnp.arange(MINISTACKS) == chosen, ITERS, counts).astype(jnp.int32)


def plant(values, rng, least, high):
    dims = values.shape
    spot = [jax.random.randint(jax.random.fold_in(rng, axis), (), 0, dims[axis]) for axis in range(len(dims))]
    values = values.at[tuple(spot)].set(least)
    longest = dims.index(max(dims))
    spot[longest] = (spot[longest] + 1) % dims[longest]
    return values.at[tuple(spot)].set(high)


def levels(own_key, extent, cuts, low, largest):
    level = 1.0
    for axis_at, blocks in cuts:
        steps = jax.random.uniform(jax.random.fold_in(jax.random.fold_in(own_key, 6), axis_at), (blocks,), jnp.float32, low / len(cuts), largest / len(cuts))
        level = level * jnp.repeat(jnp.exp(steps), extent[axis_at] // blocks).reshape((-1,) + (1,) * (len(extent) - 1 - axis_at))
    return level


def setup_inputs(seed: int = 0) -> dict:
    seeds = jax.random.split(jax.random.key(seed), 6)
    return {
        "amplitude": jnp.clip(jnp.exp(math.log(3.0) - 2.3025851 * jax.random.uniform(seeds[0], (DATES, ROWS, COLS), jnp.float32) ** levels(seeds[0], (DATES, ROWS, COLS), ((0, 8), (1, 4)), -0.2, 0.2)), 0.3, 3.0),
        "phase": jnp.clip(jax.random.uniform(seeds[1], (DATES, ROWS, COLS), jnp.float32, -3.140625, 3.140625), -3.140625, 3.140625),
        "validity": plant((jax.random.randint(seeds[2], (ROWS, COLS), 0, 8) < 7).astype(jnp.int32), jax.random.fold_in(seeds[2], 1), 0, 1),
        "iterations": draw_iterations(jax.random.fold_in(seeds[5], 71), 0),
        "reference_date": plant(jax.random.randint(seeds[4], (MINISTACKS,), 0, DATES_MS), jax.random.fold_in(seeds[4], 1), 0, DATES_MS - 1).astype(jnp.int32),
    }


masked_weight = 0.125
link_floor = 0.03

def box_valid(values):
    out_rows = values.shape[-2] - WIN_ROWS + 1
    row_sums = values[..., 0:out_rows, :]
    for offset in range(1, WIN_ROWS):
        row_sums = row_sums + values[..., offset:offset + out_rows, :]
    out_cols = values.shape[-1] - WIN_COLS + 1
    summed = row_sums[..., 0:out_cols]
    for offset in range(1, WIN_COLS):
        summed = summed + row_sums[..., offset:offset + out_cols]
    return summed

def estimate(window_block, sweep_limit):
    date_count = (window_block.shape[0] - 1) // 2
    amplitudes = window_block[:date_count]
    angles = window_block[date_count:2 * date_count]
    weights = window_block[2 * date_count]
    real_part = amplitudes * jnp.cos(angles)
    imag_part = amplitudes * jnp.sin(angles)
    cross_real = weights * (real_part[:, None] * real_part[None] + imag_part[:, None] * imag_part[None])
    cross_imag = weights * (imag_part[:, None] * real_part[None] - real_part[:, None] * imag_part[None])
    power_real = box_valid(cross_real)
    power_imag = box_valid(cross_imag)
    own_power = box_valid(weights * amplitudes * amplitudes)
    inverse = 1.0 / jnp.sqrt(own_power)
    coher_real = power_real * inverse[:, None] * inverse[None]
    coher_imag = power_imag * inverse[:, None] * inverse[None]
    start_real = jnp.full(own_power.shape, 1.0 / math.sqrt(date_count), jnp.float32)
    start_imag = jnp.zeros(own_power.shape, jnp.float32)

    def power_step(turn_no, vectors):
        old_real, old_imag = vectors
        new_real = lax.optimization_barrier(jnp.sum(coher_real * old_real[None] - coher_imag * old_imag[None], axis=1)) + old_real
        new_imag = lax.optimization_barrier(jnp.sum(coher_real * old_imag[None] + coher_imag * old_real[None], axis=1)) + old_imag
        length = jnp.sqrt(lax.optimization_barrier(jnp.sum(new_real * new_real + new_imag * new_imag, axis=0)))
        active = turn_no < sweep_limit
        return (jnp.where(active, new_real / length, old_real), jnp.where(active, new_imag / length, old_imag))
    vec_real, vec_imag = lax.fori_loop(0, ITERS, power_step, (start_real, start_imag))
    half_rows = WIN_ROWS // 2
    half_cols = WIN_COLS // 2
    inner_real = real_part[:, half_rows:real_part.shape[1] - half_rows, half_cols:real_part.shape[2] - half_cols]
    inner_imag = imag_part[:, half_rows:imag_part.shape[1] - half_rows, half_cols:imag_part.shape[2] - half_cols]
    comp_real = lax.optimization_barrier(jnp.sum(vec_real * inner_real + vec_imag * inner_imag, axis=0))
    comp_imag = lax.optimization_barrier(jnp.sum(vec_real * inner_imag - vec_imag * inner_real, axis=0))
    return (vec_real, vec_imag, comp_real, comp_imag)

def link_phases(stacked, sweep_limit):
    columns = stacked.shape[2]
    half_cols = WIN_COLS // 2
    padded = jnp.pad(stacked, ((0, 0), (0, 0), (half_cols, half_cols)))
    block_cols = min(128, columns)
    blocks = columns // block_cols

    def one_block(block_no):
        window = lax.dynamic_slice_in_dim(padded, block_no * block_cols, block_cols + 2 * half_cols, 2)
        return estimate(window, sweep_limit)
    results = lax.map(one_block, jnp.arange(blocks, dtype=jnp.int32))

    def merge_cols(pieces):
        placed = jnp.moveaxis(pieces, 0, -2)
        return placed.reshape(placed.shape[:-2] + (columns,))
    return tuple((merge_cols(result) for result in results))

def refer_dates(vec_real, vec_imag, chosen):
    date_count = vec_real.shape[0]
    picked = (jnp.arange(date_count, dtype=jnp.int32) == chosen).astype(jnp.float32)[:, None, None]
    ref_real = lax.optimization_barrier(jnp.sum(vec_real * picked, axis=0))
    ref_imag = lax.optimization_barrier(jnp.sum(vec_imag * picked, axis=0))
    linked_real = date_count * (vec_real * ref_real + vec_imag * ref_imag)
    linked_imag = date_count * (vec_imag * ref_real - vec_real * ref_imag)
    return (linked_real, linked_imag)

def pad_columns(values):
    half_cols = WIN_COLS // 2
    return jnp.pad(values, [(0, 0)] * (values.ndim - 1) + [(half_cols, half_cols)])

def link_offsets(comp_real, comp_imag, next_real, next_imag, weights):
    cross_real = box_valid(pad_columns(weights * (comp_real * next_real + comp_imag * next_imag)))
    cross_imag = box_valid(pad_columns(weights * (comp_imag * next_real - comp_real * next_imag)))
    own_power = box_valid(pad_columns(weights * (comp_real * comp_real + comp_imag * comp_imag)))
    next_power = box_valid(pad_columns(weights * (next_real * next_real + next_imag * next_imag)))
    denominator = jnp.sqrt((own_power + 1.0) * (next_power + 1.0))
    off_real = cross_real / denominator
    off_imag = cross_imag / denominator
    magnitude = jnp.sqrt(off_real * off_real + off_imag * off_imag)
    bounded = jnp.maximum(magnitude, link_floor)
    return (off_real / bounded, off_imag / bounded)

def reference(amplitude, phase, validity, iterations, reference_date):
    date_count = DATES_MS
    half_rows = WIN_ROWS // 2
    row_count = amplitude.shape[1]
    columns = amplitude.shape[2]
    weights = jnp.where(validity == 1, 1.0, masked_weight).astype(jnp.float32)
    amp_stacks = amplitude.reshape(MINISTACKS, date_count, row_count, columns)
    phase_stacks = phase.reshape(MINISTACKS, date_count, row_count, columns)

    def one_stack(inputs):
        amp_block, phase_block, sweep_limit, chosen = inputs
        stacked = jnp.concatenate([amp_block, phase_block, weights[None]], axis=0)
        stacked = jnp.pad(stacked, ((0, 0), (half_rows, half_rows), (0, 0)))
        vec_real, vec_imag, comp_real, comp_imag = link_phases(stacked, sweep_limit)
        linked_real, linked_imag = refer_dates(vec_real, vec_imag, chosen)
        return (linked_real, linked_imag, comp_real, comp_imag)
    linked_real, linked_imag, comp_real, comp_imag = lax.map(one_stack, (amp_stacks, phase_stacks, iterations, reference_date))
    next_real = jnp.concatenate([comp_real[1:], jnp.zeros_like(comp_real[:1])], axis=0)
    next_imag = jnp.concatenate([comp_imag[1:], jnp.zeros_like(comp_imag[:1])], axis=0)

    def pad_rows(values):
        return jnp.pad(values, [(0, 0)] * (values.ndim - 2) + [(half_rows, half_rows), (0, 0)])
    unit_real, unit_imag = link_offsets(pad_rows(comp_real), pad_rows(comp_imag), pad_rows(next_real), pad_rows(next_imag), pad_rows(weights))

    def chain_step(vectors, link):
        datum_real, datum_imag = vectors
        link_real, link_imag = link
        following = (datum_real * link_real - datum_imag * link_imag, datum_real * link_imag + datum_imag * link_real)
        return (following, vectors)
    start = (jnp.ones((row_count, columns), jnp.float32), jnp.zeros((row_count, columns), jnp.float32))
    final_state, datums = lax.scan(chain_step, start, (unit_real, unit_imag))
    datum_real = datums[0][:, None]
    datum_imag = datums[1][:, None]
    out_real = linked_real * datum_real - linked_imag * datum_imag
    out_imag = linked_real * datum_imag + linked_imag * datum_real
    return jnp.stack([out_real, out_imag]).reshape(2, MINISTACKS * date_count, row_count, columns)
```

```python
import jax
import jax.numpy as jnp
from jax import lax
from jax.experimental import pallas as pl
from jax.experimental.pallas import tpu as pltpu
from jax.sharding import PartitionSpec as P

WIN_ROWS = 11
WIN_COLS = 5
ITERS = 20
HALF_ROWS = WIN_ROWS // 2

MASKED_WEIGHT = 0.125
LINK_FLOOR = 0.03

LANES = 128
SUB = 8
VMEM_LIMIT = 40 * 1024 * 1024


def vmem():
    return pl.BlockSpec(memory_space=pltpu.VMEM)


def smem():
    return pl.BlockSpec(memory_space=pltpu.SMEM)


def sublane():
    return lax.broadcasted_iota(jnp.int32, (SUB, LANES), 0)


def lane():
    return lax.broadcasted_iota(jnp.int32, (SUB, LANES), 1)


def flip(x):
    return pltpu.roll(x, SUB // 2, 0)


def upper():
    return sublane() < SUB // 2


def bases(k, rows, tiles):
    def base(row):
        return (row // SUB) * SUB * tiles + row % SUB

    return base(k), base(rows - 1 - k)


def load_pair(ref, lead, k, rows, tiles, top):
    first, second = bases(k, rows, tiles)
    a = ref[lead + (pl.ds(first, SUB, stride=SUB), slice(None))]
    b = ref[lead + (pl.ds(second - SUB * tiles, SUB, stride=SUB), slice(None))]
    return jnp.where(top, a, b)


def sin_cos(x):
    turns = jnp.round(x * (2.0 / jnp.pi))
    r = (x - turns * 1.5707855224609375) - turns * 1.0804334124e-05
    s = r * r
    sine = r + r * s * (-1.6666654611e-1 + s * (8.3321608736e-3 + s * -1.9515295891e-4))
    cosine = 1.0 - 0.5 * s + s * s * (
        4.166664568298827e-2 + s * (-1.388731625493765e-3 + s * 2.443315711809948e-5)
    )
    size = jnp.abs(turns)
    odd = size == 1.0
    base_s = jnp.where(odd, cosine, sine)
    base_c = jnp.where(odd, sine, cosine)
    sin_x = jnp.where((turns == -1.0) | (size == 2.0), -base_s, base_s)
    cos_x = jnp.where((turns == 1.0) | (size == 2.0), -base_c, base_c)
    return sin_x, cos_x


def images_kernel(rows, tiles, par_ref, amp_ref, phase_ref, valid_ref, z_ref, x_ref, y_ref):
    half = rows // 2
    top = upper()
    odd = par_ref[0] == 1
    roots = []
    for k in range(half):
        valid = load_pair(valid_ref, (), k, rows, tiles, top)
        roots.append(jnp.where(valid == 1, 1.0, MASKED_WEIGHT**0.5).astype(jnp.float32))

    def one_date(t, carry):
        for k in range(half):
            amp = load_pair(amp_ref, (t,), k, rows, tiles, top) * roots[k]
            sin_x, cos_x = sin_cos(load_pair(phase_ref, (t,), k, rows, tiles, top))
            re, im = amp * cos_x, amp * sin_x
            z_ref[0, t, k] = re
            z_ref[1, t, k] = im
            if k >= half - HALF_ROWS:
                z_ref[0, t, 2 * half - 1 - k] = flip(re)
                z_ref[1, t, 2 * half - 1 - k] = flip(im)
            if k < HALF_ROWS:
                first = jnp.where(top, re, flip(im))
                second = jnp.where(top, flip(re), im)
                x_ref[t, k] = jnp.where(odd, first, second)
                y_ref[t, k] = jnp.where(odd, second, first)
        return carry

    lax.fori_loop(0, z_ref.shape[1], one_date, 0)


def unpack(first, second, top):
    return jnp.where(top, first, flip(second)), jnp.where(top, flip(first), second)


def box_sum(field, lanes, edges):
    count = len(field) - WIN_ROWS + 1
    tail = [None] * WIN_ROWS
    run = field[WIN_ROWS - 1]
    tail[WIN_ROWS - 1] = run
    for k in range(WIN_ROWS - 2, -1, -1):
        run = run + field[k]
        tail[k] = run
    sums = [tail[0]]
    run = None
    for k in range(1, count):
        new = field[WIN_ROWS - 1 + k]
        run = new if run is None else run + new
        sums.append(run if k == WIN_ROWS else tail[k] + run)
    last_two, last_one, first_one, first_two = lanes
    keep_before, keep_after = edges
    out = []
    for x in sums:
        before = jnp.where(keep_before, pltpu.roll(x, 1, 0), 0.0)
        after = jnp.where(keep_after, pltpu.roll(x, SUB - 1, 0), 0.0)
        near = pltpu.roll(jnp.where(last_one, before, x), 1, 1) + pltpu.roll(
            jnp.where(first_one, after, x), LANES - 1, 1
        )
        far = pltpu.roll(jnp.where(last_two, before, x), 2, 1) + pltpu.roll(
            jnp.where(first_two, after, x), LANES - 2, 1
        )
        out.append(x + near + far)
    return out


def masks(tiles):
    at = lane()
    lanes = (at >= LANES - 2, at >= LANES - 1, at < 1, at < 2)
    column = sublane() % tiles
    return lanes, (column != 0, column != tiles - 1)


def add_to(total, sign, value):
    if total is None:
        return value if sign > 0 else -value
    return total + value if sign > 0 else total - value


def phases_kernel(
    tiles, par_ref, iter_ref, chosen_ref, z_ref, x_ref, y_ref,
    link_ref, comp_ref, pack_x_ref, pack_y_ref,
    halo, inv, nr, ni, more, sq, vec,
):
    dates = z_ref.shape[1]
    half = comp_ref.shape[1]
    top = upper()
    odd_device = par_ref[0] == 1
    lanes, edges = masks(tiles)
    pairs = [(i, j) for i in range(dates) for j in range(i + 1, dates)]
    index = {pair: e for e, pair in enumerate(pairs)}
    count = len(pairs)
    ext = half + 2 * HALF_ROWS

    def fill(t, carry):
        for k in range(HALF_ROWS):
            a, b = x_ref[t, k], y_ref[t, k]
            first = jnp.where(odd_device, a, b)
            second = jnp.where(odd_device, b, a)
            re, im = unpack(first, second, top)
            halo[0, t, HALF_ROWS - 1 - k] = re
            halo[1, t, HALF_ROWS - 1 - k] = im
        return carry

    lax.fori_loop(0, dates, fill, 0)

    def image(part, t):
        return [halo[part, t, k] for k in range(HALF_ROWS)] + [
            z_ref[part, t, k] for k in range(ext - HALF_ROWS)
        ]

    def own_power(t, carry):
        re, im = image(0, t), image(1, t)
        power = box_sum([a * a + b * b for a, b in zip(re, im)], lanes, edges)
        for k in range(half):
            inv[t, k] = lax.rsqrt(power[k]) * 0.5
        return carry

    lax.fori_loop(0, dates, own_power, 0)

    starts = {}
    for d in range(1, dates):
        def one_pair(i, carry, d=d):
            j = i + d
            ar, ai, br, bi = image(0, i), image(1, i), image(0, j), image(1, j)
            re = box_sum([ar[k] * br[k] + ai[k] * bi[k] for k in range(ext)], lanes, edges)
            im = box_sum([ai[k] * br[k] - ar[k] * bi[k] for k in range(ext)], lanes, edges)
            at = i * (2 * dates - i - 1) // 2 + (j - i - 1)
            for k in range(half):
                scale = inv[i, k] * inv[j, k]
                nr[at, k] = re[k] * scale
                ni[at, k] = im[k] * scale
            return carry

        lax.fori_loop(0, dates - d, one_pair, 0)

    turns = jnp.minimum(iter_ref[0], ITERS)
    odd_turns = turns % 2 == 1
    steps = jnp.where(odd_turns, turns // 2, turns // 2 - 1)
    groups = []
    at = 0
    for size in (3, 3, 4) if dates == 10 else (dates,):
        groups.append(tuple(range(at, at + size)))
        at += size

    def one_vector(k, carry):
        for e in range(count):
            re, im = nr[e, k], ni[e, k]
            more[e] = re + im
            more[count + e] = im - re

        def left(i, t):
            if i < t:
                e = index[i, t]
                return (nr[e, k], 1), (more[e], 1), (more[count + e], 1)
            e = index[t, i]
            return (nr[e, k], 1), (more[count + e], -1), (more[e], -1)

        def right(t, j):
            if t < j:
                e = index[t, j]
                return (nr[e, k], 1), (ni[e, k], 1), (more[e], 1)
            e = index[j, t]
            return (nr[e, k], 1), (ni[e, k], -1), (more[count + e], -1)

        def square(out):
            sums = {pair: [None, None, None] for pair in out}
            rows_in = sorted({i for i, _ in out})
            cols_in = sorted({j for _, j in out})
            for t in range(dates):
                lefts = {i: left(i, t) for i in rows_in if i != t}
                rights = {j: right(t, j) for j in cols_in if j != t}
                for i, j in out:
                    if t in (i, j):
                        continue
                    (ar, _), (ap, sap), (aq, saq) = lefts[i]
                    (br, _), (bi, sbi), (bs, sbs) = rights[j]
                    s = sums[i, j]
                    s[0] = add_to(s[0], sbs, ar * bs)
                    s[1] = add_to(s[1], saq, aq * br)
                    s[2] = add_to(s[2], sap * sbi, ap * bi)
            for i, j in out:
                e = index[i, j]
                s = sums[i, j]
                re = s[0] - s[2] + nr[e, k]
                im = s[0] + s[1] + ni[e, k]
                sq[e] = re
                sq[count + e] = re + im
                sq[2 * count + e] = im - re

        for a in range(len(groups)):
            square([(i, j) for i in groups[a] for j in groups[a] if i < j])
            for b in range(a + 1, len(groups)):
                square([(i, j) for i in groups[a] for j in groups[b]])
        size = [None] * dates
        for e, (i, j) in enumerate(pairs):
            re, im = nr[e, k], ni[e, k]
            value = re * re + im * im
            size[i] = add_to(size[i], 1, value)
            size[j] = add_to(size[j], 1, value)
        for i in range(dates):
            sq[3 * count + i] = size[i] + 0.25

        def row_sums(re_of, im_of, own):
            sr, si = [own(i) for i in range(dates)], [None] * dates
            for e, (i, j) in enumerate(pairs):
                re, im = re_of(e), im_of(e)
                sr[i] = sr[i] + re
                sr[j] = sr[j] + re
                si[i] = add_to(si[i], 1, im)
                si[j] = add_to(si[j], -1, im)
            for i in range(dates):
                vec[i] = sr[i]
                vec[dates + i] = si[i]

        @pl.when(odd_turns)
        def _():
            row_sums(lambda e: nr[e, k], lambda e: ni[e, k],
                     lambda i: jnp.full((SUB, LANES), 0.5, jnp.float32))

        @pl.when(jnp.logical_not(odd_turns))
        def _():
            row_sums(lambda e: sq[e], lambda e: sq[count + e] - sq[e],
                     lambda i: sq[3 * count + i])

        def step(_, vectors):
            vr, vi = vectors[:dates], vectors[dates:]
            vs = [a + b for a, b in zip(vr, vi)]
            out_r, out_i = [], []
            for rows_in in groups:
                sums = {i: [None, None, None] for i in rows_in}
                for i in rows_in:
                    for j in range(dates):
                        if j == i or (j in rows_in and j < i):
                            continue
                        e = index[min(i, j), max(i, j)]
                        re, plus, minus = sq[e], sq[count + e], sq[2 * count + e]
                        s = sums[i]
                        if i < j:
                            s[0] = add_to(s[0], 1, re * vs[j])
                            s[1] = add_to(s[1], 1, minus * vr[j])
                            s[2] = add_to(s[2], 1, plus * vi[j])
                            if j in rows_in:
                                s = sums[j]
                                s[0] = add_to(s[0], 1, re * vs[i])
                                s[1] = add_to(s[1], -1, plus * vr[i])
                                s[2] = add_to(s[2], -1, minus * vi[i])
                        else:
                            s[0] = add_to(s[0], 1, re * vs[j])
                            s[1] = add_to(s[1], -1, plus * vr[j])
                            s[2] = add_to(s[2], -1, minus * vi[j])
                for i in rows_in:
                    own = sq[3 * count + i]
                    s = sums[i]
                    out_r.append(s[0] - s[2] + own * vr[i])
                    out_i.append(s[0] + s[1] + own * vi[i])
            return tuple(out_r + out_i)

        vectors = lax.fori_loop(0, steps, step, tuple(vec[i] for i in range(2 * dates)))
        length = None
        for part in vectors:
            length = add_to(length, 1, part * part)
        scale = lax.rsqrt(length)
        vr = [a * scale for a in vectors[:dates]]
        vi = [a * scale for a in vectors[dates:]]
        for i in range(dates):
            vec[i] = vr[i]
            vec[dates + i] = vi[i]
        cr = ci = None
        for i in range(dates):
            zr, zi = z_ref[0, i, k], z_ref[1, i, k]
            cr = add_to(cr, 1, vr[i] * zr + vi[i] * zi)
            ci = add_to(ci, 1, vr[i] * zi - vi[i] * zr)
        comp_ref[0, k] = cr
        comp_ref[1, k] = ci
        ref_r = vec[chosen_ref[0]] * float(dates)
        ref_i = vec[dates + chosen_ref[0]] * float(dates)
        for i in range(dates):
            link_ref[0, i, k] = vr[i] * ref_r + vi[i] * ref_i
            link_ref[1, i, k] = vi[i] * ref_r - vr[i] * ref_i
        return carry

    lax.fori_loop(0, half, one_vector, 0)
    for k in range(HALF_ROWS):
        re, im = comp_ref[0, k], comp_ref[1, k]
        first = jnp.where(top, re, flip(im))
        second = jnp.where(top, flip(re), im)
        pack_x_ref[k] = jnp.where(odd_device, first, second)
        pack_y_ref[k] = jnp.where(odd_device, second, first)


def extend_kernel(par_ref, comp_ref, x_ref, y_ref, out_ref):
    top = upper()
    odd_device = par_ref[0] == 1
    for k in range(HALF_ROWS):
        a, b = x_ref[k], y_ref[k]
        re, im = unpack(jnp.where(odd_device, a, b), jnp.where(odd_device, b, a), top)
        out_ref[0, HALF_ROWS - 1 - k] = re
        out_ref[1, HALF_ROWS - 1 - k] = im
    for part in range(2):
        for k in range(comp_ref.shape[1]):
            out_ref[part, HALF_ROWS + k] = comp_ref[part, k]


def offsets_kernel(tiles, place_ref, own_ref, a_ref, b_ref, unit_ref, total_ref):
    lanes, edges = masks(tiles)
    half = unit_ref.shape[1]
    odd_stack = place_ref[1] == 1
    first_stack = place_ref[0] == 0

    def whole(ref):
        parts = []
        for part in range(2):
            rows_in = [ref[part, k] for k in range(ref.shape[1])]
            rows_in += [flip(rows_in[-1 - k]) for k in range(HALF_ROWS)]
            parts.append(rows_in)
        return parts

    def power(re, im):
        return box_sum([a * a + b * b for a, b in zip(re, im)], lanes, edges)

    own_r, own_i = whole(own_ref)
    own = [p + 1.0 for p in power(own_r, own_i)]

    def unit(ref):
        re, im = whole(ref)
        other = power(re, im)
        cross_r = box_sum(
            [a * c + b * d for a, b, c, d in zip(own_r, own_i, re, im)], lanes, edges
        )
        cross_i = box_sum(
            [b * c - a * d for a, b, c, d in zip(own_r, own_i, re, im)], lanes, edges
        )
        out = []
        for k in range(half):
            scale = lax.rsqrt(own[k] * (other[k] + 1.0))
            off_r, off_i = cross_r[k] * scale, cross_i[k] * scale
            bound = jnp.maximum(jnp.sqrt(off_r * off_r + off_i * off_i), LINK_FLOOR)
            back = 1.0 / bound
            out.append((off_r * back, off_i * back))
        return out

    pair_a, pair_b = unit(a_ref), unit(b_ref)
    for k in range(half):
        (ar, ai), (br, bi) = pair_a[k], pair_b[k]
        before_r = jnp.where(odd_stack, ar, br)
        before_i = -jnp.where(odd_stack, ai, bi)
        after_r = jnp.where(odd_stack, br, ar)
        after_i = jnp.where(odd_stack, bi, ai)
        before_r = jnp.where(first_stack, 1.0, before_r)
        before_i = jnp.where(first_stack, 0.0, before_i)
        unit_ref[0, k] = before_r
        unit_ref[1, k] = before_i
        total_ref[0, k] = before_r * after_r - before_i * after_i
        total_ref[1, k] = before_r * after_i + before_i * after_r


def result_kernel(rows, tiles, link_ref, datum_ref, out_ref):
    half = rows // 2

    def one_date(t, carry):
        for k in range(half):
            lr, li = link_ref[0, t, k], link_ref[1, t, k]
            dr, di = datum_ref[0, k], datum_ref[1, k]
            first, second = bases(k, rows, tiles)
            for part, value in enumerate((lr * dr - li * di, lr * di + li * dr)):
                out_ref[part, t, pl.ds(first, tiles, stride=SUB), :] = value[:tiles]
                out_ref[part, t, pl.ds(second, tiles, stride=SUB), :] = value[tiles:]
        return carry

    lax.fori_loop(0, link_ref.shape[1], one_date, 0)


def swaps(count, bit=None, odd=False):
    if bit is not None:
        return [(i, i ^ bit) for i in range(count) if (i ^ bit) < count]
    first = 1 if odd else 0
    pairs = [(i, i + 1) for i in range(first, count - 1, 2)]
    return pairs + [(j, i) for i, j in pairs]


def times(a, b):
    return jnp.stack([a[0] * b[0] - a[1] * b[1], a[0] * b[1] + a[1] * b[0]])


def local(amplitude, phase, validity, iterations, reference_date):
    dates, rows, columns = amplitude.shape
    half = rows // 2
    tiles = columns // LANES
    ext = half + HALF_ROWS
    members = lax.axis_size("tm")
    blocks = lax.axis_size("space")
    place = lax.axis_index("tm")
    parity = (lax.axis_index("space") % 2).reshape(1)
    params = pltpu.CompilerParams(vmem_limit_bytes=VMEM_LIMIT)

    def shape(*dims):
        return jax.ShapeDtypeStruct(dims, jnp.float32)

    def tiled(x):
        lead = x.shape[:-2]
        x = x.reshape(lead + (rows // SUB, SUB, tiles, LANES))
        return jnp.swapaxes(x, -3, -2).reshape(lead + (rows * tiles, LANES))

    z, slab_x, slab_y = pl.pallas_call(
        lambda *refs: images_kernel(rows, tiles, *refs),
        out_shape=(
            shape(2, dates, ext, SUB, LANES),
            shape(dates, HALF_ROWS, SUB, LANES),
            shape(dates, HALF_ROWS, SUB, LANES),
        ),
        in_specs=[smem(), vmem(), vmem(), vmem()],
        out_specs=(vmem(), vmem(), vmem()),
        compiler_params=params,
        name="images",
    )(parity, tiled(amplitude), tiled(phase), tiled(validity))
    pair_x, pair_y = swaps(blocks), swaps(blocks, odd=True)
    got_y = lax.ppermute(slab_y, "space", pair_y)
    got_x = lax.ppermute(slab_x, "space", pair_x)

    count = dates * (dates - 1) // 2
    linked, comp, pack_x, pack_y = pl.pallas_call(
        lambda *refs: phases_kernel(tiles, *refs),
        out_shape=(
            shape(2, dates, half, SUB, LANES),
            shape(2, half, SUB, LANES),
            shape(HALF_ROWS, SUB, LANES),
            shape(HALF_ROWS, SUB, LANES),
        ),
        in_specs=[smem(), smem(), smem(), vmem(), vmem(), vmem()],
        out_specs=(vmem(), vmem(), vmem(), vmem()),
        scratch_shapes=[
            pltpu.VMEM((2, dates, HALF_ROWS, SUB, LANES), jnp.float32),
            pltpu.VMEM((dates, half, SUB, LANES), jnp.float32),
            pltpu.VMEM((count, half, SUB, LANES), jnp.float32),
            pltpu.VMEM((count, half, SUB, LANES), jnp.float32),
            pltpu.VMEM((2 * count, SUB, LANES), jnp.float32),
            pltpu.VMEM((3 * count + dates, SUB, LANES), jnp.float32),
            pltpu.VMEM((2 * dates, SUB, LANES), jnp.float32),
        ],
        compiler_params=params,
        name="phases",
    )(parity, iterations, reference_date, z, got_x, got_y)

    more_y = lax.ppermute(pack_y, "space", pair_y)
    more_x = lax.ppermute(pack_x, "space", pair_x)
    wide = pl.pallas_call(
        extend_kernel,
        out_shape=shape(2, ext, SUB, LANES),
        in_specs=[smem(), vmem(), vmem(), vmem()],
        out_specs=vmem(),
        compiler_params=params,
        name="extend",
    )(parity, comp, more_x, more_y)
    other_a = lax.ppermute(wide, "tm", swaps(members))
    other_b = lax.ppermute(wide, "tm", swaps(members, odd=True))
    where = jnp.stack([place, place % 2]).astype(jnp.int32)
    datum, total = pl.pallas_call(
        lambda *refs: offsets_kernel(tiles, *refs),
        out_shape=(shape(2, half, SUB, LANES), shape(2, half, SUB, LANES)),
        in_specs=[smem(), vmem(), vmem(), vmem()],
        out_specs=(vmem(), vmem()),
        compiler_params=params,
        name="offsets",
    )(where, wide, other_a, other_b)
    bit = 2
    while bit < members:
        other = lax.ppermute(total, "tm", swaps(members, bit=bit))
        datum = jnp.where((place & bit) != 0, times(datum, other), datum)
        total = times(total, other)
        bit *= 2
    out = pl.pallas_call(
        lambda *refs: result_kernel(rows, tiles, *refs),
        out_shape=shape(2, dates, rows * tiles, LANES),
        in_specs=[vmem(), vmem()],
        out_specs=vmem(),
        compiler_params=params,
        name="result",
    )(linked, datum)
    out = out.reshape(2, dates, rows // SUB, tiles, SUB, LANES)
    return jnp.swapaxes(out, -3, -2).reshape(2, dates, rows, columns)


def solution(mesh):
    return jax.shard_map(
        local,
        mesh=mesh,
        in_specs=(
            P("tm", "space", None),
            P("tm", "space", None),
            P("space", None),
            P("tm"),
            P("tm"),
        ),
        out_specs=P(None, "tm", "space", None),
        check_vma=False,
    )
```

```python
import jax
import jax.numpy as jnp
from jax import lax
from jax.experimental import pallas as pl
from jax.experimental.pallas import tpu as pltpu
from jax.sharding import PartitionSpec as P

WIN_ROWS = 11
WIN_COLS = 5
INNER_DONE = 2
ITERS = 20
HALF_ROWS = WIN_ROWS // 2

MASKED_WEIGHT = 0.125
LINK_FLOOR = 0.03

LANES = 128
SUB = 8
VMEM_LIMIT = 40 * 1024 * 1024


def vmem():
    return pl.BlockSpec(memory_space=pltpu.VMEM)


def smem():
    return pl.BlockSpec(memory_space=pltpu.SMEM)


def sublane():
    return lax.broadcasted_iota(jnp.int32, (SUB, LANES), 0)


def lane():
    return lax.broadcasted_iota(jnp.int32, (SUB, LANES), 1)


def flip(x):
    return pltpu.roll(x, SUB // 2, 0)


def upper():
    return sublane() < SUB // 2


def bases(k, rows, tiles):
    def base(row):
        return (row // SUB) * SUB * tiles + row % SUB

    return base(k), base(rows - 1 - k)


def load_pair(ref, lead, k, rows, tiles, top):
    first, second = bases(k, rows, tiles)
    a = ref[lead + (pl.ds(first, SUB, stride=SUB), slice(None))]
    b = ref[lead + (pl.ds(second - SUB * tiles, SUB, stride=SUB), slice(None))]
    return jnp.where(top, a, b)


def sin_cos(x):
    turns = jnp.round(x * (2.0 / jnp.pi))
    r = (x - turns * 1.5707855224609375) - turns * 1.0804334124e-05
    s = r * r
    sine = r + r * s * (-1.6666654611e-1 + s * (8.3321608736e-3 + s * -1.9515295891e-4))
    cosine = 1.0 - 0.5 * s + s * s * (
        4.166664568298827e-2 + s * (-1.388731625493765e-3 + s * 2.443315711809948e-5)
    )
    size = jnp.abs(turns)
    odd = size == 1.0
    base_s = jnp.where(odd, cosine, sine)
    base_c = jnp.where(odd, sine, cosine)
    sin_x = jnp.where((turns == -1.0) | (size == 2.0), -base_s, base_s)
    cos_x = jnp.where((turns == 1.0) | (size == 2.0), -base_c, base_c)
    return sin_x, cos_x


def images_kernel(rows, tiles, par_ref, amp_ref, phase_ref, valid_ref, z_ref, x_ref, y_ref):
    half = rows // 2
    top = upper()
    odd = par_ref[0] == 1
    roots = []
    for k in range(half):
        valid = load_pair(valid_ref, (), k, rows, tiles, top)
        roots.append(jnp.where(valid == 1, 1.0, MASKED_WEIGHT**0.5).astype(jnp.float32))

    def one_date(t, carry):
        for k in range(half):
            amp = load_pair(amp_ref, (t,), k, rows, tiles, top) * roots[k]
            sin_x, cos_x = sin_cos(load_pair(phase_ref, (t,), k, rows, tiles, top))
            re, im = amp * cos_x, amp * sin_x
            z_ref[0, t, k] = re
            z_ref[1, t, k] = im
            if k >= half - HALF_ROWS:
                z_ref[0, t, 2 * half - 1 - k] = flip(re)
                z_ref[1, t, 2 * half - 1 - k] = flip(im)
            if k < HALF_ROWS:
                first, second = pack(re, im, top)
                x_ref[t, k] = jnp.where(odd, first, second)
                y_ref[t, k] = jnp.where(odd, second, first)
        return carry

    lax.fori_loop(0, z_ref.shape[1], one_date, 0)


def unpack(first, second, top):
    return jnp.where(top, first, flip(second)), jnp.where(top, flip(first), second)


def pack(re, im, top):
    return jnp.where(top, re, flip(im)), jnp.where(top, flip(re), im)


def add_to(total, sign, value):
    if total is None:
        return value if sign > 0 else -value
    return total + value if sign > 0 else total - value


def running(values):
    out = [values[0]]
    for value in values[1:]:
        out.append(out[-1] + value)
    return out


def inner_sums(field):
    count = len(field) - WIN_ROWS + 1
    tails = running(field[WIN_ROWS - 1 :: -1])[::-1]
    if count <= WIN_ROWS:
        core = running(field[count - 1 : WIN_ROWS])[-1]
        tails = running([core] + field[: count - 1][::-1])[::-1]
    heads = running(field[WIN_ROWS:])
    middle = [tails[q] + heads[q - 1] for q in range(1, min(count, WIN_ROWS))]
    return [tails[0]] + middle + heads[WIN_ROWS - 1 :]


def fill_band(band_ref):
    at = lax.broadcasted_iota(jnp.int32, band_ref.shape, 0) % LANES
    to = lax.broadcasted_iota(jnp.int32, band_ref.shape, 1)
    reach = WIN_COLS // 2
    inside = (to < LANES) & (jnp.abs(at - to) <= reach)
    to = to - LANES
    beside = (to >= 0) & ((at >= to + LANES - reach) | (at <= to - LANES + reach))
    band_ref[...] = jnp.where(inside | beside, 1.0, 0.0).astype(band_ref.dtype)


def put_split(ref, at, vectors):
    x = jnp.concatenate(vectors, axis=0)
    high = x.astype(jnp.bfloat16)
    low = (x - high.astype(jnp.float32)).astype(jnp.bfloat16)
    ref[at, :, :LANES] = high
    ref[at, :, LANES:] = low


def side_masks(tiles):
    column = sublane() % tiles
    at = lane()
    return (at < LANES // 2) & (column != 0), (at >= LANES // 2) & (column != tiles - 1)


def column_sums(split_ref, first, size, band, sides):
    rows = split_ref.shape[1]
    terms = split_ref[first : first + size].reshape(size * rows, 2 * LANES)
    both = jnp.dot(terms, band, preferred_element_type=jnp.float32)
    from_before, from_after = sides
    out = []
    for k in range(size * rows // SUB):
        inside = both[k * SUB : (k + 1) * SUB, :LANES]
        beside = both[k * SUB : (k + 1) * SUB, LANES:]
        before, after = pltpu.roll(beside, 1, 0), pltpu.roll(beside, SUB - 1, 0)
        out.append(
            inside + jnp.where(from_before, before, jnp.where(from_after, after, 0.0))
        )
    return out


def pair_list(dates):
    return [(i, j) for i in range(dates) for j in range(i + 1, dates)]


CHUNK = 5


def coherence(dates, vectors, fields, split_ref, band_ref, inv_ref, nr_ref, ni_ref, sides):
    pairs = pair_list(dates)
    band = band_ref[...]
    powers = [fields(i, i) for i in range(dates)]
    half = dates // 2
    for e in range(half):
        put_split(split_ref, e, powers[2 * e] + powers[2 * e + 1])
    sums = column_sums(split_ref, 0, half, band, sides)
    for i in range(dates):
        for k in range(vectors):
            inv_ref[i, k] = lax.rsqrt(sums[i * vectors + k]) * 0.5
    for first in range(0, len(pairs), CHUNK):
        size = min(CHUNK, len(pairs) - first)
        for e in range(first, first + size):
            re, im = fields(*pairs[e])
            put_split(split_ref, half + e, re + im)
        sums = column_sums(split_ref, half + first, size, band, sides)
        for e in range(first, first + size):
            i, j = pairs[e]
            base = (e - first) * 2 * vectors
            for k in range(vectors):
                scale = inv_ref[i, k] * inv_ref[j, k]
                nr_ref[e, k] = sums[base + k] * scale
                ni_ref[e, k] = sums[base + vectors + k] * scale


def cross(a, b):
    (ar, ai), (br, bi) = a, b
    re = [p * r + q * s for p, q, r, s in zip(ar, ai, br, bi)]
    im = [q * r - p * s for p, q, r, s in zip(ar, ai, br, bi)]
    return re, im


def power_of(a):
    return [p * p + q * q for p, q in zip(*a)]


def iterate(
    first, last, offset, dates, iter_ref, chosen_ref, z_ref, nr, ni, more, sq, vec,
    link_ref, comp_ref, out_offset=0,
):
    pairs = pair_list(dates)
    index = {pair: e for e, pair in enumerate(pairs)}
    count = len(pairs)
    turns = jnp.minimum(iter_ref[0], ITERS)
    odd_turns = turns % 2 == 1
    steps = jnp.where(odd_turns, turns // 2, turns // 2 - 1)
    groups = []
    at = 0
    for size in (3, 3, 4) if dates == 10 else (dates,):
        groups.append(tuple(range(at, at + size)))
        at += size

    def one_vector(whole_k, carry):
        k = whole_k - offset
        place = whole_k - out_offset
        for e in range(count):
            re, im = nr[e, k], ni[e, k]
            more[e] = re + im
            more[count + e] = im - re

        def left(i, t):
            if i < t:
                e = index[i, t]
                return (nr[e, k], 1), (more[e], 1), (more[count + e], 1)
            e = index[t, i]
            return (nr[e, k], 1), (more[count + e], -1), (more[e], -1)

        def right(t, j):
            if t < j:
                e = index[t, j]
                return (nr[e, k], 1), (ni[e, k], 1), (more[e], 1)
            e = index[j, t]
            return (nr[e, k], 1), (ni[e, k], -1), (more[count + e], -1)

        def square(out):
            sums = {pair: [None, None, None] for pair in out}
            rows_in = sorted({i for i, _ in out})
            cols_in = sorted({j for _, j in out})
            for t in range(dates):
                lefts = {i: left(i, t) for i in rows_in if i != t}
                rights = {j: right(t, j) for j in cols_in if j != t}
                for i, j in out:
                    if t in (i, j):
                        continue
                    (ar, _), (ap, sap), (aq, saq) = lefts[i]
                    (br, _), (bi, sbi), (bs, sbs) = rights[j]
                    s = sums[i, j]
                    s[0] = add_to(s[0], sbs, ar * bs)
                    s[1] = add_to(s[1], saq, aq * br)
                    s[2] = add_to(s[2], sap * sbi, ap * bi)
            for i, j in out:
                e = index[i, j]
                s = sums[i, j]
                re = s[0] - s[2] + nr[e, k]
                im = s[0] + s[1] + ni[e, k]
                sq[e] = re
                sq[count + e] = re + im
                sq[2 * count + e] = im - re

        for a in range(len(groups)):
            square([(i, j) for i in groups[a] for j in groups[a] if i < j])
            for b in range(a + 1, len(groups)):
                square([(i, j) for i in groups[a] for j in groups[b]])
        size = [None] * dates
        for e, (i, j) in enumerate(pairs):
            re, im = nr[e, k], ni[e, k]
            value = re * re + im * im
            size[i] = add_to(size[i], 1, value)
            size[j] = add_to(size[j], 1, value)
        for i in range(dates):
            sq[3 * count + i] = size[i] + 0.25

        def row_sums(re_of, im_of, own):
            sr, si = [own(i) for i in range(dates)], [None] * dates
            for e, (i, j) in enumerate(pairs):
                re, im = re_of(e), im_of(e)
                sr[i] = sr[i] + re
                sr[j] = sr[j] + re
                si[i] = add_to(si[i], 1, im)
                si[j] = add_to(si[j], -1, im)
            for i in range(dates):
                vec[i] = sr[i]
                vec[dates + i] = si[i]

        @pl.when(odd_turns)
        def _():
            row_sums(lambda e: nr[e, k], lambda e: ni[e, k],
                     lambda i: jnp.full((SUB, LANES), 0.5, jnp.float32))

        @pl.when(jnp.logical_not(odd_turns))
        def _():
            row_sums(lambda e: sq[e], lambda e: sq[count + e] - sq[e],
                     lambda i: sq[3 * count + i])

        def step(_, vectors):
            vr, vi = vectors[:dates], vectors[dates:]
            vs = [a + b for a, b in zip(vr, vi)]
            out_r, out_i = [], []
            for rows_in in groups:
                sums = {i: [None, None, None] for i in rows_in}
                for i in rows_in:
                    for j in range(dates):
                        if j == i or (j in rows_in and j < i):
                            continue
                        e = index[min(i, j), max(i, j)]
                        re, plus, minus = sq[e], sq[count + e], sq[2 * count + e]
                        s = sums[i]
                        if i < j:
                            s[0] = add_to(s[0], 1, re * vs[j])
                            s[1] = add_to(s[1], 1, minus * vr[j])
                            s[2] = add_to(s[2], 1, plus * vi[j])
                            if j in rows_in:
                                s = sums[j]
                                s[0] = add_to(s[0], 1, re * vs[i])
                                s[1] = add_to(s[1], -1, plus * vr[i])
                                s[2] = add_to(s[2], -1, minus * vi[i])
                        else:
                            s[0] = add_to(s[0], 1, re * vs[j])
                            s[1] = add_to(s[1], -1, plus * vr[j])
                            s[2] = add_to(s[2], -1, minus * vi[j])
                for i in rows_in:
                    own = sq[3 * count + i]
                    s = sums[i]
                    out_r.append(s[0] - s[2] + own * vr[i])
                    out_i.append(s[0] + s[1] + own * vi[i])
            return tuple(out_r + out_i)

        vectors = lax.fori_loop(0, steps, step, tuple(vec[i] for i in range(2 * dates)))
        length = None
        for part in vectors:
            length = add_to(length, 1, part * part)
        scale = lax.rsqrt(length)
        vr = [a * scale for a in vectors[:dates]]
        vi = [a * scale for a in vectors[dates:]]
        for i in range(dates):
            vec[i] = vr[i]
            vec[dates + i] = vi[i]
        cr = ci = None
        for i in range(dates):
            zr, zi = z_ref[0, i, whole_k], z_ref[1, i, whole_k]
            cr = add_to(cr, 1, vr[i] * zr + vi[i] * zi)
            ci = add_to(ci, 1, vr[i] * zi - vi[i] * zr)
        comp_ref[0, place] = cr
        comp_ref[1, place] = ci
        ref_r = vec[chosen_ref[0]] * float(dates)
        ref_i = vec[dates + chosen_ref[0]] * float(dates)
        for i in range(dates):
            link_ref[0, i, place] = vr[i] * ref_r + vi[i] * ref_i
            link_ref[1, i, place] = vi[i] * ref_r - vr[i] * ref_i
        return carry

    lax.fori_loop(first, last, one_vector, 0)


def inner_kernel(
    tiles, done, iter_ref, chosen_ref, z_ref,
    nr, ni, part_ref, link_ref, comp_ref,
    band, split, inv, more, sq, vec,
):
    dates = z_ref.shape[1]
    vectors = nr.shape[1]
    ext = vectors + 2 * HALF_ROWS
    pairs = pair_list(dates)
    count = len(pairs)
    index = {pair: e for e, pair in enumerate(pairs)}
    fill_band(band)

    def image(t):
        return [[z_ref[part, t, k] for k in range(ext)] for part in range(2)]

    def keep(at, field):
        heads = running(field[: 2 * HALF_ROWS])
        for k in range(HALF_ROWS):
            part_ref[at, k] = heads[HALF_ROWS + k]

    def fields(i, j):
        if i == j:
            power = power_of(image(i))
            keep(2 * count + i, power)
            return inner_sums(power)
        re, im = cross(image(i), image(j))
        e = index[i, j]
        keep(e, re)
        keep(count + e, im)
        return inner_sums(re), inner_sums(im)

    coherence(dates, vectors, fields, split, band, inv, nr, ni, side_masks(tiles))
    iterate(
        HALF_ROWS, HALF_ROWS + done, HALF_ROWS, dates, iter_ref, chosen_ref, z_ref, nr, ni,
        more, sq, vec, link_ref, comp_ref, HALF_ROWS,
    )


def outer_kernel(
    tiles, par_ref, iter_ref, chosen_ref, z_ref, part_ref, x_ref, y_ref,
    link_ref, comp_ref, pack_x_ref, pack_y_ref,
    halo, band, split, inv, nr, ni, more, sq, vec,
):
    dates = z_ref.shape[1]
    top = upper()
    odd_device = par_ref[0] == 1
    pairs = pair_list(dates)
    count = len(pairs)
    index = {pair: e for e, pair in enumerate(pairs)}
    fill_band(band)

    def fill(t, carry):
        for k in range(HALF_ROWS):
            a, b = x_ref[t, k], y_ref[t, k]
            re, im = unpack(jnp.where(odd_device, a, b), jnp.where(odd_device, b, a), top)
            halo[0, t, k] = re
            halo[1, t, k] = im
        return carry

    lax.fori_loop(0, dates, fill, 0)

    def image(t):
        return [[halo[part, t, k] for k in range(HALF_ROWS)] for part in range(2)]

    def add(at, field):
        tails = running(field)
        return [tails[HALF_ROWS - 1 - k] + part_ref[at, k] for k in range(HALF_ROWS)]

    def fields(i, j):
        if i == j:
            return add(2 * count + i, power_of(image(i)))
        re, im = cross(image(i), image(j))
        e = index[i, j]
        return add(e, re), add(count + e, im)

    coherence(dates, HALF_ROWS, fields, split, band, inv, nr, ni, side_masks(tiles))
    iterate(
        0, HALF_ROWS, 0, dates, iter_ref, chosen_ref, z_ref, nr, ni, more, sq, vec,
        link_ref, comp_ref,
    )
    for k in range(HALF_ROWS):
        first, second = pack(comp_ref[0, k], comp_ref[1, k], top)
        pack_x_ref[k] = jnp.where(odd_device, first, second)
        pack_y_ref[k] = jnp.where(odd_device, second, first)


def rest_kernel(
    start, iter_ref, chosen_ref, z_ref, nr, ni, after_ref, link_ref, comp_ref, more, sq, vec
):
    dates = z_ref.shape[1]
    iterate(
        start, start + comp_ref.shape[1], HALF_ROWS, dates, iter_ref, chosen_ref, z_ref, nr, ni,
        more, sq, vec, link_ref, comp_ref, start,
    )


def box_sum(field, lanes, edges):
    last_two, last_one, first_one, first_two = lanes
    keep_before, keep_after = edges
    out = []
    for x in inner_sums(field):
        before = jnp.where(keep_before, pltpu.roll(x, 1, 0), 0.0)
        after = jnp.where(keep_after, pltpu.roll(x, SUB - 1, 0), 0.0)
        near = pltpu.roll(jnp.where(last_one, before, x), 1, 1) + pltpu.roll(
            jnp.where(first_one, after, x), LANES - 1, 1
        )
        far = pltpu.roll(jnp.where(last_two, before, x), 2, 1) + pltpu.roll(
            jnp.where(first_two, after, x), LANES - 2, 1
        )
        out.append(x + near + far)
    return out


def masks(tiles):
    at = lane()
    lanes = (at >= LANES - 2, at >= LANES - 1, at < 1, at < 2)
    column = sublane() % tiles
    return lanes, (column != 0, column != tiles - 1)


def extend_kernel(par_ref, outer_ref, inner_ref, rest_ref, x_ref, y_ref, out_ref):
    top = upper()
    odd_device = par_ref[0] == 1
    for k in range(HALF_ROWS):
        a, b = x_ref[k], y_ref[k]
        re, im = unpack(jnp.where(odd_device, a, b), jnp.where(odd_device, b, a), top)
        out_ref[0, HALF_ROWS - 1 - k] = re
        out_ref[1, HALF_ROWS - 1 - k] = im
    for part in range(2):
        at = HALF_ROWS
        for ref in (outer_ref, inner_ref, rest_ref):
            for k in range(ref.shape[1]):
                out_ref[part, at] = ref[part, k]
                at += 1


def offsets_kernel(tiles, place_ref, own_ref, a_ref, b_ref, unit_ref, total_ref):
    lanes, edges = masks(tiles)
    half = unit_ref.shape[1]
    odd_stack = place_ref[1] == 1
    first_stack = place_ref[0] == 0

    def whole(ref):
        parts = []
        for part in range(2):
            rows_in = [ref[part, k] for k in range(ref.shape[1])]
            rows_in += [flip(rows_in[-1 - k]) for k in range(HALF_ROWS)]
            parts.append(rows_in)
        return parts

    def power(re, im):
        return box_sum([a * a + b * b for a, b in zip(re, im)], lanes, edges)

    own_r, own_i = whole(own_ref)
    own = [p + 1.0 for p in power(own_r, own_i)]

    def unit(ref):
        re, im = whole(ref)
        other = power(re, im)
        cross_r = box_sum(
            [a * c + b * d for a, b, c, d in zip(own_r, own_i, re, im)], lanes, edges
        )
        cross_i = box_sum(
            [b * c - a * d for a, b, c, d in zip(own_r, own_i, re, im)], lanes, edges
        )
        out = []
        for k in range(half):
            scale = lax.rsqrt(own[k] * (other[k] + 1.0))
            off_r, off_i = cross_r[k] * scale, cross_i[k] * scale
            bound = jnp.maximum(jnp.sqrt(off_r * off_r + off_i * off_i), LINK_FLOOR)
            back = 1.0 / bound
            out.append((off_r * back, off_i * back))
        return out

    pair_a, pair_b = unit(a_ref), unit(b_ref)
    for k in range(half):
        (ar, ai), (br, bi) = pair_a[k], pair_b[k]
        before_r = jnp.where(odd_stack, ar, br)
        before_i = -jnp.where(odd_stack, ai, bi)
        after_r = jnp.where(odd_stack, br, ar)
        after_i = jnp.where(odd_stack, bi, ai)
        before_r = jnp.where(first_stack, 1.0, before_r)
        before_i = jnp.where(first_stack, 0.0, before_i)
        unit_ref[0, k] = before_r
        unit_ref[1, k] = before_i
        total_ref[0, k] = before_r * after_r - before_i * after_i
        total_ref[1, k] = before_r * after_i + before_i * after_r


def result_kernel(rows, tiles, outer_ref, inner_ref, rest_ref, datum_ref, out_ref):
    half = rows // 2
    links = [
        (ref, k) for ref in (outer_ref, inner_ref, rest_ref) for k in range(ref.shape[2])
    ]

    def one_date(t, carry):
        for k in range(half):
            ref, at = links[k]
            lr, li = ref[0, t, at], ref[1, t, at]
            dr, di = datum_ref[0, k], datum_ref[1, k]
            first, second = bases(k, rows, tiles)
            for part, value in enumerate((lr * dr - li * di, lr * di + li * dr)):
                out_ref[part, t, pl.ds(first, tiles, stride=SUB), :] = value[:tiles]
                out_ref[part, t, pl.ds(second, tiles, stride=SUB), :] = value[tiles:]
        return carry

    lax.fori_loop(0, outer_ref.shape[1], one_date, 0)


def swaps(count, bit=None, odd=False):
    if bit is not None:
        return [(i, i ^ bit) for i in range(count) if (i ^ bit) < count]
    first = 1 if odd else 0
    pairs = [(i, i + 1) for i in range(first, count - 1, 2)]
    return pairs + [(j, i) for i, j in pairs]


def times(a, b):
    return jnp.stack([a[0] * b[0] - a[1] * b[1], a[0] * b[1] + a[1] * b[0]])


def local(amplitude, phase, validity, iterations, reference_date):
    dates, rows, columns = amplitude.shape
    half = rows // 2
    tiles = columns // LANES
    ext = half + HALF_ROWS
    members = lax.axis_size("tm")
    blocks = lax.axis_size("space")
    place = lax.axis_index("tm")
    parity = (lax.axis_index("space") % 2).reshape(1)
    params = pltpu.CompilerParams(vmem_limit_bytes=VMEM_LIMIT)

    def shape(*dims):
        return jax.ShapeDtypeStruct(dims, jnp.float32)

    def tiled(x):
        lead = x.shape[:-2]
        x = x.reshape(lead + (rows // SUB, SUB, tiles, LANES))
        return jnp.swapaxes(x, -3, -2).reshape(lead + (rows * tiles, LANES))

    z, slab_x, slab_y = pl.pallas_call(
        lambda *refs: images_kernel(rows, tiles, *refs),
        out_shape=(
            shape(2, dates, ext, SUB, LANES),
            shape(dates, HALF_ROWS, SUB, LANES),
            shape(dates, HALF_ROWS, SUB, LANES),
        ),
        in_specs=[smem(), vmem(), vmem(), vmem()],
        out_specs=(vmem(), vmem(), vmem()),
        compiler_params=params,
        name="images",
    )(parity, tiled(amplitude), tiled(phase), tiled(validity))
    pair_x, pair_y = swaps(blocks), swaps(blocks, odd=True)
    got_y = lax.ppermute(slab_y, "space", pair_y)
    got_x = lax.ppermute(slab_x, "space", pair_x)

    count = dates * (dates - 1) // 2
    inner = half - HALF_ROWS
    done = min(INNER_DONE, inner - 1)
    work = [
        pltpu.VMEM((2 * count, SUB, LANES), jnp.float32),
        pltpu.VMEM((3 * count + dates, SUB, LANES), jnp.float32),
        pltpu.VMEM((2 * dates, SUB, LANES), jnp.float32),
    ]

    def window_work(vectors):
        return [
            pltpu.VMEM((2 * LANES, 2 * LANES), jnp.bfloat16),
            pltpu.VMEM((dates // 2 + count, 2 * vectors * SUB, 2 * LANES), jnp.bfloat16),
            pltpu.VMEM((dates, vectors, SUB, LANES), jnp.float32),
        ]

    def cost(vectors):
        return pl.CostEstimate(
            flops=vectors * 2_000_000 * 8, bytes_accessed=1 << 20, transcendentals=0
        )

    nr, ni, part, linked_a, comp_a = pl.pallas_call(
        lambda *refs: inner_kernel(tiles, done, *refs),
        out_shape=(
            shape(count, inner, SUB, LANES),
            shape(count, inner, SUB, LANES),
            shape(2 * count + dates, HALF_ROWS, SUB, LANES),
            shape(2, dates, done, SUB, LANES),
            shape(2, done, SUB, LANES),
        ),
        in_specs=[smem(), smem(), vmem()],
        out_specs=(vmem(),) * 5,
        scratch_shapes=window_work(inner) + work,
        compiler_params=params,
        cost_estimate=cost(4),
        name="inner",
    )(iterations, reference_date, z)
    linked_b, comp_b, pack_x, pack_y = pl.pallas_call(
        lambda *refs: outer_kernel(tiles, *refs),
        out_shape=(
            shape(2, dates, HALF_ROWS, SUB, LANES),
            shape(2, HALF_ROWS, SUB, LANES),
            shape(HALF_ROWS, SUB, LANES),
            shape(HALF_ROWS, SUB, LANES),
        ),
        in_specs=[smem(), smem(), smem()] + [vmem()] * 4,
        out_specs=(vmem(),) * 4,
        scratch_shapes=[pltpu.VMEM((2, dates, HALF_ROWS, SUB, LANES), jnp.float32)]
        + window_work(HALF_ROWS)
        + [
            pltpu.VMEM((count, HALF_ROWS, SUB, LANES), jnp.float32),
            pltpu.VMEM((count, HALF_ROWS, SUB, LANES), jnp.float32),
        ]
        + work,
        compiler_params=params,
        cost_estimate=cost(7),
        name="outer",
    )(parity, iterations, reference_date, z, part, got_x, got_y)
    start = HALF_ROWS + done
    linked_c, comp_c = pl.pallas_call(
        lambda *refs: rest_kernel(start, *refs),
        out_shape=(
            shape(2, dates, half - start, SUB, LANES),
            shape(2, half - start, SUB, LANES),
        ),
        in_specs=[smem(), smem()] + [vmem()] * 4,
        out_specs=(vmem(),) * 2,
        scratch_shapes=work,
        compiler_params=params,
        cost_estimate=cost(5),
        name="rest",
    )(iterations, reference_date, z, nr, ni, pack_x)

    more_y = lax.ppermute(pack_y, "space", pair_y)
    more_x = lax.ppermute(pack_x, "space", pair_x)
    wide = pl.pallas_call(
        extend_kernel,
        out_shape=shape(2, ext, SUB, LANES),
        in_specs=[smem()] + [vmem()] * 5,
        out_specs=vmem(),
        compiler_params=params,
        name="extend",
    )(parity, comp_b, comp_a, comp_c, more_x, more_y)
    other_a = lax.ppermute(wide, "tm", swaps(members))
    other_b = lax.ppermute(wide, "tm", swaps(members, odd=True))
    where = jnp.stack([place, place % 2]).astype(jnp.int32)
    datum, total = pl.pallas_call(
        lambda *refs: offsets_kernel(tiles, *refs),
        out_shape=(shape(2, half, SUB, LANES), shape(2, half, SUB, LANES)),
        in_specs=[smem(), vmem(), vmem(), vmem()],
        out_specs=(vmem(), vmem()),
        compiler_params=params,
        name="offsets",
    )(where, wide, other_a, other_b)
    bit = 2
    while bit < members:
        other = lax.ppermute(total, "tm", swaps(members, bit=bit))
        datum = jnp.where((place & bit) != 0, times(datum, other), datum)
        total = times(total, other)
        bit *= 2
    out = pl.pallas_call(
        lambda *refs: result_kernel(rows, tiles, *refs),
        out_shape=shape(2, dates, rows * tiles, LANES),
        in_specs=[vmem()] * 4,
        out_specs=vmem(),
        compiler_params=params,
        name="result",
    )(linked_b, linked_a, linked_c, datum)
    out = out.reshape(2, dates, rows // SUB, tiles, SUB, LANES)
    return jnp.swapaxes(out, -3, -2).reshape(2, dates, rows, columns)


def solution(mesh):
    return jax.shard_map(
        local,
        mesh=mesh,
        in_specs=(
            P("tm", "space", None),
            P("tm", "space", None),
            P("space", None),
            P("tm"),
            P("tm"),
        ),
        out_specs=P(None, "tm", "space", None),
        check_vma=False,
    )
```

```python
import jax
import jax.numpy as jnp
from jax import lax
from jax.experimental import pallas as pl
from jax.experimental.pallas import tpu as pltpu
from jax.sharding import PartitionSpec as P


WIN_ROWS = 11
WIN_COLS = 5
INNER_DONE = 1
MIDDLE = 2
PIECE = 5
ITERS = 20
HALF_ROWS = WIN_ROWS // 2

MASKED_WEIGHT = 0.125
LINK_FLOOR = 0.03

LANES = 128
SUB = 8
VMEM_LIMIT = 52 * 1024 * 1024


def vmem():
    return pl.BlockSpec(memory_space=pltpu.VMEM)


def hbm():
    return pl.BlockSpec(memory_space=pltpu.MemorySpace.HBM)


def smem():
    return pl.BlockSpec(memory_space=pltpu.SMEM)


def sublane():
    return lax.broadcasted_iota(jnp.int32, (SUB, LANES), 0)


def lane():
    return lax.broadcasted_iota(jnp.int32, (SUB, LANES), 1)


def flip(x):
    return pltpu.roll(x, SUB // 2, 0)


def upper():
    return sublane() < SUB // 2


def bases(k, rows, tiles):
    def base(row):
        return (row // SUB) * SUB * tiles + row % SUB

    return base(k), base(rows - 1 - k)


def load_pair(ref, lead, k, rows, tiles, top):
    first, second = bases(k, rows, tiles)
    a = ref[lead + (pl.ds(first, SUB, stride=SUB), slice(None))]
    b = ref[lead + (pl.ds(second - SUB * tiles, SUB, stride=SUB), slice(None))]
    return jnp.where(top, a, b)


def sin_cos(x):
    turns = jnp.round(x * (2.0 / jnp.pi))
    r = (x - turns * 1.5707855224609375) - turns * 1.0804334124e-05
    s = r * r
    sine = r + r * s * (-1.6666654611e-1 + s * (8.3321608736e-3 + s * -1.9515295891e-4))
    cosine = 1.0 - 0.5 * s + s * s * (
        4.166664568298827e-2 + s * (-1.388731625493765e-3 + s * 2.443315711809948e-5)
    )
    size = jnp.abs(turns)
    odd = size == 1.0
    base_s = jnp.where(odd, cosine, sine)
    base_c = jnp.where(odd, sine, cosine)
    sin_x = jnp.where((turns == -1.0) | (size == 2.0), -base_s, base_s)
    cos_x = jnp.where((turns == 1.0) | (size == 2.0), -base_c, base_c)
    return sin_x, cos_x


def images_kernel(
    rows, tiles, par_ref, amp_hbm, phase_hbm, valid_hbm, z_ref, x_ref, y_ref,
    amp_ref, phase_ref, valid_ref, sems,
):
    half = rows // 2
    dates = z_ref.shape[1]
    top = upper()
    odd = par_ref[0] == 1
    step = PIECE if dates % PIECE == 0 else dates
    copies = []
    for p in range(dates // step):
        part = pl.ds(p * step, step)
        copies.append(
            [
                pltpu.make_async_copy(amp_hbm.at[part], amp_ref.at[part], sems.at[0, p]),
                pltpu.make_async_copy(phase_hbm.at[part], phase_ref.at[part], sems.at[1, p]),
            ]
        )
    weights = pltpu.make_async_copy(valid_hbm, valid_ref, sems.at[2, 0])
    weights.start()
    for pair in copies:
        for copy in pair:
            copy.start()
    weights.wait()
    roots = []
    for k in range(half):
        valid = load_pair(valid_ref, (), k, rows, tiles, top)
        roots.append(jnp.where(valid == 1, 1.0, MASKED_WEIGHT**0.5).astype(jnp.float32))

    def one_date(t, carry):
        for k in range(half):
            amp = load_pair(amp_ref, (t,), k, rows, tiles, top) * roots[k]
            sin_x, cos_x = sin_cos(load_pair(phase_ref, (t,), k, rows, tiles, top))
            re, im = amp * cos_x, amp * sin_x
            z_ref[0, t, k] = re
            z_ref[1, t, k] = im
            if k >= half - HALF_ROWS:
                z_ref[0, t, 2 * half - 1 - k] = flip(re)
                z_ref[1, t, 2 * half - 1 - k] = flip(im)
            if k < HALF_ROWS:
                first, second = pack(re, im, top)
                x_ref[t, k] = jnp.where(odd, first, second)
                y_ref[t, k] = jnp.where(odd, second, first)
        return carry

    for p, pair in enumerate(copies):
        for copy in pair:
            copy.wait()
        lax.fori_loop(p * step, (p + 1) * step, one_date, 0)


def unpack(first, second, top):
    return jnp.where(top, first, flip(second)), jnp.where(top, flip(first), second)


def pack(re, im, top):
    return jnp.where(top, re, flip(im)), jnp.where(top, flip(re), im)


def add_to(total, sign, value):
    if total is None:
        return value if sign > 0 else -value
    return total + value if sign > 0 else total - value


def running(values):
    out = [values[0]]
    for value in values[1:]:
        out.append(out[-1] + value)
    return out


def inner_sums(field):
    count = len(field) - WIN_ROWS + 1
    tails = running(field[WIN_ROWS - 1 :: -1])[::-1]
    if count <= WIN_ROWS:
        core = running(field[count - 1 : WIN_ROWS])[-1]
        tails = running([core] + field[: count - 1][::-1])[::-1]
    heads = running(field[WIN_ROWS:])
    middle = [tails[q] + heads[q - 1] for q in range(1, min(count, WIN_ROWS))]
    return [tails[0]] + middle + heads[WIN_ROWS - 1 :]


def fill_band(band_ref):
    at = lax.broadcasted_iota(jnp.int32, band_ref.shape, 0) % LANES
    to = lax.broadcasted_iota(jnp.int32, band_ref.shape, 1)
    reach = WIN_COLS // 2
    inside = (to < LANES) & (jnp.abs(at - to) <= reach)
    to = to - LANES
    beside = (to >= 0) & ((at >= to + LANES - reach) | (at <= to - LANES + reach))
    band_ref[...] = jnp.where(inside | beside, 1.0, 0.0).astype(band_ref.dtype)


def put_split(ref, at, vectors):
    x = jnp.concatenate(vectors, axis=0)
    high = x.astype(jnp.bfloat16)
    low = (x - high.astype(jnp.float32)).astype(jnp.bfloat16)
    ref[at, :, :LANES] = high
    ref[at, :, LANES:] = low


def side_masks(tiles):
    column = sublane() % tiles
    at = lane()
    return (at < LANES // 2) & (column != 0), (at >= LANES // 2) & (column != tiles - 1)


def column_sums(split_ref, first, size, band, sides):
    rows = split_ref.shape[1]
    terms = split_ref[first : first + size].reshape(size * rows, 2 * LANES)
    both = jnp.dot(terms, band, preferred_element_type=jnp.float32)
    from_before, from_after = sides
    out = []
    for k in range(size * rows // SUB):
        inside = both[k * SUB : (k + 1) * SUB, :LANES]
        beside = both[k * SUB : (k + 1) * SUB, LANES:]
        before, after = pltpu.roll(beside, 1, 0), pltpu.roll(beside, SUB - 1, 0)
        out.append(
            inside + jnp.where(from_before, before, jnp.where(from_after, after, 0.0))
        )
    return out


def pair_list(dates):
    return [(i, j) for i in range(dates) for j in range(i + 1, dates)]


CHUNK = 5


def coherence(dates, vectors, fields, split_ref, band_ref, inv_ref, places, sides):
    pairs = pair_list(dates)
    band = band_ref[...]
    powers = [fields(i, i) for i in range(dates)]
    half = dates // 2
    for e in range(half):
        put_split(split_ref, e, powers[2 * e] + powers[2 * e + 1])
    sums = column_sums(split_ref, 0, half, band, sides)
    for i in range(dates):
        for k in range(vectors):
            inv_ref[i, k] = lax.rsqrt(sums[i * vectors + k]) * 0.5
    for first in range(0, len(pairs), CHUNK):
        size = min(CHUNK, len(pairs) - first)
        for e in range(first, first + size):
            re, im = fields(*pairs[e])
            put_split(split_ref, half + e, re + im)
        sums = column_sums(split_ref, half + first, size, band, sides)
        for e in range(first, first + size):
            i, j = pairs[e]
            base = (e - first) * 2 * vectors
            for k in range(vectors):
                scale = inv_ref[i, k] * inv_ref[j, k]
                nr_ref, ni_ref, at = places[k]
                nr_ref[e, at] = sums[base + k] * scale
                ni_ref[e, at] = sums[base + vectors + k] * scale


def cross(a, b):
    (ar, ai), (br, bi) = a, b
    re = [p * r + q * s for p, q, r, s in zip(ar, ai, br, bi)]
    im = [q * r - p * s for p, q, r, s in zip(ar, ai, br, bi)]
    return re, im


def power_of(a):
    return [p * p + q * q for p, q in zip(*a)]


def iterate(
    first, last, offset, dates, scalars, z_ref, nr, ni, more, sq, vec,
    link_ref, comp_ref, out_offset=0,
):
    pairs = pair_list(dates)
    index = {pair: e for e, pair in enumerate(pairs)}
    count = len(pairs)
    iter_ref, chosen_ref = scalars
    groups = []
    at = 0
    for size in (3, 3, 4) if dates == 10 else (dates,):
        groups.append(tuple(range(at, at + size)))
        at += size

    def one_vector(whole_k, carry):
        k = whole_k - offset
        place = whole_k - out_offset
        for e in range(count):
            re, im = nr[e, k], ni[e, k]
            more[e] = re + im
            more[count + e] = im - re

        def left(i, t):
            if i < t:
                e = index[i, t]
                return (nr[e, k], 1), (more[e], 1), (more[count + e], 1)
            e = index[t, i]
            return (nr[e, k], 1), (more[count + e], -1), (more[e], -1)

        def right(t, j):
            if t < j:
                e = index[t, j]
                return (nr[e, k], 1), (ni[e, k], 1), (more[e], 1)
            e = index[j, t]
            return (nr[e, k], 1), (ni[e, k], -1), (more[count + e], -1)

        def square(out):
            sums = {pair: [None, None, None] for pair in out}
            rows_in = sorted({i for i, _ in out})
            cols_in = sorted({j for _, j in out})
            for t in range(dates):
                lefts = {i: left(i, t) for i in rows_in if i != t}
                rights = {j: right(t, j) for j in cols_in if j != t}
                for i, j in out:
                    if t in (i, j):
                        continue
                    (ar, _), (ap, sap), (aq, saq) = lefts[i]
                    (br, _), (bi, sbi), (bs, sbs) = rights[j]
                    s = sums[i, j]
                    s[0] = add_to(s[0], sbs, ar * bs)
                    s[1] = add_to(s[1], saq, aq * br)
                    s[2] = add_to(s[2], sap * sbi, ap * bi)
            for i, j in out:
                e = index[i, j]
                s = sums[i, j]
                re = s[0] - s[2] + nr[e, k]
                im = s[0] + s[1] + ni[e, k]
                sq[e] = re
                sq[count + e] = re + im
                sq[2 * count + e] = im - re

        for a in range(len(groups)):
            square([(i, j) for i in groups[a] for j in groups[a] if i < j])
            for b in range(a + 1, len(groups)):
                square([(i, j) for i in groups[a] for j in groups[b]])
        size = [None] * dates
        for e, (i, j) in enumerate(pairs):
            re, im = nr[e, k], ni[e, k]
            value = re * re + im * im
            size[i] = add_to(size[i], 1, value)
            size[j] = add_to(size[j], 1, value)
        for i in range(dates):
            sq[3 * count + i] = size[i] + 0.25

        turns = jnp.minimum(iter_ref[0], ITERS)
        odd_turns = turns % 2 == 1
        steps = jnp.where(odd_turns, turns // 2, turns // 2 - 1)

        def row_sums(re_of, im_of, own):
            sr, si = [own(i) for i in range(dates)], [None] * dates
            for e, (i, j) in enumerate(pairs):
                re, im = re_of(e), im_of(e)
                sr[i] = sr[i] + re
                sr[j] = sr[j] + re
                si[i] = add_to(si[i], 1, im)
                si[j] = add_to(si[j], -1, im)
            for i in range(dates):
                vec[i] = sr[i]
                vec[dates + i] = si[i]

        @pl.when(odd_turns)
        def _():
            row_sums(lambda e: nr[e, k], lambda e: ni[e, k],
                     lambda i: jnp.full((SUB, LANES), 0.5, jnp.float32))

        @pl.when(jnp.logical_not(odd_turns))
        def _():
            row_sums(lambda e: sq[e], lambda e: sq[count + e] - sq[e],
                     lambda i: sq[3 * count + i])

        def step(_, vectors):
            vr, vi = vectors[:dates], vectors[dates:]
            vs = [a + b for a, b in zip(vr, vi)]
            out_r, out_i = [], []
            for rows_in in groups:
                sums = {i: [None, None, None] for i in rows_in}
                for i in rows_in:
                    for j in range(dates):
                        if j == i or (j in rows_in and j < i):
                            continue
                        e = index[min(i, j), max(i, j)]
                        re, plus, minus = sq[e], sq[count + e], sq[2 * count + e]
                        s = sums[i]
                        if i < j:
                            s[0] = add_to(s[0], 1, re * vs[j])
                            s[1] = add_to(s[1], 1, minus * vr[j])
                            s[2] = add_to(s[2], 1, plus * vi[j])
                            if j in rows_in:
                                s = sums[j]
                                s[0] = add_to(s[0], 1, re * vs[i])
                                s[1] = add_to(s[1], -1, plus * vr[i])
                                s[2] = add_to(s[2], -1, minus * vi[i])
                        else:
                            s[0] = add_to(s[0], 1, re * vs[j])
                            s[1] = add_to(s[1], -1, plus * vr[j])
                            s[2] = add_to(s[2], -1, minus * vi[j])
                for i in rows_in:
                    own = sq[3 * count + i]
                    s = sums[i]
                    out_r.append(s[0] - s[2] + own * vr[i])
                    out_i.append(s[0] + s[1] + own * vi[i])
            return tuple(out_r + out_i)

        vectors = lax.fori_loop(0, steps, step, tuple(vec[i] for i in range(2 * dates)))
        length = None
        for part in vectors:
            length = add_to(length, 1, part * part)
        scale = lax.rsqrt(length)
        vr = [a * scale for a in vectors[:dates]]
        vi = [a * scale for a in vectors[dates:]]
        for i in range(dates):
            vec[i] = vr[i]
            vec[dates + i] = vi[i]
        cr = ci = None
        for i in range(dates):
            zr, zi = z_ref[0, i, whole_k], z_ref[1, i, whole_k]
            cr = add_to(cr, 1, vr[i] * zr + vi[i] * zi)
            ci = add_to(ci, 1, vr[i] * zi - vi[i] * zr)
        comp_ref[0, place] = cr
        comp_ref[1, place] = ci
        ref_r = vec[chosen_ref[0]] * float(dates)
        ref_i = vec[dates + chosen_ref[0]] * float(dates)
        for i in range(dates):
            link_ref[0, i, place] = vr[i] * ref_r + vi[i] * ref_i
            link_ref[1, i, place] = vi[i] * ref_r - vr[i] * ref_i
        return carry

    lax.fori_loop(first, last, one_vector, 0)


def inner_kernel(
    tiles, done, iter_ref, chosen_ref, z_ref,
    nr_b, ni_b, nr_c, ni_c, part_ref, link_ref, comp_ref,
    band, split, inv, nr_a, ni_a, more, sq, vec,
):
    dates = z_ref.shape[1]
    places = [
        (nr, ni, k)
        for nr, ni in ((nr_a, ni_a), (nr_b, ni_b), (nr_c, ni_c))
        for k in range(nr.shape[1])
    ]
    vectors = len(places)
    ext = vectors + 2 * HALF_ROWS
    pairs = pair_list(dates)
    count = len(pairs)
    index = {pair: e for e, pair in enumerate(pairs)}
    scalars = iter_ref, chosen_ref
    fill_band(band)

    def image(t):
        return [[z_ref[part, t, k] for k in range(ext)] for part in range(2)]

    def keep(at, field):
        heads = running(field[: 2 * HALF_ROWS])
        for k in range(HALF_ROWS):
            part_ref[at, k] = heads[HALF_ROWS + k]

    def fields(i, j):
        if i == j:
            power = power_of(image(i))
            keep(2 * count + i, power)
            return inner_sums(power)
        re, im = cross(image(i), image(j))
        e = index[i, j]
        keep(e, re)
        keep(count + e, im)
        return inner_sums(re), inner_sums(im)

    coherence(dates, vectors, fields, split, band, inv, places, side_masks(tiles))
    iterate(
        HALF_ROWS, HALF_ROWS + done, HALF_ROWS, dates, scalars, z_ref, nr_a, ni_a,
        more, sq, vec, link_ref, comp_ref, HALF_ROWS,
    )


def outer_kernel(
    tiles, par_ref, iter_ref, chosen_ref, z_ref, part_ref, x_ref, y_ref,
    link_ref, comp_ref, pack_x_ref, pack_y_ref,
    halo, band, split, inv, nr, ni, more, sq, vec,
):
    dates = z_ref.shape[1]
    top = upper()
    odd_device = par_ref[0] == 1
    edge = par_ref[1] == 1
    pairs = pair_list(dates)
    count = len(pairs)
    index = {pair: e for e, pair in enumerate(pairs)}
    scalars = iter_ref, chosen_ref
    fill_band(band)

    def fill(t, carry):
        for k in range(HALF_ROWS):
            a, b = x_ref[t, k], jnp.where(edge, 0.0, y_ref[t, k])
            re, im = unpack(jnp.where(odd_device, a, b), jnp.where(odd_device, b, a), top)
            halo[0, t, k] = re
            halo[1, t, k] = im
        return carry

    lax.fori_loop(0, dates, fill, 0)

    def image(t):
        return [[halo[part, t, k] for k in range(HALF_ROWS)] for part in range(2)]

    def add(at, field):
        tails = running(field)
        return [tails[HALF_ROWS - 1 - k] + part_ref[at, k] for k in range(HALF_ROWS)]

    def fields(i, j):
        if i == j:
            return add(2 * count + i, power_of(image(i)))
        re, im = cross(image(i), image(j))
        e = index[i, j]
        return add(e, re), add(count + e, im)

    places = [(nr, ni, k) for k in range(HALF_ROWS)]
    coherence(dates, HALF_ROWS, fields, split, band, inv, places, side_masks(tiles))
    iterate(
        0, HALF_ROWS, 0, dates, scalars, z_ref, nr, ni, more, sq, vec,
        link_ref, comp_ref,
    )
    for k in range(HALF_ROWS):
        first, second = pack(comp_ref[0, k], comp_ref[1, k], top)
        pack_x_ref[k] = jnp.where(odd_device, first, second)
        pack_y_ref[k] = jnp.where(odd_device, second, first)


def rest_kernel(
    start, iter_ref, chosen_ref, z_ref, nr, ni, after_ref, link_ref, comp_ref,
    more, sq, vec,
):
    dates = z_ref.shape[1]
    scalars = iter_ref, chosen_ref
    iterate(
        start, start + comp_ref.shape[1], start, dates, scalars, z_ref, nr, ni,
        more, sq, vec, link_ref, comp_ref, start,
    )


def box_sum(field, lanes, edges):
    last_two, last_one, first_one, first_two = lanes
    keep_before, keep_after = edges
    out = []
    for x in inner_sums(field):
        before = jnp.where(keep_before, pltpu.roll(x, 1, 0), 0.0)
        after = jnp.where(keep_after, pltpu.roll(x, SUB - 1, 0), 0.0)
        near = pltpu.roll(jnp.where(last_one, before, x), 1, 1) + pltpu.roll(
            jnp.where(first_one, after, x), LANES - 1, 1
        )
        far = pltpu.roll(jnp.where(last_two, before, x), 2, 1) + pltpu.roll(
            jnp.where(first_two, after, x), LANES - 2, 1
        )
        out.append(x + near + far)
    return out


def masks(tiles):
    at = lane()
    lanes = (at >= LANES - 2, at >= LANES - 1, at < 1, at < 2)
    column = sublane() % tiles
    return lanes, (column != 0, column != tiles - 1)


def extend_kernel(par_ref, outer_ref, inner_ref, x_ref, y_ref, out_ref):
    top = upper()
    odd_device = par_ref[0] == 1
    edge = par_ref[1] == 1
    for k in range(HALF_ROWS):
        a, b = x_ref[k], jnp.where(edge, 0.0, y_ref[k])
        re, im = unpack(jnp.where(odd_device, a, b), jnp.where(odd_device, b, a), top)
        out_ref[0, HALF_ROWS - 1 - k] = re
        out_ref[1, HALF_ROWS - 1 - k] = im
    for part in range(2):
        at = HALF_ROWS
        for ref in (outer_ref, inner_ref):
            for k in range(ref.shape[1]):
                out_ref[part, at] = ref[part, k]
                at += 1


def gather_kernel(first_ref, second_ref, out_ref):
    for part in range(2):
        at = 0
        for ref in (first_ref, second_ref):
            for k in range(ref.shape[1]):
                out_ref[part, at] = ref[part, k]
                at += 1


def offsets_kernel(
    tiles, place_ref, own_w, own_n, a_w, a_n, b_w, b_n, unit_ref, total_ref
):
    lanes, edges = masks(tiles)
    half = unit_ref.shape[1]
    odd_stack = place_ref[1] == 1
    first_stack = place_ref[0] == 0

    def whole(*refs):
        parts = []
        for part in range(2):
            rows_in = [ref[part, k] for ref in refs for k in range(ref.shape[1])]
            rows_in += [flip(rows_in[-1 - k]) for k in range(HALF_ROWS)]
            parts.append(rows_in)
        return parts

    def power(re, im):
        return box_sum([a * a + b * b for a, b in zip(re, im)], lanes, edges)

    own_r, own_i = whole(own_w, own_n)
    own = [p + 1.0 for p in power(own_r, own_i)]

    def unit(*refs):
        re, im = whole(*refs)
        other = power(re, im)
        cross_r = box_sum(
            [a * c + b * d for a, b, c, d in zip(own_r, own_i, re, im)], lanes, edges
        )
        cross_i = box_sum(
            [b * c - a * d for a, b, c, d in zip(own_r, own_i, re, im)], lanes, edges
        )
        out = []
        for k in range(half):
            scale = lax.rsqrt(own[k] * (other[k] + 1.0))
            off_r, off_i = cross_r[k] * scale, cross_i[k] * scale
            bound = jnp.maximum(jnp.sqrt(off_r * off_r + off_i * off_i), LINK_FLOOR)
            back = 1.0 / bound
            out.append((off_r * back, off_i * back))
        return out

    pair_a, pair_b = unit(a_w, a_n), unit(b_w, b_n)
    for k in range(half):
        (ar, ai), (br, bi) = pair_a[k], pair_b[k]
        before_r = jnp.where(odd_stack, ar, br)
        before_i = -jnp.where(odd_stack, ai, bi)
        after_r = jnp.where(odd_stack, br, ar)
        after_i = jnp.where(odd_stack, bi, ai)
        before_r = jnp.where(first_stack, 1.0, before_r)
        before_i = jnp.where(first_stack, 0.0, before_i)
        unit_ref[0, k] = before_r
        unit_ref[1, k] = before_i
        total_ref[0, k] = before_r * after_r - before_i * after_i
        total_ref[1, k] = before_r * after_i + before_i * after_r


def result_kernel(rows, tiles, outer_ref, inner_ref, middle_ref, last_ref, datum_ref, out_ref):
    half = rows // 2
    parts = (outer_ref, inner_ref, middle_ref, last_ref)
    links = [(ref, k) for ref in parts for k in range(ref.shape[2])]

    def one_date(t, carry):
        for k in range(half):
            ref, at = links[k]
            lr, li = ref[0, t, at], ref[1, t, at]
            dr, di = datum_ref[0, k], datum_ref[1, k]
            first, second = bases(k, rows, tiles)
            for part, value in enumerate((lr * dr - li * di, lr * di + li * dr)):
                out_ref[part, t, pl.ds(first, tiles, stride=SUB), :] = value[:tiles]
                out_ref[part, t, pl.ds(second, tiles, stride=SUB), :] = value[tiles:]
        return carry

    lax.fori_loop(0, outer_ref.shape[1], one_date, 0)


def swaps(count, bit=None, odd=False):
    if bit is not None:
        return [(i, i ^ bit) for i in range(count)]
    if odd:
        return [(i, (i + 1 if i % 2 else i - 1) % count) for i in range(count)]
    return [(i, i ^ 1) for i in range(count)]


def times(a, b):
    return jnp.stack([a[0] * b[0] - a[1] * b[1], a[0] * b[1] + a[1] * b[0]])


def linked_phases(amplitude, phase, validity, iterations, reference_date):
    dates, rows, columns = amplitude.shape
    half = rows // 2
    tiles = columns // LANES
    ext = half + HALF_ROWS
    members = lax.axis_size("tm")
    blocks = lax.axis_size("space")
    place = lax.axis_index("tm")
    block = lax.axis_index("space")
    edge = (block == 0) | (block == blocks - 1)
    parity = jnp.stack([block % 2, edge.astype(jnp.int32)])
    params = pltpu.CompilerParams(vmem_limit_bytes=VMEM_LIMIT)

    def shape(*dims):
        return jax.ShapeDtypeStruct(dims, jnp.float32)

    def tiled(x):
        lead = x.shape[:-2]
        x = x.reshape(lead + (rows // SUB, SUB, tiles, LANES))
        return jnp.swapaxes(x, -3, -2).reshape(lead + (rows * tiles, LANES))

    def far_memory(x):
        return pltpu.with_memory_space_constraint(x, pltpu.MemorySpace.HBM)

    z, slab_x, slab_y = pl.pallas_call(
        lambda *refs: images_kernel(rows, tiles, *refs),
        out_shape=(
            shape(2, dates, ext, SUB, LANES),
            shape(dates, HALF_ROWS, SUB, LANES),
            shape(dates, HALF_ROWS, SUB, LANES),
        ),
        in_specs=[smem(), hbm(), hbm(), hbm()],
        out_specs=(vmem(), vmem(), vmem()),
        scratch_shapes=[
            pltpu.VMEM((dates, rows * tiles, LANES), jnp.float32),
            pltpu.VMEM((dates, rows * tiles, LANES), jnp.float32),
            pltpu.VMEM((rows * tiles, LANES), jnp.int32),
            pltpu.SemaphoreType.DMA((3, dates)),
        ],
        compiler_params=params,
        name="images",
    )(parity, *(far_memory(tiled(x)) for x in (amplitude, phase, validity)))
    pair_x, pair_y = swaps(blocks), swaps(blocks, odd=True)
    got_y = lax.ppermute(slab_y, "space", pair_y)
    got_x = lax.ppermute(slab_x, "space", pair_x)

    count = dates * (dates - 1) // 2
    inner = half - HALF_ROWS
    done = min(INNER_DONE, inner - 1)
    work = [
        pltpu.VMEM((2 * count, SUB, LANES), jnp.float32),
        pltpu.VMEM((3 * count + dates, SUB, LANES), jnp.float32),
        pltpu.VMEM((2 * dates, SUB, LANES), jnp.float32),
    ]

    def window_work(vectors):
        return [
            pltpu.VMEM((2 * LANES, 2 * LANES), jnp.bfloat16),
            pltpu.VMEM((dates // 2 + count, 2 * vectors * SUB, 2 * LANES), jnp.bfloat16),
            pltpu.VMEM((dates, vectors, SUB, LANES), jnp.float32),
        ]

    def cost(vectors):
        return pl.CostEstimate(
            flops=vectors * 2_000_000 * 8, bytes_accessed=1 << 20, transcendentals=0
        )

    middle = min(MIDDLE, inner - done - 1)
    last = inner - done - middle
    nr_b, ni_b, nr_c, ni_c, part, linked_a, comp_a = pl.pallas_call(
        lambda *refs: inner_kernel(tiles, done, *refs),
        out_shape=(
            shape(count, middle, SUB, LANES),
            shape(count, middle, SUB, LANES),
            shape(count, last, SUB, LANES),
            shape(count, last, SUB, LANES),
            shape(2 * count + dates, HALF_ROWS, SUB, LANES),
            shape(2, dates, done, SUB, LANES),
            shape(2, done, SUB, LANES),
        ),
        in_specs=[smem(), smem(), vmem()],
        out_specs=(vmem(),) * 7,
        scratch_shapes=window_work(inner)
        + [pltpu.VMEM((count, done, SUB, LANES), jnp.float32)] * 2
        + work,
        compiler_params=params,
        cost_estimate=cost(4),
        name="inner",
    )(iterations, reference_date, z)
    linked_b, comp_b, pack_x, pack_y = pl.pallas_call(
        lambda *refs: outer_kernel(tiles, *refs),
        out_shape=(
            shape(2, dates, HALF_ROWS, SUB, LANES),
            shape(2, HALF_ROWS, SUB, LANES),
            shape(HALF_ROWS, SUB, LANES),
            shape(HALF_ROWS, SUB, LANES),
        ),
        in_specs=[smem()] * 3 + [vmem()] * 4,
        out_specs=(vmem(),) * 4,
        scratch_shapes=[pltpu.VMEM((2, dates, HALF_ROWS, SUB, LANES), jnp.float32)]
        + window_work(HALF_ROWS)
        + [
            pltpu.VMEM((count, HALF_ROWS, SUB, LANES), jnp.float32),
            pltpu.VMEM((count, HALF_ROWS, SUB, LANES), jnp.float32),
        ]
        + work,
        compiler_params=params,
        cost_estimate=cost(7),
        name="outer",
    )(parity, iterations, reference_date, z, part, got_x, got_y)
    more_y = lax.ppermute(pack_y, "space", pair_y)
    more_x = lax.ppermute(pack_x, "space", pair_x)

    def rest(start, nr, ni, after):
        vectors = nr.shape[1]

        return pl.pallas_call(
            lambda *refs: rest_kernel(start, *refs),
            out_shape=(
                shape(2, dates, vectors, SUB, LANES),
                shape(2, vectors, SUB, LANES),
            ),
            in_specs=[smem()] * 2 + [vmem()] * 4,
            out_specs=(vmem(),) * 2,
            scratch_shapes=work,
            compiler_params=params,
            cost_estimate=cost(vectors),
            name="rest",
        )(iterations, reference_date, z, nr, ni, after)

    start = HALF_ROWS + done
    linked_c, comp_c = rest(start, nr_b, ni_b, pack_x)
    start += middle
    wide = pl.pallas_call(
        extend_kernel,
        out_shape=shape(2, 2 * HALF_ROWS + done, SUB, LANES),
        in_specs=[smem()] + [vmem()] * 4,
        out_specs=vmem(),
        compiler_params=params,
        name="extend",
    )(parity, comp_b, comp_a, more_x, more_y)
    near, far = swaps(members), swaps(members, odd=True)
    wide_b = lax.ppermute(wide, "tm", far)
    wide_a = lax.ppermute(wide, "tm", near)
    linked_d, comp_d = rest(start, nr_c, ni_c, wide)
    narrow = pl.pallas_call(
        gather_kernel,
        out_shape=shape(2, half - HALF_ROWS - done, SUB, LANES),
        in_specs=[vmem()] * 2,
        out_specs=vmem(),
        compiler_params=params,
        name="gather",
    )(comp_c, comp_d)
    narrow_b = lax.ppermute(narrow, "tm", far)
    narrow_a = lax.ppermute(narrow, "tm", near)
    where = jnp.stack([place, place % 2]).astype(jnp.int32)
    datum, total = pl.pallas_call(
        lambda *refs: offsets_kernel(tiles, *refs),
        out_shape=(shape(2, half, SUB, LANES), shape(2, half, SUB, LANES)),
        in_specs=[smem()] + [vmem()] * 6,
        out_specs=(vmem(), vmem()),
        compiler_params=params,
        name="offsets",
    )(where, wide, narrow, wide_a, narrow_a, wide_b, narrow_b)
    bit = 2
    while bit < members:
        other = lax.ppermute(total, "tm", swaps(members, bit=2 * bit - 2))
        datum = jnp.where((place & bit) != 0, times(datum, other), datum)
        total = times(total, other)
        bit *= 2
    out = pl.pallas_call(
        lambda *refs: result_kernel(rows, tiles, *refs),
        out_shape=shape(2, dates, rows * tiles, LANES),
        in_specs=[vmem()] * 5,
        out_specs=vmem(),
        compiler_params=params,
        name="result",
    )(linked_b, linked_a, linked_c, linked_d, datum)
    out = out.reshape(2, dates, rows // SUB, tiles, SUB, LANES)
    return jnp.swapaxes(out, -3, -2).reshape(2, dates, rows, columns)


def solution(mesh):
    return jax.shard_map(
        linked_phases,
        mesh=mesh,
        in_specs=(
            P("tm", "space", None),
            P("tm", "space", None),
            P("space", None),
            P("tm"),
            P("tm"),
        ),
        out_specs=P(None, "tm", "space", None),
        check_vma=False,
    )
```

```python
import jax
import jax.numpy as jnp
from jax import lax
from jax.experimental import pallas as pl
from jax.experimental.pallas import tpu as pltpu
from jax.sharding import PartitionSpec as P

WIN_ROWS = 11
WIN_COLS = 5
INNER_DONE = 2
PIECE = 5
ITERS = 20
HALF_ROWS = WIN_ROWS // 2

MASKED_WEIGHT = 0.125
LINK_FLOOR = 0.03

LANES = 128
SUB = 8
VMEM_LIMIT = 40 * 1024 * 1024


def vmem():
    return pl.BlockSpec(memory_space=pltpu.VMEM)


def hbm():
    return pl.BlockSpec(memory_space=pltpu.MemorySpace.HBM)


def smem():
    return pl.BlockSpec(memory_space=pltpu.SMEM)


def sublane():
    return lax.broadcasted_iota(jnp.int32, (SUB, LANES), 0)


def lane():
    return lax.broadcasted_iota(jnp.int32, (SUB, LANES), 1)


def flip(x):
    return pltpu.roll(x, SUB // 2, 0)


def upper():
    return sublane() < SUB // 2


def bases(k, rows, tiles):
    def base(row):
        return (row // SUB) * SUB * tiles + row % SUB

    return base(k), base(rows - 1 - k)


def load_pair(ref, lead, k, rows, tiles, top):
    first, second = bases(k, rows, tiles)
    a = ref[lead + (pl.ds(first, SUB, stride=SUB), slice(None))]
    b = ref[lead + (pl.ds(second - SUB * tiles, SUB, stride=SUB), slice(None))]
    return jnp.where(top, a, b)


def sin_cos(x):
    turns = jnp.round(x * (2.0 / jnp.pi))
    r = (x - turns * 1.5707855224609375) - turns * 1.0804334124e-05
    s = r * r
    sine = r + r * s * (-1.6666654611e-1 + s * (8.3321608736e-3 + s * -1.9515295891e-4))
    cosine = 1.0 - 0.5 * s + s * s * (
        4.166664568298827e-2 + s * (-1.388731625493765e-3 + s * 2.443315711809948e-5)
    )
    size = jnp.abs(turns)
    odd = size == 1.0
    base_s = jnp.where(odd, cosine, sine)
    base_c = jnp.where(odd, sine, cosine)
    sin_x = jnp.where((turns == -1.0) | (size == 2.0), -base_s, base_s)
    cos_x = jnp.where((turns == 1.0) | (size == 2.0), -base_c, base_c)
    return sin_x, cos_x


def images_kernel(
    rows, tiles, par_ref, amp_hbm, phase_hbm, valid_hbm, z_ref, x_ref, y_ref,
    amp_ref, phase_ref, valid_ref, sems,
):
    half = rows // 2
    dates = z_ref.shape[1]
    top = upper()
    odd = par_ref[0] == 1
    step = PIECE if dates % PIECE == 0 else dates
    copies = []
    for p in range(dates // step):
        part = pl.ds(p * step, step)
        copies.append(
            [
                pltpu.make_async_copy(amp_hbm.at[part], amp_ref.at[part], sems.at[0, p]),
                pltpu.make_async_copy(phase_hbm.at[part], phase_ref.at[part], sems.at[1, p]),
            ]
        )
    weights = pltpu.make_async_copy(valid_hbm, valid_ref, sems.at[2, 0])
    weights.start()
    for pair in copies:
        for copy in pair:
            copy.start()
    weights.wait()
    roots = []
    for k in range(half):
        valid = load_pair(valid_ref, (), k, rows, tiles, top)
        roots.append(jnp.where(valid == 1, 1.0, MASKED_WEIGHT**0.5).astype(jnp.float32))

    def one_date(t, carry):
        for k in range(half):
            amp = load_pair(amp_ref, (t,), k, rows, tiles, top) * roots[k]
            sin_x, cos_x = sin_cos(load_pair(phase_ref, (t,), k, rows, tiles, top))
            re, im = amp * cos_x, amp * sin_x
            z_ref[0, t, k] = re
            z_ref[1, t, k] = im
            if k >= half - HALF_ROWS:
                z_ref[0, t, 2 * half - 1 - k] = flip(re)
                z_ref[1, t, 2 * half - 1 - k] = flip(im)
            if k < HALF_ROWS:
                first, second = pack(re, im, top)
                x_ref[t, k] = jnp.where(odd, first, second)
                y_ref[t, k] = jnp.where(odd, second, first)
        return carry

    for p, pair in enumerate(copies):
        for copy in pair:
            copy.wait()
        lax.fori_loop(p * step, (p + 1) * step, one_date, 0)


def unpack(first, second, top):
    return jnp.where(top, first, flip(second)), jnp.where(top, flip(first), second)


def pack(re, im, top):
    return jnp.where(top, re, flip(im)), jnp.where(top, flip(re), im)


def add_to(total, sign, value):
    if total is None:
        return value if sign > 0 else -value
    return total + value if sign > 0 else total - value


def running(values):
    out = [values[0]]
    for value in values[1:]:
        out.append(out[-1] + value)
    return out


def inner_sums(field):
    count = len(field) - WIN_ROWS + 1
    tails = running(field[WIN_ROWS - 1 :: -1])[::-1]
    if count <= WIN_ROWS:
        core = running(field[count - 1 : WIN_ROWS])[-1]
        tails = running([core] + field[: count - 1][::-1])[::-1]
    heads = running(field[WIN_ROWS:])
    middle = [tails[q] + heads[q - 1] for q in range(1, min(count, WIN_ROWS))]
    return [tails[0]] + middle + heads[WIN_ROWS - 1 :]


def fill_band(band_ref):
    at = lax.broadcasted_iota(jnp.int32, band_ref.shape, 0) % LANES
    to = lax.broadcasted_iota(jnp.int32, band_ref.shape, 1)
    reach = WIN_COLS // 2
    inside = (to < LANES) & (jnp.abs(at - to) <= reach)
    to = to - LANES
    beside = (to >= 0) & ((at >= to + LANES - reach) | (at <= to - LANES + reach))
    band_ref[...] = jnp.where(inside | beside, 1.0, 0.0).astype(band_ref.dtype)


def put_split(ref, at, vectors):
    x = jnp.concatenate(vectors, axis=0)
    high = x.astype(jnp.bfloat16)
    low = (x - high.astype(jnp.float32)).astype(jnp.bfloat16)
    ref[at, :, :LANES] = high
    ref[at, :, LANES:] = low


def side_masks(tiles):
    column = sublane() % tiles
    at = lane()
    return (at < LANES // 2) & (column != 0), (at >= LANES // 2) & (column != tiles - 1)


def column_sums(split_ref, first, size, band, sides):
    rows = split_ref.shape[1]
    terms = split_ref[first : first + size].reshape(size * rows, 2 * LANES)
    both = jnp.dot(terms, band, preferred_element_type=jnp.float32)
    from_before, from_after = sides
    out = []
    for k in range(size * rows // SUB):
        inside = both[k * SUB : (k + 1) * SUB, :LANES]
        beside = both[k * SUB : (k + 1) * SUB, LANES:]
        before, after = pltpu.roll(beside, 1, 0), pltpu.roll(beside, SUB - 1, 0)
        out.append(
            inside + jnp.where(from_before, before, jnp.where(from_after, after, 0.0))
        )
    return out


def pair_list(dates):
    return [(i, j) for i in range(dates) for j in range(i + 1, dates)]


CHUNK = 5


def coherence(dates, vectors, fields, split_ref, band_ref, inv_ref, places, sides):
    pairs = pair_list(dates)
    band = band_ref[...]
    powers = [fields(i, i) for i in range(dates)]
    half = dates // 2
    for e in range(half):
        put_split(split_ref, e, powers[2 * e] + powers[2 * e + 1])
    sums = column_sums(split_ref, 0, half, band, sides)
    for i in range(dates):
        for k in range(vectors):
            inv_ref[i, k] = lax.rsqrt(sums[i * vectors + k]) * 0.5
    for first in range(0, len(pairs), CHUNK):
        size = min(CHUNK, len(pairs) - first)
        for e in range(first, first + size):
            re, im = fields(*pairs[e])
            put_split(split_ref, half + e, re + im)
        sums = column_sums(split_ref, half + first, size, band, sides)
        for e in range(first, first + size):
            i, j = pairs[e]
            base = (e - first) * 2 * vectors
            for k in range(vectors):
                scale = inv_ref[i, k] * inv_ref[j, k]
                nr_ref, ni_ref, at = places[k]
                nr_ref[e, at] = sums[base + k] * scale
                ni_ref[e, at] = sums[base + vectors + k] * scale


def cross(a, b):
    (ar, ai), (br, bi) = a, b
    re = [p * r + q * s for p, q, r, s in zip(ar, ai, br, bi)]
    im = [q * r - p * s for p, q, r, s in zip(ar, ai, br, bi)]
    return re, im


def power_of(a):
    return [p * p + q * q for p, q in zip(*a)]


def iterate(
    first, last, offset, dates, scalars, z_ref, nr, ni, more, sq, vec,
    link_ref, comp_ref, out_offset=0,
):
    pairs = pair_list(dates)
    index = {pair: e for e, pair in enumerate(pairs)}
    count = len(pairs)
    iter_ref, chosen_ref = scalars
    groups = []
    at = 0
    for size in (3, 3, 4) if dates == 10 else (dates,):
        groups.append(tuple(range(at, at + size)))
        at += size

    def one_vector(whole_k, carry):
        k = whole_k - offset
        place = whole_k - out_offset
        for e in range(count):
            re, im = nr[e, k], ni[e, k]
            more[e] = re + im
            more[count + e] = im - re

        def left(i, t):
            if i < t:
                e = index[i, t]
                return (nr[e, k], 1), (more[e], 1), (more[count + e], 1)
            e = index[t, i]
            return (nr[e, k], 1), (more[count + e], -1), (more[e], -1)

        def right(t, j):
            if t < j:
                e = index[t, j]
                return (nr[e, k], 1), (ni[e, k], 1), (more[e], 1)
            e = index[j, t]
            return (nr[e, k], 1), (ni[e, k], -1), (more[count + e], -1)

        def square(out):
            sums = {pair: [None, None, None] for pair in out}
            rows_in = sorted({i for i, _ in out})
            cols_in = sorted({j for _, j in out})
            for t in range(dates):
                lefts = {i: left(i, t) for i in rows_in if i != t}
                rights = {j: right(t, j) for j in cols_in if j != t}
                for i, j in out:
                    if t in (i, j):
                        continue
                    (ar, _), (ap, sap), (aq, saq) = lefts[i]
                    (br, _), (bi, sbi), (bs, sbs) = rights[j]
                    s = sums[i, j]
                    s[0] = add_to(s[0], sbs, ar * bs)
                    s[1] = add_to(s[1], saq, aq * br)
                    s[2] = add_to(s[2], sap * sbi, ap * bi)
            for i, j in out:
                e = index[i, j]
                s = sums[i, j]
                re = s[0] - s[2] + nr[e, k]
                im = s[0] + s[1] + ni[e, k]
                sq[e] = re
                sq[count + e] = re + im
                sq[2 * count + e] = im - re

        for a in range(len(groups)):
            square([(i, j) for i in groups[a] for j in groups[a] if i < j])
            for b in range(a + 1, len(groups)):
                square([(i, j) for i in groups[a] for j in groups[b]])
        size = [None] * dates
        for e, (i, j) in enumerate(pairs):
            re, im = nr[e, k], ni[e, k]
            value = re * re + im * im
            size[i] = add_to(size[i], 1, value)
            size[j] = add_to(size[j], 1, value)
        for i in range(dates):
            sq[3 * count + i] = size[i] + 0.25

        turns = jnp.minimum(iter_ref[0], ITERS)
        odd_turns = turns % 2 == 1
        steps = jnp.where(odd_turns, turns // 2, turns // 2 - 1)

        def row_sums(re_of, im_of, own):
            sr, si = [own(i) for i in range(dates)], [None] * dates
            for e, (i, j) in enumerate(pairs):
                re, im = re_of(e), im_of(e)
                sr[i] = sr[i] + re
                sr[j] = sr[j] + re
                si[i] = add_to(si[i], 1, im)
                si[j] = add_to(si[j], -1, im)
            for i in range(dates):
                vec[i] = sr[i]
                vec[dates + i] = si[i]

        @pl.when(odd_turns)
        def _():
            row_sums(lambda e: nr[e, k], lambda e: ni[e, k],
                     lambda i: jnp.full((SUB, LANES), 0.5, jnp.float32))

        @pl.when(jnp.logical_not(odd_turns))
        def _():
            row_sums(lambda e: sq[e], lambda e: sq[count + e] - sq[e],
                     lambda i: sq[3 * count + i])

        def step(_, vectors):
            vr, vi = vectors[:dates], vectors[dates:]
            vs = [a + b for a, b in zip(vr, vi)]
            out_r, out_i = [], []
            for rows_in in groups:
                sums = {i: [None, None, None] for i in rows_in}
                for i in rows_in:
                    for j in range(dates):
                        if j == i or (j in rows_in and j < i):
                            continue
                        e = index[min(i, j), max(i, j)]
                        re, plus, minus = sq[e], sq[count + e], sq[2 * count + e]
                        s = sums[i]
                        if i < j:
                            s[0] = add_to(s[0], 1, re * vs[j])
                            s[1] = add_to(s[1], 1, minus * vr[j])
                            s[2] = add_to(s[2], 1, plus * vi[j])
                            if j in rows_in:
                                s = sums[j]
                                s[0] = add_to(s[0], 1, re * vs[i])
                                s[1] = add_to(s[1], -1, plus * vr[i])
                                s[2] = add_to(s[2], -1, minus * vi[i])
                        else:
                            s[0] = add_to(s[0], 1, re * vs[j])
                            s[1] = add_to(s[1], -1, plus * vr[j])
                            s[2] = add_to(s[2], -1, minus * vi[j])
                for i in rows_in:
                    own = sq[3 * count + i]
                    s = sums[i]
                    out_r.append(s[0] - s[2] + own * vr[i])
                    out_i.append(s[0] + s[1] + own * vi[i])
            return tuple(out_r + out_i)

        vectors = lax.fori_loop(0, steps, step, tuple(vec[i] for i in range(2 * dates)))
        length = None
        for part in vectors:
            length = add_to(length, 1, part * part)
        scale = lax.rsqrt(length)
        vr = [a * scale for a in vectors[:dates]]
        vi = [a * scale for a in vectors[dates:]]
        for i in range(dates):
            vec[i] = vr[i]
            vec[dates + i] = vi[i]
        cr = ci = None
        for i in range(dates):
            zr, zi = z_ref[0, i, whole_k], z_ref[1, i, whole_k]
            cr = add_to(cr, 1, vr[i] * zr + vi[i] * zi)
            ci = add_to(ci, 1, vr[i] * zi - vi[i] * zr)
        comp_ref[0, place] = cr
        comp_ref[1, place] = ci
        ref_r = vec[chosen_ref[0]] * float(dates)
        ref_i = vec[dates + chosen_ref[0]] * float(dates)
        for i in range(dates):
            link_ref[0, i, place] = vr[i] * ref_r + vi[i] * ref_i
            link_ref[1, i, place] = vi[i] * ref_r - vr[i] * ref_i
        return carry

    lax.fori_loop(first, last, one_vector, 0)


def inner_kernel(
    tiles, done, iter_ref, chosen_ref, z_ref,
    nr_b, ni_b, part_ref, link_ref, comp_ref,
    band, split, inv, nr_a, ni_a, more, sq, vec,
):
    dates = z_ref.shape[1]
    places = [
        (nr, ni, k)
        for nr, ni in ((nr_a, ni_a), (nr_b, ni_b))
        for k in range(nr.shape[1])
    ]
    vectors = len(places)
    ext = vectors + 2 * HALF_ROWS
    pairs = pair_list(dates)
    count = len(pairs)
    index = {pair: e for e, pair in enumerate(pairs)}
    scalars = iter_ref, chosen_ref
    fill_band(band)

    def image(t):
        return [[z_ref[part, t, k] for k in range(ext)] for part in range(2)]

    def keep(at, field):
        heads = running(field[: 2 * HALF_ROWS])
        for k in range(HALF_ROWS):
            part_ref[at, k] = heads[HALF_ROWS + k]

    def fields(i, j):
        if i == j:
            power = power_of(image(i))
            keep(2 * count + i, power)
            return inner_sums(power)
        re, im = cross(image(i), image(j))
        e = index[i, j]
        keep(e, re)
        keep(count + e, im)
        return inner_sums(re), inner_sums(im)

    coherence(dates, vectors, fields, split, band, inv, places, side_masks(tiles))
    iterate(
        HALF_ROWS, HALF_ROWS + done, HALF_ROWS, dates, scalars, z_ref, nr_a, ni_a,
        more, sq, vec, link_ref, comp_ref, HALF_ROWS,
    )


def outer_kernel(
    tiles, par_ref, iter_ref, chosen_ref, z_ref, part_ref, x_ref, y_ref,
    link_ref, comp_ref, pack_x_ref, pack_y_ref,
    halo, band, split, inv, nr, ni, more, sq, vec,
):
    dates = z_ref.shape[1]
    top = upper()
    odd_device = par_ref[0] == 1
    edge = par_ref[1] == 1
    pairs = pair_list(dates)
    count = len(pairs)
    index = {pair: e for e, pair in enumerate(pairs)}
    scalars = iter_ref, chosen_ref
    fill_band(band)

    def fill(t, carry):
        for k in range(HALF_ROWS):
            a, b = x_ref[t, k], jnp.where(edge, 0.0, y_ref[t, k])
            re, im = unpack(jnp.where(odd_device, a, b), jnp.where(odd_device, b, a), top)
            halo[0, t, k] = re
            halo[1, t, k] = im
        return carry

    lax.fori_loop(0, dates, fill, 0)

    def image(t):
        return [[halo[part, t, k] for k in range(HALF_ROWS)] for part in range(2)]

    def add(at, field):
        tails = running(field)
        return [tails[HALF_ROWS - 1 - k] + part_ref[at, k] for k in range(HALF_ROWS)]

    def fields(i, j):
        if i == j:
            return add(2 * count + i, power_of(image(i)))
        re, im = cross(image(i), image(j))
        e = index[i, j]
        return add(e, re), add(count + e, im)

    places = [(nr, ni, k) for k in range(HALF_ROWS)]
    coherence(dates, HALF_ROWS, fields, split, band, inv, places, side_masks(tiles))
    iterate(
        0, HALF_ROWS, 0, dates, scalars, z_ref, nr, ni, more, sq, vec,
        link_ref, comp_ref,
    )
    for k in range(HALF_ROWS):
        first, second = pack(comp_ref[0, k], comp_ref[1, k], top)
        pack_x_ref[k] = jnp.where(odd_device, first, second)
        pack_y_ref[k] = jnp.where(odd_device, second, first)


def rest_kernel(
    start, iter_ref, chosen_ref, z_ref, nr, ni, after_ref, link_ref, comp_ref,
    more, sq, vec,
):
    dates = z_ref.shape[1]
    scalars = iter_ref, chosen_ref
    iterate(
        start, start + comp_ref.shape[1], start, dates, scalars, z_ref, nr, ni,
        more, sq, vec, link_ref, comp_ref, start,
    )


def box_sum(field, lanes, edges):
    last_two, last_one, first_one, first_two = lanes
    keep_before, keep_after = edges
    out = []
    for x in inner_sums(field):
        before = jnp.where(keep_before, pltpu.roll(x, 1, 0), 0.0)
        after = jnp.where(keep_after, pltpu.roll(x, SUB - 1, 0), 0.0)
        near = pltpu.roll(jnp.where(last_one, before, x), 1, 1) + pltpu.roll(
            jnp.where(first_one, after, x), LANES - 1, 1
        )
        far = pltpu.roll(jnp.where(last_two, before, x), 2, 1) + pltpu.roll(
            jnp.where(first_two, after, x), LANES - 2, 1
        )
        out.append(x + near + far)
    return out


def masks(tiles):
    at = lane()
    lanes = (at >= LANES - 2, at >= LANES - 1, at < 1, at < 2)
    column = sublane() % tiles
    return lanes, (column != 0, column != tiles - 1)


def extend_kernel(par_ref, outer_ref, inner_ref, rest_ref, x_ref, y_ref, out_ref):
    top = upper()
    odd_device = par_ref[0] == 1
    edge = par_ref[1] == 1
    for k in range(HALF_ROWS):
        a, b = x_ref[k], jnp.where(edge, 0.0, y_ref[k])
        re, im = unpack(jnp.where(odd_device, a, b), jnp.where(odd_device, b, a), top)
        out_ref[0, HALF_ROWS - 1 - k] = re
        out_ref[1, HALF_ROWS - 1 - k] = im
    for part in range(2):
        at = HALF_ROWS
        for ref in (outer_ref, inner_ref, rest_ref):
            for k in range(ref.shape[1]):
                out_ref[part, at] = ref[part, k]
                at += 1


def offsets_kernel(
    tiles, place_ref, own_ref, a_ref, b_ref, unit_ref, total_ref
):
    lanes, edges = masks(tiles)
    half = unit_ref.shape[1]
    odd_stack = place_ref[1] == 1
    first_stack = place_ref[0] == 0

    def whole(*refs):
        parts = []
        for part in range(2):
            rows_in = [ref[part, k] for ref in refs for k in range(ref.shape[1])]
            rows_in += [flip(rows_in[-1 - k]) for k in range(HALF_ROWS)]
            parts.append(rows_in)
        return parts

    def power(re, im):
        return box_sum([a * a + b * b for a, b in zip(re, im)], lanes, edges)

    own_r, own_i = whole(own_ref)
    own = [p + 1.0 for p in power(own_r, own_i)]

    def unit(*refs):
        re, im = whole(*refs)
        other = power(re, im)
        cross_r = box_sum(
            [a * c + b * d for a, b, c, d in zip(own_r, own_i, re, im)], lanes, edges
        )
        cross_i = box_sum(
            [b * c - a * d for a, b, c, d in zip(own_r, own_i, re, im)], lanes, edges
        )
        out = []
        for k in range(half):
            scale = lax.rsqrt(own[k] * (other[k] + 1.0))
            off_r, off_i = cross_r[k] * scale, cross_i[k] * scale
            bound = jnp.maximum(jnp.sqrt(off_r * off_r + off_i * off_i), LINK_FLOOR)
            back = 1.0 / bound
            out.append((off_r * back, off_i * back))
        return out

    pair_a, pair_b = unit(a_ref), unit(b_ref)
    for k in range(half):
        (ar, ai), (br, bi) = pair_a[k], pair_b[k]
        before_r = jnp.where(odd_stack, ar, br)
        before_i = -jnp.where(odd_stack, ai, bi)
        after_r = jnp.where(odd_stack, br, ar)
        after_i = jnp.where(odd_stack, bi, ai)
        before_r = jnp.where(first_stack, 1.0, before_r)
        before_i = jnp.where(first_stack, 0.0, before_i)
        unit_ref[0, k] = before_r
        unit_ref[1, k] = before_i
        total_ref[0, k] = before_r * after_r - before_i * after_i
        total_ref[1, k] = before_r * after_i + before_i * after_r


def result_kernel(rows, tiles, outer_ref, inner_ref, rest_ref, datum_ref, out_ref):
    half = rows // 2
    parts = (outer_ref, inner_ref, rest_ref)
    links = [(ref, k) for ref in parts for k in range(ref.shape[2])]

    def one_date(t, carry):
        for k in range(half):
            ref, at = links[k]
            lr, li = ref[0, t, at], ref[1, t, at]
            dr, di = datum_ref[0, k], datum_ref[1, k]
            first, second = bases(k, rows, tiles)
            for part, value in enumerate((lr * dr - li * di, lr * di + li * dr)):
                out_ref[part, t, pl.ds(first, tiles, stride=SUB), :] = value[:tiles]
                out_ref[part, t, pl.ds(second, tiles, stride=SUB), :] = value[tiles:]
        return carry

    lax.fori_loop(0, outer_ref.shape[1], one_date, 0)


def swaps(count, bit=None, odd=False):
    if bit is not None:
        return [(i, i ^ bit) for i in range(count)]
    if odd:
        return [(i, (i + 1 if i % 2 else i - 1) % count) for i in range(count)]
    return [(i, i ^ 1) for i in range(count)]


def inner_swaps(count):
    pairs = [(i, i + 1) for i in range(1, count - 1, 2)]
    return pairs + [(j, i) for i, j in pairs]


def times(a, b):
    return jnp.stack([a[0] * b[0] - a[1] * b[1], a[0] * b[1] + a[1] * b[0]])


def local(amplitude, phase, validity, iterations, reference_date):
    dates, rows, columns = amplitude.shape
    half = rows // 2
    tiles = columns // LANES
    ext = half + HALF_ROWS
    members = lax.axis_size("tm")
    blocks = lax.axis_size("space")
    place = lax.axis_index("tm")
    block = lax.axis_index("space")
    edge = (block == 0) | (block == blocks - 1)
    parity = jnp.stack([block % 2, edge.astype(jnp.int32)])
    params = pltpu.CompilerParams(vmem_limit_bytes=VMEM_LIMIT)

    def shape(*dims):
        return jax.ShapeDtypeStruct(dims, jnp.float32)

    def tiled(x):
        lead = x.shape[:-2]
        x = x.reshape(lead + (rows // SUB, SUB, tiles, LANES))
        return jnp.swapaxes(x, -3, -2).reshape(lead + (rows * tiles, LANES))

    def far_memory(x):
        return pltpu.with_memory_space_constraint(x, pltpu.MemorySpace.HBM)

    z, slab_x, slab_y = pl.pallas_call(
        lambda *refs: images_kernel(rows, tiles, *refs),
        out_shape=(
            shape(2, dates, ext, SUB, LANES),
            shape(dates, HALF_ROWS, SUB, LANES),
            shape(dates, HALF_ROWS, SUB, LANES),
        ),
        in_specs=[smem(), hbm(), hbm(), hbm()],
        out_specs=(vmem(), vmem(), vmem()),
        scratch_shapes=[
            pltpu.VMEM((dates, rows * tiles, LANES), jnp.float32),
            pltpu.VMEM((dates, rows * tiles, LANES), jnp.float32),
            pltpu.VMEM((rows * tiles, LANES), jnp.int32),
            pltpu.SemaphoreType.DMA((3, dates)),
        ],
        compiler_params=params,
        name="images",
    )(parity, *(far_memory(tiled(x)) for x in (amplitude, phase, validity)))
    pair_x, pair_y = swaps(blocks), swaps(blocks, odd=True)
    got_y = lax.ppermute(slab_y, "space", pair_y)
    got_x = lax.ppermute(slab_x, "space", pair_x)

    count = dates * (dates - 1) // 2
    inner = half - HALF_ROWS
    done = min(INNER_DONE, inner - 1)
    work = [
        pltpu.VMEM((2 * count, SUB, LANES), jnp.float32),
        pltpu.VMEM((3 * count + dates, SUB, LANES), jnp.float32),
        pltpu.VMEM((2 * dates, SUB, LANES), jnp.float32),
    ]

    def window_work(vectors):
        return [
            pltpu.VMEM((2 * LANES, 2 * LANES), jnp.bfloat16),
            pltpu.VMEM((dates // 2 + count, 2 * vectors * SUB, 2 * LANES), jnp.bfloat16),
            pltpu.VMEM((dates, vectors, SUB, LANES), jnp.float32),
        ]

    def cost(vectors):
        return pl.CostEstimate(
            flops=vectors * 2_000_000 * 8, bytes_accessed=1 << 20, transcendentals=0
        )

    nr, ni, part, linked_a, comp_a = pl.pallas_call(
        lambda *refs: inner_kernel(tiles, done, *refs),
        out_shape=(
            shape(count, inner - done, SUB, LANES),
            shape(count, inner - done, SUB, LANES),
            shape(2 * count + dates, HALF_ROWS, SUB, LANES),
            shape(2, dates, done, SUB, LANES),
            shape(2, done, SUB, LANES),
        ),
        in_specs=[smem(), smem(), vmem()],
        out_specs=(vmem(),) * 5,
        scratch_shapes=window_work(inner)
        + [pltpu.VMEM((count, done, SUB, LANES), jnp.float32)] * 2
        + work,
        compiler_params=params,
        cost_estimate=cost(4),
        name="inner",
    )(iterations, reference_date, z)
    linked_b, comp_b, pack_x, pack_y = pl.pallas_call(
        lambda *refs: outer_kernel(tiles, *refs),
        out_shape=(
            shape(2, dates, HALF_ROWS, SUB, LANES),
            shape(2, HALF_ROWS, SUB, LANES),
            shape(HALF_ROWS, SUB, LANES),
            shape(HALF_ROWS, SUB, LANES),
        ),
        in_specs=[smem()] * 3 + [vmem()] * 4,
        out_specs=(vmem(),) * 4,
        scratch_shapes=[pltpu.VMEM((2, dates, HALF_ROWS, SUB, LANES), jnp.float32)]
        + window_work(HALF_ROWS)
        + [
            pltpu.VMEM((count, HALF_ROWS, SUB, LANES), jnp.float32),
            pltpu.VMEM((count, HALF_ROWS, SUB, LANES), jnp.float32),
        ]
        + work,
        compiler_params=params,
        cost_estimate=cost(7),
        name="outer",
    )(parity, iterations, reference_date, z, part, got_x, got_y)
    more_y = lax.ppermute(pack_y, "space", pair_y)
    more_x = lax.ppermute(pack_x, "space", pair_x)

    start = HALF_ROWS + done
    linked_c, comp_c = pl.pallas_call(
        lambda *refs: rest_kernel(start, *refs),
        out_shape=(
            shape(2, dates, half - start, SUB, LANES),
            shape(2, half - start, SUB, LANES),
        ),
        in_specs=[smem()] * 2 + [vmem()] * 4,
        out_specs=(vmem(),) * 2,
        scratch_shapes=work,
        compiler_params=params,
        cost_estimate=cost(5),
        name="rest",
    )(iterations, reference_date, z, nr, ni, pack_x)
    wide = pl.pallas_call(
        extend_kernel,
        out_shape=shape(2, ext, SUB, LANES),
        in_specs=[smem()] + [vmem()] * 5,
        out_specs=vmem(),
        compiler_params=params,
        name="extend",
    )(parity, comp_b, comp_a, comp_c, more_x, more_y)
    other_a = lax.ppermute(wide, "tm", swaps(members))
    other_b = lax.ppermute(wide, "tm", inner_swaps(members))
    where = jnp.stack([place, place % 2]).astype(jnp.int32)
    datum, total = pl.pallas_call(
        lambda *refs: offsets_kernel(tiles, *refs),
        out_shape=(shape(2, half, SUB, LANES), shape(2, half, SUB, LANES)),
        in_specs=[smem()] + [vmem()] * 3,
        out_specs=(vmem(), vmem()),
        compiler_params=params,
        name="offsets",
    )(where, wide, other_a, other_b)
    bit = 2
    while bit < members:
        other = lax.ppermute(total, "tm", swaps(members, bit=2 * bit - 2))
        datum = jnp.where((place & bit) != 0, times(datum, other), datum)
        total = times(total, other)
        bit *= 2
    out = pl.pallas_call(
        lambda *refs: result_kernel(rows, tiles, *refs),
        out_shape=shape(2, dates, rows * tiles, LANES),
        in_specs=[vmem()] * 4,
        out_specs=vmem(),
        compiler_params=params,
        name="result",
    )(linked_b, linked_a, linked_c, datum)
    out = out.reshape(2, dates, rows // SUB, tiles, SUB, LANES)
    return jnp.swapaxes(out, -3, -2).reshape(2, dates, rows, columns)


def solution(mesh):
    return jax.shard_map(
        local,
        mesh=mesh,
        in_specs=(
            P("tm", "space", None),
            P("tm", "space", None),
            P("space", None),
            P("tm"),
            P("tm"),
        ),
        out_specs=P(None, "tm", "space", None),
        check_vma=False,
    )
```

```python
import jax
import jax.numpy as jnp
from jax import lax
from jax.experimental import pallas as pl
from jax.experimental.pallas import tpu as pltpu
from jax.sharding import PartitionSpec as P

WIN_ROWS = 11
WIN_COLS = 5
INNER_DONE = 2
PIECE = 2
ITERS = 20
HALF_ROWS = WIN_ROWS // 2

MASKED_WEIGHT = 0.125
LINK_FLOOR = 0.03

LANES = 128
SUB = 8
VMEM_LIMIT = 40 * 1024 * 1024


def vmem():
    return pl.BlockSpec(memory_space=pltpu.VMEM)


def hbm():
    return pl.BlockSpec(memory_space=pltpu.MemorySpace.HBM)


def smem():
    return pl.BlockSpec(memory_space=pltpu.SMEM)


def sublane():
    return lax.broadcasted_iota(jnp.int32, (SUB, LANES), 0)


def lane():
    return lax.broadcasted_iota(jnp.int32, (SUB, LANES), 1)


def row_place():
    at = lax.axis_index("space")
    return at % 2 == 1, (at == 0) | (at == lax.axis_size("space") - 1)


def flip(x):
    return pltpu.roll(x, SUB // 2, 0)


def upper():
    return sublane() < SUB // 2


def bases(k, rows, tiles):
    def base(row):
        return (row // SUB) * SUB * tiles + row % SUB

    return base(k), base(rows - 1 - k)


def load_pair(ref, lead, k, rows, tiles, top):
    first, second = bases(k, rows, tiles)
    a = ref[lead + (pl.ds(first, SUB, stride=SUB), slice(None))]
    b = ref[lead + (pl.ds(second - SUB * tiles, SUB, stride=SUB), slice(None))]
    return jnp.where(top, a, b)


def sin_cos(x):
    turns = jnp.round(x * (2.0 / jnp.pi))
    r = (x - turns * 1.5707855224609375) - turns * 1.0804334124e-05
    s = r * r
    sine = r + r * s * (-1.6666654611e-1 + s * (8.3321608736e-3 + s * -1.9515295891e-4))
    cosine = 1.0 - 0.5 * s + s * s * (
        4.166664568298827e-2 + s * (-1.388731625493765e-3 + s * 2.443315711809948e-5)
    )
    size = jnp.abs(turns)
    odd = size == 1.0
    base_s = jnp.where(odd, cosine, sine)
    base_c = jnp.where(odd, sine, cosine)
    sin_x = jnp.where((turns == -1.0) | (size == 2.0), -base_s, base_s)
    cos_x = jnp.where((turns == 1.0) | (size == 2.0), -base_c, base_c)
    return sin_x, cos_x


def images_kernel(
    rows, tiles, amp_hbm, phase_hbm, valid_hbm, z_ref, x_ref, y_ref,
    amp_ref, phase_ref, valid_ref, sems,
):
    half = rows // 2
    dates = z_ref.shape[1]
    top = upper()
    odd, _ = row_place()
    step = PIECE if dates % PIECE == 0 else dates
    copies = []
    for p in range(dates // step):
        part = pl.ds(p * step, step)
        copies.append(
            [
                pltpu.make_async_copy(amp_hbm.at[part], amp_ref.at[part], sems.at[0, p]),
                pltpu.make_async_copy(phase_hbm.at[part], phase_ref.at[part], sems.at[1, p]),
            ]
        )
    weights = pltpu.make_async_copy(valid_hbm, valid_ref, sems.at[2, 0])
    weights.start()
    for pair in copies:
        for copy in pair:
            copy.start()
    weights.wait()
    roots = []
    for k in range(half):
        valid = load_pair(valid_ref, (), k, rows, tiles, top)
        roots.append(jnp.where(valid == 1, 1.0, MASKED_WEIGHT**0.5).astype(jnp.float32))

    def one_date(t, carry):
        for k in range(half):
            amp = load_pair(amp_ref, (t,), k, rows, tiles, top) * roots[k]
            sin_x, cos_x = sin_cos(load_pair(phase_ref, (t,), k, rows, tiles, top))
            re, im = amp * cos_x, amp * sin_x
            z_ref[0, t, k] = re
            z_ref[1, t, k] = im
            if k >= half - HALF_ROWS:
                z_ref[0, t, 2 * half - 1 - k] = flip(re)
                z_ref[1, t, 2 * half - 1 - k] = flip(im)
            if k < HALF_ROWS:
                first, second = pack(re, im, top)
                x_ref[t, k] = jnp.where(odd, first, second)
                y_ref[t, k] = jnp.where(odd, second, first)
        return carry

    for p, pair in enumerate(copies):
        for copy in pair:
            copy.wait()
        lax.fori_loop(p * step, (p + 1) * step, one_date, 0)


def unpack(first, second, top):
    return jnp.where(top, first, flip(second)), jnp.where(top, flip(first), second)


def pack(re, im, top):
    return jnp.where(top, re, flip(im)), jnp.where(top, flip(re), im)


def add_to(total, sign, value):
    if total is None:
        return value if sign > 0 else -value
    return total + value if sign > 0 else total - value


def running(values):
    out = [values[0]]
    for value in values[1:]:
        out.append(out[-1] + value)
    return out


def inner_sums(field):
    count = len(field) - WIN_ROWS + 1
    tails = running(field[WIN_ROWS - 1 :: -1])[::-1]
    if count <= WIN_ROWS:
        core = running(field[count - 1 : WIN_ROWS])[-1]
        tails = running([core] + field[: count - 1][::-1])[::-1]
    heads = running(field[WIN_ROWS:])
    middle = [tails[q] + heads[q - 1] for q in range(1, min(count, WIN_ROWS))]
    return [tails[0]] + middle + heads[WIN_ROWS - 1 :]


def fill_band(band_ref):
    at = lax.broadcasted_iota(jnp.int32, band_ref.shape, 0) % LANES
    to = lax.broadcasted_iota(jnp.int32, band_ref.shape, 1)
    reach = WIN_COLS // 2
    inside = (to < LANES) & (jnp.abs(at - to) <= reach)
    to = to - LANES
    beside = (to >= 0) & ((at >= to + LANES - reach) | (at <= to - LANES + reach))
    band_ref[...] = jnp.where(inside | beside, 1.0, 0.0).astype(band_ref.dtype)


def put_split(ref, at, vectors):
    x = jnp.concatenate(vectors, axis=0)
    high = x.astype(jnp.bfloat16)
    low = (x - high.astype(jnp.float32)).astype(jnp.bfloat16)
    ref[at, :, :LANES] = high
    ref[at, :, LANES:] = low


def side_masks(tiles):
    column = sublane() % tiles
    at = lane()
    return (at < LANES // 2) & (column != 0), (at >= LANES // 2) & (column != tiles - 1)


def column_sums(split_ref, first, size, band, sides):
    rows = split_ref.shape[1]
    terms = split_ref[first : first + size].reshape(size * rows, 2 * LANES)
    both = jnp.dot(terms, band, preferred_element_type=jnp.float32)
    from_before, from_after = sides
    out = []
    for k in range(size * rows // SUB):
        inside = both[k * SUB : (k + 1) * SUB, :LANES]
        beside = both[k * SUB : (k + 1) * SUB, LANES:]
        before, after = pltpu.roll(beside, 1, 0), pltpu.roll(beside, SUB - 1, 0)
        out.append(
            inside + jnp.where(from_before, before, jnp.where(from_after, after, 0.0))
        )
    return out


def pair_list(dates):
    return [(i, j) for i in range(dates) for j in range(i + 1, dates)]


CHUNK = 5


def coherence(dates, vectors, fields, split_ref, band_ref, inv_ref, places, sides):
    pairs = pair_list(dates)
    band = band_ref[...]
    powers = [fields(i, i) for i in range(dates)]
    half = dates // 2
    for e in range(half):
        put_split(split_ref, e, powers[2 * e] + powers[2 * e + 1])
    sums = column_sums(split_ref, 0, half, band, sides)
    for i in range(dates):
        for k in range(vectors):
            inv_ref[i, k] = lax.rsqrt(sums[i * vectors + k]) * 0.5
    for first in range(0, len(pairs), CHUNK):
        size = min(CHUNK, len(pairs) - first)
        for e in range(first, first + size):
            re, im = fields(*pairs[e])
            put_split(split_ref, half + e, re + im)
        sums = column_sums(split_ref, half + first, size, band, sides)
        for e in range(first, first + size):
            i, j = pairs[e]
            base = (e - first) * 2 * vectors
            for k in range(vectors):
                scale = inv_ref[i, k] * inv_ref[j, k]
                nr_ref, ni_ref, at = places[k]
                nr_ref[e, at] = sums[base + k] * scale
                ni_ref[e, at] = sums[base + vectors + k] * scale


def cross(a, b):
    (ar, ai), (br, bi) = a, b
    re = [p * r + q * s for p, q, r, s in zip(ar, ai, br, bi)]
    im = [q * r - p * s for p, q, r, s in zip(ar, ai, br, bi)]
    return re, im


def power_of(a):
    return [p * p + q * q for p, q in zip(*a)]


def iterate(
    first, last, offset, dates, iter_ref, z_ref, nr, ni, more, sq, vec,
    link_ref, comp_ref, out_offset=0,
):
    pairs = pair_list(dates)
    index = {pair: e for e, pair in enumerate(pairs)}
    count = len(pairs)
    groups = []
    at = 0
    for size in (3, 3, 4) if dates == 10 else (dates,):
        groups.append(tuple(range(at, at + size)))
        at += size

    def one_vector(whole_k, carry):
        k = whole_k - offset
        place = whole_k - out_offset
        for e in range(count):
            re, im = nr[e, k], ni[e, k]
            more[e] = re + im
            more[count + e] = im - re

        def left(i, t):
            if i < t:
                e = index[i, t]
                return (nr[e, k], 1), (more[e], 1), (more[count + e], 1)
            e = index[t, i]
            return (nr[e, k], 1), (more[count + e], -1), (more[e], -1)

        def right(t, j):
            if t < j:
                e = index[t, j]
                return (nr[e, k], 1), (ni[e, k], 1), (more[e], 1)
            e = index[j, t]
            return (nr[e, k], 1), (ni[e, k], -1), (more[count + e], -1)

        def square(out):
            sums = {pair: [None, None, None] for pair in out}
            rows_in = sorted({i for i, _ in out})
            cols_in = sorted({j for _, j in out})
            for t in range(dates):
                lefts = {i: left(i, t) for i in rows_in if i != t}
                rights = {j: right(t, j) for j in cols_in if j != t}
                for i, j in out:
                    if t in (i, j):
                        continue
                    (ar, _), (ap, sap), (aq, saq) = lefts[i]
                    (br, _), (bi, sbi), (bs, sbs) = rights[j]
                    s = sums[i, j]
                    s[0] = add_to(s[0], sbs, ar * bs)
                    s[1] = add_to(s[1], saq, aq * br)
                    s[2] = add_to(s[2], sap * sbi, ap * bi)
            for i, j in out:
                e = index[i, j]
                s = sums[i, j]
                re = s[0] - s[2] + nr[e, k]
                im = s[0] + s[1] + ni[e, k]
                sq[e] = re
                sq[count + e] = re + im
                sq[2 * count + e] = im - re

        for a in range(len(groups)):
            square([(i, j) for i in groups[a] for j in groups[a] if i < j])
            for b in range(a + 1, len(groups)):
                square([(i, j) for i in groups[a] for j in groups[b]])
        size = [None] * dates
        for e, (i, j) in enumerate(pairs):
            re, im = nr[e, k], ni[e, k]
            value = re * re + im * im
            size[i] = add_to(size[i], 1, value)
            size[j] = add_to(size[j], 1, value)
        for i in range(dates):
            sq[3 * count + i] = size[i] + 0.25

        turns = jnp.minimum(iter_ref[0], ITERS)
        odd_turns = turns % 2 == 1
        steps = jnp.where(odd_turns, turns // 2, turns // 2 - 1)

        def row_sums(re_of, im_of, own):
            sr, si = [own(i) for i in range(dates)], [None] * dates
            for e, (i, j) in enumerate(pairs):
                re, im = re_of(e), im_of(e)
                sr[i] = sr[i] + re
                sr[j] = sr[j] + re
                si[i] = add_to(si[i], 1, im)
                si[j] = add_to(si[j], -1, im)
            for i in range(dates):
                vec[i] = sr[i]
                vec[dates + i] = si[i]

        @pl.when(odd_turns)
        def _():
            row_sums(lambda e: nr[e, k], lambda e: ni[e, k],
                     lambda i: jnp.full((SUB, LANES), 0.5, jnp.float32))

        @pl.when(jnp.logical_not(odd_turns))
        def _():
            row_sums(lambda e: sq[e], lambda e: sq[count + e] - sq[e],
                     lambda i: sq[3 * count + i])

        def step(_, vectors):
            vr, vi = vectors[:dates], vectors[dates:]
            vs = [a + b for a, b in zip(vr, vi)]
            out_r, out_i = [], []
            for rows_in in groups:
                sums = {i: [None, None, None] for i in rows_in}
                for i in rows_in:
                    for j in range(dates):
                        if j == i or (j in rows_in and j < i):
                            continue
                        e = index[min(i, j), max(i, j)]
                        re, plus, minus = sq[e], sq[count + e], sq[2 * count + e]
                        s = sums[i]
                        if i < j:
                            s[0] = add_to(s[0], 1, re * vs[j])
                            s[1] = add_to(s[1], 1, minus * vr[j])
                            s[2] = add_to(s[2], 1, plus * vi[j])
                            if j in rows_in:
                                s = sums[j]
                                s[0] = add_to(s[0], 1, re * vs[i])
                                s[1] = add_to(s[1], -1, plus * vr[i])
                                s[2] = add_to(s[2], -1, minus * vi[i])
                        else:
                            s[0] = add_to(s[0], 1, re * vs[j])
                            s[1] = add_to(s[1], -1, plus * vr[j])
                            s[2] = add_to(s[2], -1, minus * vi[j])
                for i in rows_in:
                    own = sq[3 * count + i]
                    s = sums[i]
                    out_r.append(s[0] - s[2] + own * vr[i])
                    out_i.append(s[0] + s[1] + own * vi[i])
            return tuple(out_r + out_i)

        vectors = lax.fori_loop(0, steps, step, tuple(vec[i] for i in range(2 * dates)))
        length = None
        for part in vectors:
            length = add_to(length, 1, part * part)
        scale = lax.rsqrt(length)
        vr = [a * scale for a in vectors[:dates]]
        vi = [a * scale for a in vectors[dates:]]
        cr = ci = None
        for i in range(dates):
            zr, zi = z_ref[0, i, whole_k], z_ref[1, i, whole_k]
            cr = add_to(cr, 1, vr[i] * zr + vi[i] * zi)
            ci = add_to(ci, 1, vr[i] * zi - vi[i] * zr)
        comp_ref[0, place] = cr
        comp_ref[1, place] = ci
        for i in range(dates):
            link_ref[0, i, place] = vr[i]
            link_ref[1, i, place] = vi[i]
        return carry

    lax.fori_loop(first, last, one_vector, 0)


def inner_kernel(
    tiles, done, iter_ref, z_ref,
    nr_b, ni_b, part_ref, link_ref, comp_ref,
    band, split, inv, nr_a, ni_a, more, sq, vec,
):
    dates = z_ref.shape[1]
    places = [
        (nr, ni, k)
        for nr, ni in ((nr_a, ni_a), (nr_b, ni_b))
        for k in range(nr.shape[1])
    ]
    vectors = len(places)
    ext = vectors + 2 * HALF_ROWS
    pairs = pair_list(dates)
    count = len(pairs)
    index = {pair: e for e, pair in enumerate(pairs)}
    fill_band(band)

    def image(t):
        return [[z_ref[part, t, k] for k in range(ext)] for part in range(2)]

    def keep(at, field):
        heads = running(field[: 2 * HALF_ROWS])
        for k in range(HALF_ROWS):
            part_ref[at, k] = heads[HALF_ROWS + k]

    def fields(i, j):
        if i == j:
            power = power_of(image(i))
            keep(2 * count + i, power)
            return inner_sums(power)
        re, im = cross(image(i), image(j))
        e = index[i, j]
        keep(e, re)
        keep(count + e, im)
        return inner_sums(re), inner_sums(im)

    coherence(dates, vectors, fields, split, band, inv, places, side_masks(tiles))
    iterate(
        HALF_ROWS, HALF_ROWS + done, HALF_ROWS, dates, iter_ref, z_ref, nr_a, ni_a,
        more, sq, vec, link_ref, comp_ref, HALF_ROWS,
    )


def outer_kernel(
    tiles, iter_ref, z_ref, part_ref, x_ref, y_ref,
    link_ref, comp_ref, pack_x_ref, pack_y_ref,
    halo, band, split, inv, nr, ni, more, sq, vec,
):
    dates = z_ref.shape[1]
    top = upper()
    odd_device, edge = row_place()
    pairs = pair_list(dates)
    count = len(pairs)
    index = {pair: e for e, pair in enumerate(pairs)}
    fill_band(band)

    def fill(t, carry):
        for k in range(HALF_ROWS):
            a, b = x_ref[t, k], jnp.where(edge, 0.0, y_ref[t, k])
            re, im = unpack(jnp.where(odd_device, a, b), jnp.where(odd_device, b, a), top)
            halo[0, t, k] = re
            halo[1, t, k] = im
        return carry

    lax.fori_loop(0, dates, fill, 0)

    def image(t):
        return [[halo[part, t, k] for k in range(HALF_ROWS)] for part in range(2)]

    def add(at, field):
        tails = running(field)
        return [tails[HALF_ROWS - 1 - k] + part_ref[at, k] for k in range(HALF_ROWS)]

    def fields(i, j):
        if i == j:
            return add(2 * count + i, power_of(image(i)))
        re, im = cross(image(i), image(j))
        e = index[i, j]
        return add(e, re), add(count + e, im)

    places = [(nr, ni, k) for k in range(HALF_ROWS)]
    coherence(dates, HALF_ROWS, fields, split, band, inv, places, side_masks(tiles))
    iterate(
        0, HALF_ROWS, 0, dates, iter_ref, z_ref, nr, ni, more, sq, vec,
        link_ref, comp_ref,
    )
    for k in range(HALF_ROWS):
        first, second = pack(comp_ref[0, k], comp_ref[1, k], top)
        pack_x_ref[k] = jnp.where(odd_device, first, second)
        pack_y_ref[k] = jnp.where(odd_device, second, first)


def rest_kernel(
    start, iter_ref, z_ref, nr, ni, after_ref, link_ref, comp_ref,
    more, sq, vec,
):
    dates = z_ref.shape[1]
    iterate(
        start, start + comp_ref.shape[1], start, dates, iter_ref, z_ref, nr, ni,
        more, sq, vec, link_ref, comp_ref, start,
    )


def box_sum(field, lanes, edges):
    last_two, last_one, first_one, first_two = lanes
    keep_before, keep_after = edges
    out = []
    for x in inner_sums(field):
        before = jnp.where(keep_before, pltpu.roll(x, 1, 0), 0.0)
        after = jnp.where(keep_after, pltpu.roll(x, SUB - 1, 0), 0.0)
        near = pltpu.roll(jnp.where(last_one, before, x), 1, 1) + pltpu.roll(
            jnp.where(first_one, after, x), LANES - 1, 1
        )
        far = pltpu.roll(jnp.where(last_two, before, x), 2, 1) + pltpu.roll(
            jnp.where(first_two, after, x), LANES - 2, 1
        )
        out.append(x + near + far)
    return out


def masks(tiles):
    at = lane()
    lanes = (at >= LANES - 2, at >= LANES - 1, at < 1, at < 2)
    column = sublane() % tiles
    return lanes, (column != 0, column != tiles - 1)


def extend_kernel(outer_ref, inner_ref, rest_ref, x_ref, y_ref, out_ref):
    top = upper()
    odd_device, edge = row_place()
    for k in range(HALF_ROWS):
        a, b = x_ref[k], jnp.where(edge, 0.0, y_ref[k])
        re, im = unpack(jnp.where(odd_device, a, b), jnp.where(odd_device, b, a), top)
        out_ref[0, HALF_ROWS - 1 - k] = re
        out_ref[1, HALF_ROWS - 1 - k] = im
    for part in range(2):
        at = HALF_ROWS
        for ref in (outer_ref, inner_ref, rest_ref):
            for k in range(ref.shape[1]):
                out_ref[part, at] = ref[part, k]
                at += 1


def offsets_kernel(
    tiles, own_ref, a_ref, b_ref, unit_ref, total_ref
):
    lanes, edges = masks(tiles)
    half = unit_ref.shape[1]
    place = lax.axis_index("tm")
    odd_stack = place % 2 == 1
    first_stack = place == 0

    def whole(*refs):
        parts = []
        for part in range(2):
            rows_in = [ref[part, k] for ref in refs for k in range(ref.shape[1])]
            rows_in += [flip(rows_in[-1 - k]) for k in range(HALF_ROWS)]
            parts.append(rows_in)
        return parts

    def power(re, im):
        return box_sum([a * a + b * b for a, b in zip(re, im)], lanes, edges)

    own_r, own_i = whole(own_ref)
    own = [p + 1.0 for p in power(own_r, own_i)]

    def unit(*refs):
        re, im = whole(*refs)
        other = power(re, im)
        cross_r = box_sum(
            [a * c + b * d for a, b, c, d in zip(own_r, own_i, re, im)], lanes, edges
        )
        cross_i = box_sum(
            [b * c - a * d for a, b, c, d in zip(own_r, own_i, re, im)], lanes, edges
        )
        out = []
        for k in range(half):
            scale = lax.rsqrt(own[k] * (other[k] + 1.0))
            off_r, off_i = cross_r[k] * scale, cross_i[k] * scale
            bound = jnp.maximum(jnp.sqrt(off_r * off_r + off_i * off_i), LINK_FLOOR)
            back = 1.0 / bound
            out.append((off_r * back, off_i * back))
        return out

    pair_a, pair_b = unit(a_ref), unit(b_ref)
    for k in range(half):
        (ar, ai), (br, bi) = pair_a[k], pair_b[k]
        before_r = jnp.where(odd_stack, ar, br)
        before_i = -jnp.where(odd_stack, ai, bi)
        after_r = jnp.where(odd_stack, br, ar)
        after_i = jnp.where(odd_stack, bi, ai)
        before_r = jnp.where(first_stack, 1.0, before_r)
        before_i = jnp.where(first_stack, 0.0, before_i)
        unit_ref[0, k] = before_r
        unit_ref[1, k] = before_i
        total_ref[0, k] = before_r * after_r - before_i * after_i
        total_ref[1, k] = before_r * after_i + before_i * after_r


def result_kernel(
    rows, tiles, chosen_ref, outer_ref, inner_ref, rest_ref, datum_ref, out_hbm,
    out_ref, turn, sems,
):
    half = rows // 2
    parts = (outer_ref, inner_ref, rest_ref)
    links = [(ref, k) for ref in parts for k in range(ref.shape[2])]
    dates = outer_ref.shape[1]

    chosen = chosen_ref[0]
    for k, (ref, at) in enumerate(links):
        vr = ref[0, chosen, at] * float(dates)
        vi = ref[1, chosen, at] * float(dates)
        dr, di = datum_ref[0, k], datum_ref[1, k]
        turn[0, k] = dr * vr + di * vi
        turn[1, k] = di * vr - dr * vi

    def copies(t):
        return [
            pltpu.make_async_copy(out_ref.at[part, t], out_hbm.at[part, t], sems.at[part, t])
            for part in range(2)
        ]

    def one_date(t, carry):
        for k in range(half):
            ref, at = links[k]
            lr, li = ref[0, t, at], ref[1, t, at]
            dr, di = turn[0, k], turn[1, k]
            first, second = bases(k, rows, tiles)
            for part, value in enumerate((lr * dr - li * di, lr * di + li * dr)):
                out_ref[part, t, pl.ds(first, tiles, stride=SUB), :] = value[:tiles]
                out_ref[part, t, pl.ds(second, tiles, stride=SUB), :] = value[tiles:]
        for copy in copies(t):
            copy.start()
        return carry

    lax.fori_loop(0, dates, one_date, 0)
    for t in range(dates):
        for copy in copies(t):
            copy.wait()


def swaps(count, bit=None, odd=False):
    if bit is not None:
        return [(i, i ^ bit) for i in range(count)]
    if odd:
        return [(i, (i + 1 if i % 2 else i - 1) % count) for i in range(count)]
    return [(i, i ^ 1) for i in range(count)]


def inner_swaps(count):
    pairs = [(i, i + 1) for i in range(1, count - 1, 2)]
    return pairs + [(j, i) for i, j in pairs]


def times(a, b):
    return jnp.stack([a[0] * b[0] - a[1] * b[1], a[0] * b[1] + a[1] * b[0]])


def local(amplitude, phase, validity, iterations, reference_date):
    dates, rows, columns = amplitude.shape
    half = rows // 2
    tiles = columns // LANES
    ext = half + HALF_ROWS
    members = lax.axis_size("tm")
    blocks = lax.axis_size("space")
    place = lax.axis_index("tm")
    params = pltpu.CompilerParams(vmem_limit_bytes=VMEM_LIMIT)

    def shape(*dims):
        return jax.ShapeDtypeStruct(dims, jnp.float32)

    def tiled(x):
        lead = x.shape[:-2]
        x = x.reshape(lead + (rows // SUB, SUB, tiles, LANES))
        return jnp.swapaxes(x, -3, -2).reshape(lead + (rows * tiles, LANES))

    def far_memory(x):
        return pltpu.with_memory_space_constraint(x, pltpu.MemorySpace.HBM)

    z, slab_x, slab_y = pl.pallas_call(
        lambda *refs: images_kernel(rows, tiles, *refs),
        out_shape=(
            shape(2, dates, ext, SUB, LANES),
            shape(dates, HALF_ROWS, SUB, LANES),
            shape(dates, HALF_ROWS, SUB, LANES),
        ),
        in_specs=[hbm(), hbm(), hbm()],
        out_specs=(vmem(), vmem(), vmem()),
        scratch_shapes=[
            pltpu.VMEM((dates, rows * tiles, LANES), jnp.float32),
            pltpu.VMEM((dates, rows * tiles, LANES), jnp.float32),
            pltpu.VMEM((rows * tiles, LANES), jnp.int32),
            pltpu.SemaphoreType.DMA((3, dates)),
        ],
        compiler_params=params,
        name="images",
    )(*(far_memory(tiled(x)) for x in (amplitude, phase, validity)))
    pair_x, pair_y = swaps(blocks), swaps(blocks, odd=True)
    got_y = lax.ppermute(slab_y, "space", pair_y)
    got_x = lax.ppermute(slab_x, "space", pair_x)

    count = dates * (dates - 1) // 2
    inner = half - HALF_ROWS
    done = min(INNER_DONE, inner - 1)
    work = [
        pltpu.VMEM((2 * count, SUB, LANES), jnp.float32),
        pltpu.VMEM((3 * count + dates, SUB, LANES), jnp.float32),
        pltpu.VMEM((2 * dates, SUB, LANES), jnp.float32),
    ]

    def window_work(vectors):
        return [
            pltpu.VMEM((2 * LANES, 2 * LANES), jnp.bfloat16),
            pltpu.VMEM((dates // 2 + count, 2 * vectors * SUB, 2 * LANES), jnp.bfloat16),
            pltpu.VMEM((dates, vectors, SUB, LANES), jnp.float32),
        ]

    def cost(vectors):
        return pl.CostEstimate(
            flops=vectors * 2_000_000 * 8, bytes_accessed=1 << 20, transcendentals=0
        )

    nr, ni, part, linked_a, comp_a = pl.pallas_call(
        lambda *refs: inner_kernel(tiles, done, *refs),
        out_shape=(
            shape(count, inner - done, SUB, LANES),
            shape(count, inner - done, SUB, LANES),
            shape(2 * count + dates, HALF_ROWS, SUB, LANES),
            shape(2, dates, done, SUB, LANES),
            shape(2, done, SUB, LANES),
        ),
        in_specs=[smem(), vmem()],
        out_specs=(vmem(),) * 5,
        scratch_shapes=window_work(inner)
        + [pltpu.VMEM((count, done, SUB, LANES), jnp.float32)] * 2
        + work,
        compiler_params=params,
        cost_estimate=cost(4),
        name="inner",
    )(iterations, z)
    linked_b, comp_b, pack_x, pack_y = pl.pallas_call(
        lambda *refs: outer_kernel(tiles, *refs),
        out_shape=(
            shape(2, dates, HALF_ROWS, SUB, LANES),
            shape(2, HALF_ROWS, SUB, LANES),
            shape(HALF_ROWS, SUB, LANES),
            shape(HALF_ROWS, SUB, LANES),
        ),
        in_specs=[smem()] + [vmem()] * 4,
        out_specs=(vmem(),) * 4,
        scratch_shapes=[pltpu.VMEM((2, dates, HALF_ROWS, SUB, LANES), jnp.float32)]
        + window_work(HALF_ROWS)
        + [
            pltpu.VMEM((count, HALF_ROWS, SUB, LANES), jnp.float32),
            pltpu.VMEM((count, HALF_ROWS, SUB, LANES), jnp.float32),
        ]
        + work,
        compiler_params=params,
        cost_estimate=cost(7),
        name="outer",
    )(iterations, z, part, got_x, got_y)
    more_y = lax.ppermute(pack_y, "space", pair_y)
    more_x = lax.ppermute(pack_x, "space", pair_x)

    start = HALF_ROWS + done
    linked_c, comp_c = pl.pallas_call(
        lambda *refs: rest_kernel(start, *refs),
        out_shape=(
            shape(2, dates, half - start, SUB, LANES),
            shape(2, half - start, SUB, LANES),
        ),
        in_specs=[smem()] + [vmem()] * 4,
        out_specs=(vmem(),) * 2,
        scratch_shapes=work,
        compiler_params=params,
        cost_estimate=cost(5),
        name="rest",
    )(iterations, z, nr, ni, pack_x)
    wide = pl.pallas_call(
        extend_kernel,
        out_shape=shape(2, ext, SUB, LANES),
        in_specs=[vmem()] * 5,
        out_specs=vmem(),
        compiler_params=params,
        name="extend",
    )(comp_b, comp_a, comp_c, more_x, more_y)
    other_a = lax.ppermute(wide, "tm", swaps(members))
    other_b = lax.ppermute(wide, "tm", inner_swaps(members))
    datum, total = pl.pallas_call(
        lambda *refs: offsets_kernel(tiles, *refs),
        out_shape=(shape(2, half, SUB, LANES), shape(2, half, SUB, LANES)),
        in_specs=[vmem()] * 3,
        out_specs=(vmem(), vmem()),
        compiler_params=params,
        name="offsets",
    )(wide, other_a, other_b)
    bit = 2
    while bit < members:
        other = lax.ppermute(total, "tm", swaps(members, bit=2 * bit - 2))
        datum = jnp.where((place & bit) != 0, times(datum, other), datum)
        total = times(total, other)
        bit *= 2
    out = pl.pallas_call(
        lambda *refs: result_kernel(rows, tiles, *refs),
        out_shape=shape(2, dates, rows * tiles, LANES),
        in_specs=[smem()] + [vmem()] * 4,
        out_specs=hbm(),
        scratch_shapes=[
            pltpu.VMEM((2, dates, rows * tiles, LANES), jnp.float32),
            pltpu.VMEM((2, half, SUB, LANES), jnp.float32),
            pltpu.SemaphoreType.DMA((2, dates)),
        ],
        compiler_params=params,
        name="result",
    )(reference_date, linked_b, linked_a, linked_c, datum)
    out = out.reshape(2, dates, rows // SUB, tiles, SUB, LANES)
    return jnp.swapaxes(out, -3, -2).reshape(2, dates, rows, columns)


def solution(mesh):
    return jax.shard_map(
        local,
        mesh=mesh,
        in_specs=(
            P("tm", "space", None),
            P("tm", "space", None),
            P("space", None),
            P("tm"),
            P("tm"),
        ),
        out_specs=P(None, "tm", "space", None),
        check_vma=False,
    )
```

```python
import jax
import jax.numpy as jnp
from jax import lax
from jax.experimental import pallas as pl
from jax.experimental.pallas import tpu as pltpu
from jax.sharding import PartitionSpec as P


WIN_ROWS = 11
WIN_COLS = 5
INNER_DONE = 3
PIECE = 2
ITERS = 20
HALF_ROWS = WIN_ROWS // 2

MASKED_WEIGHT = 0.125
LINK_FLOOR = 0.03

LANES = 128
SUB = 8
VMEM_LIMIT = 40 * 1024 * 1024


def vmem():
    return pl.BlockSpec(memory_space=pltpu.VMEM)


def hbm():
    return pl.BlockSpec(memory_space=pltpu.MemorySpace.HBM)


def smem():
    return pl.BlockSpec(memory_space=pltpu.SMEM)


def sublane():
    return lax.broadcasted_iota(jnp.int32, (SUB, LANES), 0)


def lane():
    return lax.broadcasted_iota(jnp.int32, (SUB, LANES), 1)


def row_place():
    at = lax.axis_index("space")
    return at % 2 == 1, (at == 0) | (at == lax.axis_size("space") - 1)


def flip(x):
    return pltpu.roll(x, SUB // 2, 0)


def upper():
    return sublane() < SUB // 2


def bases(k, rows, tiles):
    def base(row):
        return (row // SUB) * SUB * tiles + row % SUB

    return base(k), base(rows - 1 - k)


def load_pair(ref, lead, k, rows, tiles, top):
    first, second = bases(k, rows, tiles)
    a = ref[lead + (pl.ds(first, SUB, stride=SUB), slice(None))]
    b = ref[lead + (pl.ds(second - SUB * tiles, SUB, stride=SUB), slice(None))]
    return jnp.where(top, a, b)


def sin_cos(x):
    turns = jnp.round(x * (2.0 / jnp.pi))
    r = (x - turns * 1.5707855224609375) - turns * 1.0804334124e-05
    s = r * r
    sine = r + r * s * (-1.6666654611e-1 + s * (8.3321608736e-3 + s * -1.9515295891e-4))
    cosine = 1.0 - 0.5 * s + s * s * (
        4.166664568298827e-2 + s * (-1.388731625493765e-3 + s * 2.443315711809948e-5)
    )
    size = jnp.abs(turns)
    odd = size == 1.0
    base_s = jnp.where(odd, cosine, sine)
    base_c = jnp.where(odd, sine, cosine)
    sin_x = jnp.where((turns == -1.0) | (size == 2.0), -base_s, base_s)
    cos_x = jnp.where((turns == 1.0) | (size == 2.0), -base_c, base_c)
    return sin_x, cos_x


def images_kernel(
    rows, tiles, amp_hbm, phase_hbm, valid_hbm, z_ref, x_ref, y_ref,
    amp_ref, phase_ref, valid_ref, sems,
):
    half = rows // 2
    dates = z_ref.shape[1]
    top = upper()
    odd, _ = row_place()
    step = PIECE if dates % PIECE == 0 else dates
    copies = []
    for p in range(dates // step):
        part = pl.ds(p * step, step)
        copies.append(
            [
                pltpu.make_async_copy(amp_hbm.at[part], amp_ref.at[part], sems.at[0, p]),
                pltpu.make_async_copy(phase_hbm.at[part], phase_ref.at[part], sems.at[1, p]),
            ]
        )
    weights = pltpu.make_async_copy(valid_hbm, valid_ref, sems.at[2, 0])
    weights.start()
    for pair in copies:
        for copy in pair:
            copy.start()
    weights.wait()
    roots = []
    for k in range(half):
        valid = load_pair(valid_ref, (), k, rows, tiles, top)
        roots.append(jnp.where(valid == 1, 1.0, MASKED_WEIGHT**0.5).astype(jnp.float32))

    def one_date(t, carry):
        for k in range(half):
            amp = load_pair(amp_ref, (t,), k, rows, tiles, top) * roots[k]
            sin_x, cos_x = sin_cos(load_pair(phase_ref, (t,), k, rows, tiles, top))
            re, im = amp * cos_x, amp * sin_x
            z_ref[0, t, k] = re
            z_ref[1, t, k] = im
            if k >= half - HALF_ROWS:
                z_ref[0, t, 2 * half - 1 - k] = flip(re)
                z_ref[1, t, 2 * half - 1 - k] = flip(im)
            if k < HALF_ROWS:
                first, second = pack(re, im, top)
                x_ref[t, k] = jnp.where(odd, first, second)
                y_ref[t, k] = jnp.where(odd, second, first)
        return carry

    for p, pair in enumerate(copies):
        for copy in pair:
            copy.wait()
        lax.fori_loop(p * step, (p + 1) * step, one_date, 0)


def unpack(first, second, top):
    return jnp.where(top, first, flip(second)), jnp.where(top, flip(first), second)


def pack(re, im, top):
    return jnp.where(top, re, flip(im)), jnp.where(top, flip(re), im)


def add_to(total, sign, value):
    if total is None:
        return value if sign > 0 else -value
    return total + value if sign > 0 else total - value


def running(values):
    out = [values[0]]
    for value in values[1:]:
        out.append(out[-1] + value)
    return out


def inner_sums(field):
    count = len(field) - WIN_ROWS + 1
    tails = running(field[WIN_ROWS - 1 :: -1])[::-1]
    if count <= WIN_ROWS:
        core = running(field[count - 1 : WIN_ROWS])[-1]
        tails = running([core] + field[: count - 1][::-1])[::-1]
    heads = running(field[WIN_ROWS:])
    middle = [tails[q] + heads[q - 1] for q in range(1, min(count, WIN_ROWS))]
    return [tails[0]] + middle + heads[WIN_ROWS - 1 :]


def fill_band(band_ref):
    at = lax.broadcasted_iota(jnp.int32, band_ref.shape, 0) % LANES
    to = lax.broadcasted_iota(jnp.int32, band_ref.shape, 1)
    reach = WIN_COLS // 2
    inside = (to < LANES) & (jnp.abs(at - to) <= reach)
    to = to - LANES
    beside = (to >= 0) & ((at >= to + LANES - reach) | (at <= to - LANES + reach))
    band_ref[...] = jnp.where(inside | beside, 1.0, 0.0).astype(band_ref.dtype)


def put_split(ref, at, vectors):
    x = jnp.concatenate(vectors, axis=0)
    high = x.astype(jnp.bfloat16)
    low = (x - high.astype(jnp.float32)).astype(jnp.bfloat16)
    ref[at, :, :LANES] = high
    ref[at, :, LANES:] = low


def side_masks(tiles):
    column = sublane() % tiles
    at = lane()
    return (at < LANES // 2) & (column != 0), (at >= LANES // 2) & (column != tiles - 1)


def column_sums(split_ref, first, size, band, sides):
    rows = split_ref.shape[1]
    terms = split_ref[first : first + size].reshape(size * rows, 2 * LANES)
    both = jnp.dot(terms, band, preferred_element_type=jnp.float32)
    from_before, from_after = sides
    out = []
    for k in range(size * rows // SUB):
        inside = both[k * SUB : (k + 1) * SUB, :LANES]
        beside = both[k * SUB : (k + 1) * SUB, LANES:]
        before, after = pltpu.roll(beside, 1, 0), pltpu.roll(beside, SUB - 1, 0)
        out.append(
            inside + jnp.where(from_before, before, jnp.where(from_after, after, 0.0))
        )
    return out


def pair_list(dates):
    return [(i, j) for i in range(dates) for j in range(i + 1, dates)]


CHUNK = 5


def coherence(dates, vectors, fields, split_ref, band_ref, inv_ref, places, sides):
    pairs = pair_list(dates)
    band = band_ref[...]
    powers = [fields(i, i) for i in range(dates)]
    half = dates // 2
    for e in range(half):
        put_split(split_ref, e, powers[2 * e] + powers[2 * e + 1])
    sums = column_sums(split_ref, 0, half, band, sides)
    for i in range(dates):
        for k in range(vectors):
            inv_ref[i, k] = lax.rsqrt(sums[i * vectors + k]) * 0.5
    for first in range(0, len(pairs), CHUNK):
        size = min(CHUNK, len(pairs) - first)
        for e in range(first, first + size):
            re, im = fields(*pairs[e])
            put_split(split_ref, half + e, re + im)
        sums = column_sums(split_ref, half + first, size, band, sides)
        for e in range(first, first + size):
            i, j = pairs[e]
            base = (e - first) * 2 * vectors
            for k in range(vectors):
                scale = inv_ref[i, k] * inv_ref[j, k]
                nr_ref, ni_ref, at = places[k]
                nr_ref[e, at] = sums[base + k] * scale
                ni_ref[e, at] = sums[base + vectors + k] * scale


def cross(a, b):
    (ar, ai), (br, bi) = a, b
    re = [p * r + q * s for p, q, r, s in zip(ar, ai, br, bi)]
    im = [q * r - p * s for p, q, r, s in zip(ar, ai, br, bi)]
    return re, im


def power_of(a):
    return [p * p + q * q for p, q in zip(*a)]


def iterate(
    first, last, offset, dates, iter_ref, z_ref, nr, ni, more, sq, vec,
    link_ref, comp_ref, out_offset=0,
):
    pairs = pair_list(dates)
    index = {pair: e for e, pair in enumerate(pairs)}
    count = len(pairs)
    groups = []
    at = 0
    for size in (3, 3, 4) if dates == 10 else (dates,):
        groups.append(tuple(range(at, at + size)))
        at += size

    def one_vector(whole_k, carry):
        k = whole_k - offset
        place = whole_k - out_offset
        for e in range(count):
            re, im = nr[e, k], ni[e, k]
            more[e] = re + im
            more[count + e] = im - re

        def left(i, t):
            if i < t:
                e = index[i, t]
                return (nr[e, k], 1), (more[e], 1), (more[count + e], 1)
            e = index[t, i]
            return (nr[e, k], 1), (more[count + e], -1), (more[e], -1)

        def right(t, j):
            if t < j:
                e = index[t, j]
                return (nr[e, k], 1), (ni[e, k], 1), (more[e], 1)
            e = index[j, t]
            return (nr[e, k], 1), (ni[e, k], -1), (more[count + e], -1)

        def square(out):
            sums = {pair: [None, None, None] for pair in out}
            rows_in = sorted({i for i, _ in out})
            cols_in = sorted({j for _, j in out})
            for t in range(dates):
                lefts = {i: left(i, t) for i in rows_in if i != t}
                rights = {j: right(t, j) for j in cols_in if j != t}
                for i, j in out:
                    if t in (i, j):
                        continue
                    (ar, _), (ap, sap), (aq, saq) = lefts[i]
                    (br, _), (bi, sbi), (bs, sbs) = rights[j]
                    s = sums[i, j]
                    s[0] = add_to(s[0], sbs, ar * bs)
                    s[1] = add_to(s[1], saq, aq * br)
                    s[2] = add_to(s[2], sap * sbi, ap * bi)
            for i, j in out:
                e = index[i, j]
                s = sums[i, j]
                re = s[0] - s[2] + nr[e, k]
                im = s[0] + s[1] + ni[e, k]
                sq[e] = re
                sq[count + e] = re + im
                sq[2 * count + e] = im - re

        for a in range(len(groups)):
            square([(i, j) for i in groups[a] for j in groups[a] if i < j])
            for b in range(a + 1, len(groups)):
                square([(i, j) for i in groups[a] for j in groups[b]])
        size = [None] * dates
        for e, (i, j) in enumerate(pairs):
            re, im = nr[e, k], ni[e, k]
            value = re * re + im * im
            size[i] = add_to(size[i], 1, value)
            size[j] = add_to(size[j], 1, value)
        for i in range(dates):
            sq[3 * count + i] = size[i] + 0.25

        turns = jnp.minimum(iter_ref[0], ITERS)
        odd_turns = turns % 2 == 1
        steps = jnp.where(odd_turns, turns // 2, turns // 2 - 1)

        def row_sums(re_of, im_of, own):
            sr, si = [own(i) for i in range(dates)], [None] * dates
            for e, (i, j) in enumerate(pairs):
                re, im = re_of(e), im_of(e)
                sr[i] = sr[i] + re
                sr[j] = sr[j] + re
                si[i] = add_to(si[i], 1, im)
                si[j] = add_to(si[j], -1, im)
            for i in range(dates):
                vec[i] = sr[i]
                vec[dates + i] = si[i]

        @pl.when(odd_turns)
        def _():
            row_sums(lambda e: nr[e, k], lambda e: ni[e, k],
                     lambda i: jnp.full((SUB, LANES), 0.5, jnp.float32))

        @pl.when(jnp.logical_not(odd_turns))
        def _():
            row_sums(lambda e: sq[e], lambda e: sq[count + e] - sq[e],
                     lambda i: sq[3 * count + i])

        def step(_, vectors):
            vr, vi = vectors[:dates], vectors[dates:]
            vs = [a + b for a, b in zip(vr, vi)]
            out_r, out_i = [], []
            for rows_in in groups:
                sums = {i: [None, None, None] for i in rows_in}
                for i in rows_in:
                    for j in range(dates):
                        if j == i or (j in rows_in and j < i):
                            continue
                        e = index[min(i, j), max(i, j)]
                        re, plus, minus = sq[e], sq[count + e], sq[2 * count + e]
                        s = sums[i]
                        if i < j:
                            s[0] = add_to(s[0], 1, re * vs[j])
                            s[1] = add_to(s[1], 1, minus * vr[j])
                            s[2] = add_to(s[2], 1, plus * vi[j])
                            if j in rows_in:
                                s = sums[j]
                                s[0] = add_to(s[0], 1, re * vs[i])
                                s[1] = add_to(s[1], -1, plus * vr[i])
                                s[2] = add_to(s[2], -1, minus * vi[i])
                        else:
                            s[0] = add_to(s[0], 1, re * vs[j])
                            s[1] = add_to(s[1], -1, plus * vr[j])
                            s[2] = add_to(s[2], -1, minus * vi[j])
                for i in rows_in:
                    own = sq[3 * count + i]
                    s = sums[i]
                    out_r.append(s[0] - s[2] + own * vr[i])
                    out_i.append(s[0] + s[1] + own * vi[i])
            return tuple(out_r + out_i)

        vectors = lax.fori_loop(0, steps, step, tuple(vec[i] for i in range(2 * dates)))
        length = None
        for part in vectors:
            length = add_to(length, 1, part * part)
        scale = lax.rsqrt(length)
        vr = [a * scale for a in vectors[:dates]]
        vi = [a * scale for a in vectors[dates:]]
        cr = ci = None
        for i in range(dates):
            zr, zi = z_ref[0, i, whole_k], z_ref[1, i, whole_k]
            cr = add_to(cr, 1, vr[i] * zr + vi[i] * zi)
            ci = add_to(ci, 1, vr[i] * zi - vi[i] * zr)
        comp_ref[0, place] = cr
        comp_ref[1, place] = ci
        for i in range(dates):
            link_ref[0, i, place] = vr[i]
            link_ref[1, i, place] = vi[i]
        return carry

    lax.fori_loop(first, last, one_vector, 0)


def inner_kernel(
    tiles, done, iter_ref, z_ref,
    nr_b, ni_b, part_ref, link_ref, comp_ref,
    band, split, inv, nr_a, ni_a, more, sq, vec,
):
    dates = z_ref.shape[1]
    places = [
        (nr, ni, k)
        for nr, ni in ((nr_a, ni_a), (nr_b, ni_b))
        for k in range(nr.shape[1])
    ]
    vectors = len(places)
    ext = vectors + 2 * HALF_ROWS
    pairs = pair_list(dates)
    count = len(pairs)
    index = {pair: e for e, pair in enumerate(pairs)}
    fill_band(band)

    def image(t):
        return [[z_ref[part, t, k] for k in range(ext)] for part in range(2)]

    def keep(at, field):
        heads = running(field[: 2 * HALF_ROWS])
        for k in range(HALF_ROWS):
            part_ref[at, k] = heads[HALF_ROWS + k]

    def fields(i, j):
        if i == j:
            power = power_of(image(i))
            keep(2 * count + i, power)
            return inner_sums(power)
        re, im = cross(image(i), image(j))
        e = index[i, j]
        keep(e, re)
        keep(count + e, im)
        return inner_sums(re), inner_sums(im)

    coherence(dates, vectors, fields, split, band, inv, places, side_masks(tiles))
    iterate(
        HALF_ROWS, HALF_ROWS + done, HALF_ROWS, dates, iter_ref, z_ref, nr_a, ni_a,
        more, sq, vec, link_ref, comp_ref, HALF_ROWS,
    )


def outer_kernel(
    tiles, iter_ref, z_ref, part_ref, x_ref, y_ref,
    link_ref, comp_ref, pack_x_ref, pack_y_ref,
    halo, band, split, inv, nr, ni, more, sq, vec,
):
    dates = z_ref.shape[1]
    top = upper()
    odd_device, edge = row_place()
    pairs = pair_list(dates)
    count = len(pairs)
    index = {pair: e for e, pair in enumerate(pairs)}
    fill_band(band)

    def fill(t, carry):
        for k in range(HALF_ROWS):
            a, b = x_ref[t, k], jnp.where(edge, 0.0, y_ref[t, k])
            re, im = unpack(jnp.where(odd_device, a, b), jnp.where(odd_device, b, a), top)
            halo[0, t, k] = re
            halo[1, t, k] = im
        return carry

    lax.fori_loop(0, dates, fill, 0)

    def image(t):
        return [[halo[part, t, k] for k in range(HALF_ROWS)] for part in range(2)]

    def add(at, field):
        tails = running(field)
        return [tails[HALF_ROWS - 1 - k] + part_ref[at, k] for k in range(HALF_ROWS)]

    def fields(i, j):
        if i == j:
            return add(2 * count + i, power_of(image(i)))
        re, im = cross(image(i), image(j))
        e = index[i, j]
        return add(e, re), add(count + e, im)

    places = [(nr, ni, k) for k in range(HALF_ROWS)]
    coherence(dates, HALF_ROWS, fields, split, band, inv, places, side_masks(tiles))
    iterate(
        0, HALF_ROWS, 0, dates, iter_ref, z_ref, nr, ni, more, sq, vec,
        link_ref, comp_ref,
    )
    for k in range(HALF_ROWS):
        first, second = pack(comp_ref[0, k], comp_ref[1, k], top)
        pack_x_ref[k] = jnp.where(odd_device, first, second)
        pack_y_ref[k] = jnp.where(odd_device, second, first)


def rest_kernel(
    start, iter_ref, z_ref, nr, ni, after_ref, link_ref, comp_ref,
    more, sq, vec,
):
    dates = z_ref.shape[1]
    iterate(
        start, start + comp_ref.shape[1], start, dates, iter_ref, z_ref, nr, ni,
        more, sq, vec, link_ref, comp_ref, start,
    )


def box_sum(field, lanes, edges):
    last_two, last_one, first_one, first_two = lanes
    keep_before, keep_after = edges
    out = []
    for x in inner_sums(field):
        before = jnp.where(keep_before, pltpu.roll(x, 1, 0), 0.0)
        after = jnp.where(keep_after, pltpu.roll(x, SUB - 1, 0), 0.0)
        near = pltpu.roll(jnp.where(last_one, before, x), 1, 1) + pltpu.roll(
            jnp.where(first_one, after, x), LANES - 1, 1
        )
        far = pltpu.roll(jnp.where(last_two, before, x), 2, 1) + pltpu.roll(
            jnp.where(first_two, after, x), LANES - 2, 1
        )
        out.append(x + near + far)
    return out


def masks(tiles):
    at = lane()
    lanes = (at >= LANES - 2, at >= LANES - 1, at < 1, at < 2)
    column = sublane() % tiles
    return lanes, (column != 0, column != tiles - 1)


def extend_kernel(outer_ref, inner_ref, rest_ref, x_ref, y_ref, out_ref):
    top = upper()
    odd_device, edge = row_place()
    for k in range(HALF_ROWS):
        a, b = x_ref[k], jnp.where(edge, 0.0, y_ref[k])
        re, im = unpack(jnp.where(odd_device, a, b), jnp.where(odd_device, b, a), top)
        out_ref[0, HALF_ROWS - 1 - k] = re
        out_ref[1, HALF_ROWS - 1 - k] = im
    for part in range(2):
        at = HALF_ROWS
        for ref in (outer_ref, inner_ref, rest_ref):
            for k in range(ref.shape[1]):
                out_ref[part, at] = ref[part, k]
                at += 1


def offsets_kernel(
    tiles, own_ref, a_ref, b_ref, unit_ref, total_ref
):
    lanes, edges = masks(tiles)
    half = unit_ref.shape[1]
    place = lax.axis_index("tm")
    odd_stack = place % 2 == 1
    first_stack = place == 0

    def whole(*refs):
        parts = []
        for part in range(2):
            rows_in = [ref[part, k] for ref in refs for k in range(ref.shape[1])]
            rows_in += [flip(rows_in[-1 - k]) for k in range(HALF_ROWS)]
            parts.append(rows_in)
        return parts

    def power(re, im):
        return box_sum([a * a + b * b for a, b in zip(re, im)], lanes, edges)

    own_r, own_i = whole(own_ref)
    own = [p + 1.0 for p in power(own_r, own_i)]

    def unit(*refs):
        re, im = whole(*refs)
        other = power(re, im)
        cross_r = box_sum(
            [a * c + b * d for a, b, c, d in zip(own_r, own_i, re, im)], lanes, edges
        )
        cross_i = box_sum(
            [b * c - a * d for a, b, c, d in zip(own_r, own_i, re, im)], lanes, edges
        )
        out = []
        for k in range(half):
            scale = lax.rsqrt(own[k] * (other[k] + 1.0))
            off_r, off_i = cross_r[k] * scale, cross_i[k] * scale
            bound = jnp.maximum(jnp.sqrt(off_r * off_r + off_i * off_i), LINK_FLOOR)
            back = 1.0 / bound
            out.append((off_r * back, off_i * back))
        return out

    pair_a, pair_b = unit(a_ref), unit(b_ref)
    for k in range(half):
        (ar, ai), (br, bi) = pair_a[k], pair_b[k]
        before_r = jnp.where(odd_stack, ar, br)
        before_i = -jnp.where(odd_stack, ai, bi)
        after_r = jnp.where(odd_stack, br, ar)
        after_i = jnp.where(odd_stack, bi, ai)
        before_r = jnp.where(first_stack, 1.0, before_r)
        before_i = jnp.where(first_stack, 0.0, before_i)
        unit_ref[0, k] = before_r
        unit_ref[1, k] = before_i
        total_ref[0, k] = before_r * after_r - before_i * after_i
        total_ref[1, k] = before_r * after_i + before_i * after_r


def result_kernel(
    rows, tiles, chosen_ref, outer_ref, inner_ref, rest_ref, datum_ref, out_hbm,
    out_ref, turn, sems,
):
    half = rows // 2
    parts = (outer_ref, inner_ref, rest_ref)
    links = [(ref, k) for ref in parts for k in range(ref.shape[2])]
    dates = outer_ref.shape[1]

    chosen = chosen_ref[0]
    for k, (ref, at) in enumerate(links):
        vr = ref[0, chosen, at] * float(dates)
        vi = ref[1, chosen, at] * float(dates)
        dr, di = datum_ref[0, k], datum_ref[1, k]
        turn[0, k] = dr * vr + di * vi
        turn[1, k] = di * vr - dr * vi

    def copies(t):
        return [
            pltpu.make_async_copy(out_ref.at[part, t], out_hbm.at[part, t], sems.at[part, t])
            for part in range(2)
        ]

    def one_date(t, carry):
        for k in range(half):
            ref, at = links[k]
            lr, li = ref[0, t, at], ref[1, t, at]
            dr, di = turn[0, k], turn[1, k]
            first, second = bases(k, rows, tiles)
            for part, value in enumerate((lr * dr - li * di, lr * di + li * dr)):
                out_ref[part, t, pl.ds(first, tiles, stride=SUB), :] = value[:tiles]
                out_ref[part, t, pl.ds(second, tiles, stride=SUB), :] = value[tiles:]
        for copy in copies(t):
            copy.start()
        return carry

    lax.fori_loop(0, dates, one_date, 0)
    for t in range(dates):
        for copy in copies(t):
            copy.wait()


def swaps(count, bit=None, odd=False):
    if bit is not None:
        return [(i, i ^ bit) for i in range(count)]
    if odd:
        return [(i, (i + 1 if i % 2 else i - 1) % count) for i in range(count)]
    return [(i, i ^ 1) for i in range(count)]


def inner_swaps(count):
    pairs = [(i, i + 1) for i in range(1, count - 1, 2)]
    return pairs + [(j, i) for i, j in pairs]


def times(a, b):
    return jnp.stack([a[0] * b[0] - a[1] * b[1], a[0] * b[1] + a[1] * b[0]])


def linked_phases(amplitude, phase, validity, iterations, reference_date):
    dates, rows, columns = amplitude.shape
    half = rows // 2
    tiles = columns // LANES
    ext = half + HALF_ROWS
    members = lax.axis_size("tm")
    blocks = lax.axis_size("space")
    place = lax.axis_index("tm")
    params = pltpu.CompilerParams(vmem_limit_bytes=VMEM_LIMIT)

    def shape(*dims):
        return jax.ShapeDtypeStruct(dims, jnp.float32)

    def tiled(x):
        lead = x.shape[:-2]
        x = x.reshape(lead + (rows // SUB, SUB, tiles, LANES))
        return jnp.swapaxes(x, -3, -2).reshape(lead + (rows * tiles, LANES))

    def far_memory(x):
        return pltpu.with_memory_space_constraint(x, pltpu.MemorySpace.HBM)

    z, slab_x, slab_y = pl.pallas_call(
        lambda *refs: images_kernel(rows, tiles, *refs),
        out_shape=(
            shape(2, dates, ext, SUB, LANES),
            shape(dates, HALF_ROWS, SUB, LANES),
            shape(dates, HALF_ROWS, SUB, LANES),
        ),
        in_specs=[hbm(), hbm(), hbm()],
        out_specs=(vmem(), vmem(), vmem()),
        scratch_shapes=[
            pltpu.VMEM((dates, rows * tiles, LANES), jnp.float32),
            pltpu.VMEM((dates, rows * tiles, LANES), jnp.float32),
            pltpu.VMEM((rows * tiles, LANES), jnp.int32),
            pltpu.SemaphoreType.DMA((3, dates)),
        ],
        compiler_params=params,
        name="images",
    )(*(far_memory(tiled(x)) for x in (amplitude, phase, validity)))
    pair_x, pair_y = swaps(blocks), swaps(blocks, odd=True)
    got_y = lax.ppermute(slab_y, "space", pair_y)
    got_x = lax.ppermute(slab_x, "space", pair_x)

    count = dates * (dates - 1) // 2
    inner = half - HALF_ROWS
    done = min(INNER_DONE, inner - 1)
    work = [
        pltpu.VMEM((2 * count, SUB, LANES), jnp.float32),
        pltpu.VMEM((3 * count + dates, SUB, LANES), jnp.float32),
        pltpu.VMEM((2 * dates, SUB, LANES), jnp.float32),
    ]

    def window_work(vectors):
        return [
            pltpu.VMEM((2 * LANES, 2 * LANES), jnp.bfloat16),
            pltpu.VMEM((dates // 2 + count, 2 * vectors * SUB, 2 * LANES), jnp.bfloat16),
            pltpu.VMEM((dates, vectors, SUB, LANES), jnp.float32),
        ]

    def cost(vectors):
        return pl.CostEstimate(
            flops=vectors * 2_000_000 * 8, bytes_accessed=1 << 20, transcendentals=0
        )

    nr, ni, part, linked_a, comp_a = pl.pallas_call(
        lambda *refs: inner_kernel(tiles, done, *refs),
        out_shape=(
            shape(count, inner - done, SUB, LANES),
            shape(count, inner - done, SUB, LANES),
            shape(2 * count + dates, HALF_ROWS, SUB, LANES),
            shape(2, dates, done, SUB, LANES),
            shape(2, done, SUB, LANES),
        ),
        in_specs=[smem(), vmem()],
        out_specs=(vmem(),) * 5,
        scratch_shapes=window_work(inner)
        + [pltpu.VMEM((count, done, SUB, LANES), jnp.float32)] * 2
        + work,
        compiler_params=params,
        cost_estimate=cost(4),
        name="inner",
    )(iterations, z)
    linked_b, comp_b, pack_x, pack_y = pl.pallas_call(
        lambda *refs: outer_kernel(tiles, *refs),
        out_shape=(
            shape(2, dates, HALF_ROWS, SUB, LANES),
            shape(2, HALF_ROWS, SUB, LANES),
            shape(HALF_ROWS, SUB, LANES),
            shape(HALF_ROWS, SUB, LANES),
        ),
        in_specs=[smem()] + [vmem()] * 4,
        out_specs=(vmem(),) * 4,
        scratch_shapes=[pltpu.VMEM((2, dates, HALF_ROWS, SUB, LANES), jnp.float32)]
        + window_work(HALF_ROWS)
        + [
            pltpu.VMEM((count, HALF_ROWS, SUB, LANES), jnp.float32),
            pltpu.VMEM((count, HALF_ROWS, SUB, LANES), jnp.float32),
        ]
        + work,
        compiler_params=params,
        cost_estimate=cost(7),
        name="outer",
    )(iterations, z, part, got_x, got_y)
    more_y = lax.ppermute(pack_y, "space", pair_y)
    more_x = lax.ppermute(pack_x, "space", pair_x)

    start = HALF_ROWS + done
    linked_c, comp_c = pl.pallas_call(
        lambda *refs: rest_kernel(start, *refs),
        out_shape=(
            shape(2, dates, half - start, SUB, LANES),
            shape(2, half - start, SUB, LANES),
        ),
        in_specs=[smem()] + [vmem()] * 4,
        out_specs=(vmem(),) * 2,
        scratch_shapes=work,
        compiler_params=params,
        cost_estimate=cost(5),
        name="rest",
    )(iterations, z, nr, ni, pack_x)
    wide = pl.pallas_call(
        extend_kernel,
        out_shape=shape(2, ext, SUB, LANES),
        in_specs=[vmem()] * 5,
        out_specs=vmem(),
        compiler_params=params,
        name="extend",
    )(comp_b, comp_a, comp_c, more_x, more_y)
    other_a = lax.ppermute(wide, "tm", swaps(members))
    other_b = lax.ppermute(wide, "tm", inner_swaps(members))
    datum, total = pl.pallas_call(
        lambda *refs: offsets_kernel(tiles, *refs),
        out_shape=(shape(2, half, SUB, LANES), shape(2, half, SUB, LANES)),
        in_specs=[vmem()] * 3,
        out_specs=(vmem(), vmem()),
        compiler_params=params,
        name="offsets",
    )(wide, other_a, other_b)
    bit = 2
    while bit < members:
        other = lax.ppermute(total, "tm", swaps(members, bit=2 * bit - 2))
        datum = jnp.where((place & bit) != 0, times(datum, other), datum)
        total = times(total, other)
        bit *= 2
    out = pl.pallas_call(
        lambda *refs: result_kernel(rows, tiles, *refs),
        out_shape=shape(2, dates, rows * tiles, LANES),
        in_specs=[smem()] + [vmem()] * 4,
        out_specs=hbm(),
        scratch_shapes=[
            pltpu.VMEM((2, dates, rows * tiles, LANES), jnp.float32),
            pltpu.VMEM((2, half, SUB, LANES), jnp.float32),
            pltpu.SemaphoreType.DMA((2, dates)),
        ],
        compiler_params=params,
        name="result",
    )(reference_date, linked_b, linked_a, linked_c, datum)
    out = out.reshape(2, dates, rows // SUB, tiles, SUB, LANES)
    return jnp.swapaxes(out, -3, -2).reshape(2, dates, rows, columns)


def solution(mesh):
    return jax.shard_map(
        linked_phases,
        mesh=mesh,
        in_specs=(
            P("tm", "space", None),
            P("tm", "space", None),
            P("space", None),
            P("tm"),
            P("tm"),
        ),
        out_specs=P(None, "tm", "space", None),
        check_vma=False,
    )
```

```python
import jax
import jax.numpy as jnp
from jax import lax
from jax.experimental import pallas as pl
from jax.experimental.pallas import tpu as pltpu
from jax.sharding import PartitionSpec as P


WIN_ROWS = 11
WIN_COLS = 5
INNER_DONE = 3
PIECE = 2
ITERS = 20
HALF_ROWS = WIN_ROWS // 2

MASKED_WEIGHT = 0.125
LINK_FLOOR = 0.03

LANES = 128
SUB = 8
VMEM_LIMIT = 40 * 1024 * 1024


def vmem():
    return pl.BlockSpec(memory_space=pltpu.VMEM)


def hbm():
    return pl.BlockSpec(memory_space=pltpu.MemorySpace.HBM)


def smem():
    return pl.BlockSpec(memory_space=pltpu.SMEM)


def sublane():
    return lax.broadcasted_iota(jnp.int32, (SUB, LANES), 0)


def lane():
    return lax.broadcasted_iota(jnp.int32, (SUB, LANES), 1)


def row_place():
    at = lax.axis_index("space")
    return at % 2 == 1, (at == 0) | (at == lax.axis_size("space") - 1)


def flip(x):
    return pltpu.roll(x, SUB // 2, 0)


def upper():
    return sublane() < SUB // 2


def bases(k, rows, tiles):
    def base(row):
        return (row // SUB) * SUB * tiles + row % SUB

    return base(k), base(rows - 1 - k)


def load_pair(ref, lead, k, rows, tiles, top):
    first, second = bases(k, rows, tiles)
    a = ref[lead + (pl.ds(first, SUB, stride=SUB), slice(None))]
    b = ref[lead + (pl.ds(second - SUB * tiles, SUB, stride=SUB), slice(None))]
    return jnp.where(top, a, b)


def sin_cos(x):
    turns = jnp.round(x * (2.0 / jnp.pi))
    r = (x - turns * 1.5707855224609375) - turns * 1.0804334124e-05
    s = r * r
    sine = r + r * s * (-1.6666654611e-1 + s * (8.3321608736e-3 + s * -1.9515295891e-4))
    cosine = 1.0 - 0.5 * s + s * s * (
        4.166664568298827e-2 + s * (-1.388731625493765e-3 + s * 2.443315711809948e-5)
    )
    size = jnp.abs(turns)
    odd = size == 1.0
    base_s = jnp.where(odd, cosine, sine)
    base_c = jnp.where(odd, sine, cosine)
    sin_x = jnp.where((turns == -1.0) | (size == 2.0), -base_s, base_s)
    cos_x = jnp.where((turns == 1.0) | (size == 2.0), -base_c, base_c)
    return sin_x, cos_x


def images_kernel(
    rows, tiles, amp_hbm, phase_hbm, valid_hbm, z_ref, x_ref, y_ref,
    amp_ref, phase_ref, valid_ref, sems,
):
    half = rows // 2
    dates = z_ref.shape[1]
    top = upper()
    odd, _ = row_place()
    step = PIECE if dates % PIECE == 0 else dates
    copies = []
    for p in range(dates // step):
        part = pl.ds(p * step, step)
        copies.append(
            [
                pltpu.make_async_copy(amp_hbm.at[part], amp_ref.at[part], sems.at[0, p]),
                pltpu.make_async_copy(phase_hbm.at[part], phase_ref.at[part], sems.at[1, p]),
            ]
        )
    weights = pltpu.make_async_copy(valid_hbm, valid_ref, sems.at[2, 0])
    weights.start()
    for pair in copies:
        for copy in pair:
            copy.start()
    weights.wait()
    roots = []
    for k in range(half):
        valid = load_pair(valid_ref, (), k, rows, tiles, top)
        roots.append(jnp.where(valid == 1, 1.0, MASKED_WEIGHT**0.5).astype(jnp.float32))

    def one_date(t, carry):
        for k in range(half):
            amp = load_pair(amp_ref, (t,), k, rows, tiles, top) * roots[k]
            sin_x, cos_x = sin_cos(load_pair(phase_ref, (t,), k, rows, tiles, top))
            re, im = amp * cos_x, amp * sin_x
            z_ref[0, t, k] = re
            z_ref[1, t, k] = im
            if k >= half - HALF_ROWS:
                z_ref[0, t, 2 * half - 1 - k] = flip(re)
                z_ref[1, t, 2 * half - 1 - k] = flip(im)
            if k < HALF_ROWS:
                first, second = pack(re, im, top)
                x_ref[t, k] = jnp.where(odd, first, second)
                y_ref[t, k] = jnp.where(odd, second, first)
        return carry

    for p, pair in enumerate(copies):
        for copy in pair:
            copy.wait()
        lax.fori_loop(p * step, (p + 1) * step, one_date, 0)


def unpack(first, second, top):
    return jnp.where(top, first, flip(second)), jnp.where(top, flip(first), second)


def pack(re, im, top):
    return jnp.where(top, re, flip(im)), jnp.where(top, flip(re), im)


def add_to(total, sign, value):
    if total is None:
        return value if sign > 0 else -value
    return total + value if sign > 0 else total - value


def running(values):
    out = [values[0]]
    for value in values[1:]:
        out.append(out[-1] + value)
    return out


def inner_sums(field):
    count = len(field) - WIN_ROWS + 1
    tails = running(field[WIN_ROWS - 1 :: -1])[::-1]
    if count <= WIN_ROWS:
        core = running(field[count - 1 : WIN_ROWS])[-1]
        tails = running([core] + field[: count - 1][::-1])[::-1]
    heads = running(field[WIN_ROWS:])
    middle = [tails[q] + heads[q - 1] for q in range(1, min(count, WIN_ROWS))]
    return [tails[0]] + middle + heads[WIN_ROWS - 1 :]


def fill_band(band_ref):
    at = lax.broadcasted_iota(jnp.int32, band_ref.shape, 0) % LANES
    to = lax.broadcasted_iota(jnp.int32, band_ref.shape, 1)
    reach = WIN_COLS // 2
    inside = (to < LANES) & (jnp.abs(at - to) <= reach)
    to = to - LANES
    beside = (to >= 0) & ((at >= to + LANES - reach) | (at <= to - LANES + reach))
    band_ref[...] = jnp.where(inside | beside, 1.0, 0.0).astype(band_ref.dtype)


def put_split(ref, at, vectors):
    x = jnp.concatenate(vectors, axis=0)
    high = x.astype(jnp.bfloat16)
    low = (x - high.astype(jnp.float32)).astype(jnp.bfloat16)
    ref[at, :, :LANES] = high
    ref[at, :, LANES:] = low


def side_masks(tiles):
    column = sublane() % tiles
    at = lane()
    return (at < LANES // 2) & (column != 0), (at >= LANES // 2) & (column != tiles - 1)


def column_sums(split_ref, first, size, band, sides):
    rows = split_ref.shape[1]
    terms = split_ref[first : first + size].reshape(size * rows, 2 * LANES)
    both = jnp.dot(terms, band, preferred_element_type=jnp.float32)
    from_before, from_after = sides
    out = []
    for k in range(size * rows // SUB):
        inside = both[k * SUB : (k + 1) * SUB, :LANES]
        beside = both[k * SUB : (k + 1) * SUB, LANES:]
        before, after = pltpu.roll(beside, 1, 0), pltpu.roll(beside, SUB - 1, 0)
        out.append(
            inside + jnp.where(from_before, before, jnp.where(from_after, after, 0.0))
        )
    return out


def pair_list(dates):
    return [(i, j) for i in range(dates) for j in range(i + 1, dates)]


CHUNK = 5


def coherence(dates, vectors, fields, split_ref, band_ref, inv_ref, places, sides):
    pairs = pair_list(dates)
    band = band_ref[...]
    powers = [fields(i, i) for i in range(dates)]
    half = dates // 2
    for e in range(half):
        put_split(split_ref, e, powers[2 * e] + powers[2 * e + 1])
    sums = column_sums(split_ref, 0, half, band, sides)
    for i in range(dates):
        for k in range(vectors):
            inv_ref[i, k] = lax.rsqrt(sums[i * vectors + k]) * 0.5
    for first in range(0, len(pairs), CHUNK):
        size = min(CHUNK, len(pairs) - first)
        for e in range(first, first + size):
            re, im = fields(*pairs[e])
            put_split(split_ref, half + e, re + im)
        sums = column_sums(split_ref, half + first, size, band, sides)
        for e in range(first, first + size):
            i, j = pairs[e]
            base = (e - first) * 2 * vectors
            for k in range(vectors):
                scale = inv_ref[i, k] * inv_ref[j, k]
                nr_ref, ni_ref, at = places[k]
                nr_ref[e, at] = sums[base + k] * scale
                ni_ref[e, at] = sums[base + vectors + k] * scale


def cross(a, b):
    (ar, ai), (br, bi) = a, b
    re = [p * r + q * s for p, q, r, s in zip(ar, ai, br, bi)]
    im = [q * r - p * s for p, q, r, s in zip(ar, ai, br, bi)]
    return re, im


def power_of(a):
    return [p * p + q * q for p, q in zip(*a)]


def iterate(
    first, last, offset, dates, iter_ref, z_ref, nr, ni, more, sq, vec,
    link_ref, comp_ref, out_offset=0,
):
    pairs = pair_list(dates)
    index = {pair: e for e, pair in enumerate(pairs)}
    count = len(pairs)
    groups = []
    at = 0
    for size in (3, 3, 4) if dates == 10 else (dates,):
        groups.append(tuple(range(at, at + size)))
        at += size

    def one_vector(whole_k, carry):
        k = whole_k - offset
        place = whole_k - out_offset
        for e in range(count):
            re, im = nr[e, k], ni[e, k]
            more[e] = re + im
            more[count + e] = im - re

        def left(i, t):
            if i < t:
                e = index[i, t]
                return (nr[e, k], 1), (more[e], 1), (more[count + e], 1)
            e = index[t, i]
            return (nr[e, k], 1), (more[count + e], -1), (more[e], -1)

        def right(t, j):
            if t < j:
                e = index[t, j]
                return (nr[e, k], 1), (ni[e, k], 1), (more[e], 1)
            e = index[j, t]
            return (nr[e, k], 1), (ni[e, k], -1), (more[count + e], -1)

        def square(out):
            sums = {pair: [None, None, None] for pair in out}
            rows_in = sorted({i for i, _ in out})
            cols_in = sorted({j for _, j in out})
            for t in range(dates):
                lefts = {i: left(i, t) for i in rows_in if i != t}
                rights = {j: right(t, j) for j in cols_in if j != t}
                for i, j in out:
                    if t in (i, j):
                        continue
                    (ar, _), (ap, sap), (aq, saq) = lefts[i]
                    (br, _), (bi, sbi), (bs, sbs) = rights[j]
                    s = sums[i, j]
                    s[0] = add_to(s[0], sbs, ar * bs)
                    s[1] = add_to(s[1], saq, aq * br)
                    s[2] = add_to(s[2], sap * sbi, ap * bi)
            for i, j in out:
                e = index[i, j]
                s = sums[i, j]
                re = s[0] - s[2] + nr[e, k]
                im = s[0] + s[1] + ni[e, k]
                sq[e] = re
                sq[count + e] = re + im
                sq[2 * count + e] = im - re

        for a in range(len(groups)):
            square([(i, j) for i in groups[a] for j in groups[a] if i < j])
            for b in range(a + 1, len(groups)):
                square([(i, j) for i in groups[a] for j in groups[b]])
        size = [None] * dates
        for e, (i, j) in enumerate(pairs):
            re, im = nr[e, k], ni[e, k]
            value = re * re + im * im
            size[i] = add_to(size[i], 1, value)
            size[j] = add_to(size[j], 1, value)
        for i in range(dates):
            sq[3 * count + i] = size[i] + 0.25

        turns = jnp.minimum(iter_ref[0], ITERS)
        odd_turns = turns % 2 == 1
        steps = jnp.where(odd_turns, turns // 2, turns // 2 - 1)

        def row_sums(re_of, im_of, own):
            sr, si = [own(i) for i in range(dates)], [None] * dates
            for e, (i, j) in enumerate(pairs):
                re, im = re_of(e), im_of(e)
                sr[i] = sr[i] + re
                sr[j] = sr[j] + re
                si[i] = add_to(si[i], 1, im)
                si[j] = add_to(si[j], -1, im)
            for i in range(dates):
                vec[i] = sr[i]
                vec[dates + i] = si[i]

        @pl.when(odd_turns)
        def _():
            row_sums(lambda e: nr[e, k], lambda e: ni[e, k],
                     lambda i: jnp.full((SUB, LANES), 0.5, jnp.float32))

        @pl.when(jnp.logical_not(odd_turns))
        def _():
            row_sums(lambda e: sq[e], lambda e: sq[count + e] - sq[e],
                     lambda i: sq[3 * count + i])

        def step(_, vectors):
            vr, vi = vectors[:dates], vectors[dates:]
            vs = [a + b for a, b in zip(vr, vi)]
            out_r, out_i = [], []
            for rows_in in groups:
                sums = {i: [None, None, None] for i in rows_in}
                for i in rows_in:
                    for j in range(dates):
                        if j == i or (j in rows_in and j < i):
                            continue
                        e = index[min(i, j), max(i, j)]
                        re, plus, minus = sq[e], sq[count + e], sq[2 * count + e]
                        s = sums[i]
                        if i < j:
                            s[0] = add_to(s[0], 1, re * vs[j])
                            s[1] = add_to(s[1], 1, minus * vr[j])
                            s[2] = add_to(s[2], 1, plus * vi[j])
                            if j in rows_in:
                                s = sums[j]
                                s[0] = add_to(s[0], 1, re * vs[i])
                                s[1] = add_to(s[1], -1, plus * vr[i])
                                s[2] = add_to(s[2], -1, minus * vi[i])
                        else:
                            s[0] = add_to(s[0], 1, re * vs[j])
                            s[1] = add_to(s[1], -1, plus * vr[j])
                            s[2] = add_to(s[2], -1, minus * vi[j])
                for i in rows_in:
                    own = sq[3 * count + i]
                    s = sums[i]
                    out_r.append(s[0] - s[2] + own * vr[i])
                    out_i.append(s[0] + s[1] + own * vi[i])
            return tuple(out_r + out_i)

        vectors = lax.fori_loop(0, steps, step, tuple(vec[i] for i in range(2 * dates)))
        length = None
        for part in vectors:
            length = add_to(length, 1, part * part)
        scale = lax.rsqrt(length)
        vr = [a * scale for a in vectors[:dates]]
        vi = [a * scale for a in vectors[dates:]]
        cr = ci = None
        for i in range(dates):
            zr, zi = z_ref[0, i, whole_k], z_ref[1, i, whole_k]
            cr = add_to(cr, 1, vr[i] * zr + vi[i] * zi)
            ci = add_to(ci, 1, vr[i] * zi - vi[i] * zr)
        comp_ref[0, place] = cr
        comp_ref[1, place] = ci
        for i in range(dates):
            link_ref[0, i, place] = vr[i]
            link_ref[1, i, place] = vi[i]
        return carry

    lax.fori_loop(first, last, one_vector, 0)


def inner_kernel(
    tiles, done, iter_ref, z_ref,
    nr_b, ni_b, part_ref, link_ref, comp_ref,
    band, split, inv, nr_a, ni_a, more, sq, vec,
):
    dates = z_ref.shape[1]
    places = [
        (nr, ni, k)
        for nr, ni in ((nr_a, ni_a), (nr_b, ni_b))
        for k in range(nr.shape[1])
    ]
    vectors = len(places)
    ext = vectors + 2 * HALF_ROWS
    pairs = pair_list(dates)
    count = len(pairs)
    index = {pair: e for e, pair in enumerate(pairs)}
    fill_band(band)

    def image(t):
        return [[z_ref[part, t, k] for k in range(ext)] for part in range(2)]

    def keep(at, field):
        heads = running(field[: 2 * HALF_ROWS])
        for k in range(HALF_ROWS):
            part_ref[at, k] = heads[HALF_ROWS + k]

    def fields(i, j):
        if i == j:
            power = power_of(image(i))
            keep(2 * count + i, power)
            return inner_sums(power)
        re, im = cross(image(i), image(j))
        e = index[i, j]
        keep(e, re)
        keep(count + e, im)
        return inner_sums(re), inner_sums(im)

    coherence(dates, vectors, fields, split, band, inv, places, side_masks(tiles))
    iterate(
        HALF_ROWS, HALF_ROWS + done, HALF_ROWS, dates, iter_ref, z_ref, nr_a, ni_a,
        more, sq, vec, link_ref, comp_ref, HALF_ROWS,
    )


def outer_kernel(
    tiles, iter_ref, z_ref, part_ref, x_ref, y_ref,
    link_ref, comp_ref, pack_x_ref, pack_y_ref,
    halo, band, split, inv, nr, ni, more, sq, vec,
):
    dates = z_ref.shape[1]
    top = upper()
    odd_device, edge = row_place()
    pairs = pair_list(dates)
    count = len(pairs)
    index = {pair: e for e, pair in enumerate(pairs)}
    fill_band(band)

    def fill(t, carry):
        for k in range(HALF_ROWS):
            a, b = x_ref[t, k], jnp.where(edge, 0.0, y_ref[t, k])
            re, im = unpack(jnp.where(odd_device, a, b), jnp.where(odd_device, b, a), top)
            halo[0, t, k] = re
            halo[1, t, k] = im
        return carry

    lax.fori_loop(0, dates, fill, 0)

    def image(t):
        return [[halo[part, t, k] for k in range(HALF_ROWS)] for part in range(2)]

    def add(at, field):
        tails = running(field)
        return [tails[HALF_ROWS - 1 - k] + part_ref[at, k] for k in range(HALF_ROWS)]

    def fields(i, j):
        if i == j:
            return add(2 * count + i, power_of(image(i)))
        re, im = cross(image(i), image(j))
        e = index[i, j]
        return add(e, re), add(count + e, im)

    places = [(nr, ni, k) for k in range(HALF_ROWS)]
    coherence(dates, HALF_ROWS, fields, split, band, inv, places, side_masks(tiles))
    iterate(
        0, HALF_ROWS, 0, dates, iter_ref, z_ref, nr, ni, more, sq, vec,
        link_ref, comp_ref,
    )
    for k in range(HALF_ROWS):
        first, second = pack(comp_ref[0, k], comp_ref[1, k], top)
        pack_x_ref[k] = jnp.where(odd_device, first, second)
        pack_y_ref[k] = jnp.where(odd_device, second, first)


def rest_kernel(
    start, iter_ref, z_ref, nr, ni, after_ref, link_ref, comp_ref,
    more, sq, vec,
):
    dates = z_ref.shape[1]
    iterate(
        start, start + comp_ref.shape[1], start, dates, iter_ref, z_ref, nr, ni,
        more, sq, vec, link_ref, comp_ref, start,
    )


def box_sum(field, lanes, edges):
    last_two, last_one, first_one, first_two = lanes
    keep_before, keep_after = edges
    out = []
    for x in inner_sums(field):
        before = jnp.where(keep_before, pltpu.roll(x, 1, 0), 0.0)
        after = jnp.where(keep_after, pltpu.roll(x, SUB - 1, 0), 0.0)
        near = pltpu.roll(jnp.where(last_one, before, x), 1, 1) + pltpu.roll(
            jnp.where(first_one, after, x), LANES - 1, 1
        )
        far = pltpu.roll(jnp.where(last_two, before, x), 2, 1) + pltpu.roll(
            jnp.where(first_two, after, x), LANES - 2, 1
        )
        out.append(x + near + far)
    return out


def masks(tiles):
    at = lane()
    lanes = (at >= LANES - 2, at >= LANES - 1, at < 1, at < 2)
    column = sublane() % tiles
    return lanes, (column != 0, column != tiles - 1)


def extend_kernel(outer_ref, inner_ref, rest_ref, x_ref, y_ref, out_ref):
    top = upper()
    odd_device, edge = row_place()
    for k in range(HALF_ROWS):
        a, b = x_ref[k], jnp.where(edge, 0.0, y_ref[k])
        re, im = unpack(jnp.where(odd_device, a, b), jnp.where(odd_device, b, a), top)
        out_ref[0, HALF_ROWS - 1 - k] = re
        out_ref[1, HALF_ROWS - 1 - k] = im
    for part in range(2):
        at = HALF_ROWS
        for ref in (outer_ref, inner_ref, rest_ref):
            for k in range(ref.shape[1]):
                out_ref[part, at] = ref[part, k]
                at += 1


def offsets_kernel(
    tiles, own_ref, a_ref, b_ref, unit_ref, total_ref
):
    lanes, edges = masks(tiles)
    half = unit_ref.shape[1]
    place = lax.axis_index("tm")
    odd_stack = place % 2 == 1
    no_second = place == 1

    def whole(*refs):
        parts = []
        for part in range(2):
            rows_in = [ref[part, k] for ref in refs for k in range(ref.shape[1])]
            rows_in += [flip(rows_in[-1 - k]) for k in range(HALF_ROWS)]
            parts.append(rows_in)
        return parts

    def power(re, im):
        return box_sum([a * a + b * b for a, b in zip(re, im)], lanes, edges)

    images = [whole(ref) for ref in (own_ref, a_ref, b_ref)]
    powers = [[p + 1.0 for p in power(*image)] for image in images]

    def unit(one, two):
        (ar, ai), (br, bi) = images[one], images[two]
        cross_r = box_sum([p * r + q * s for p, q, r, s in zip(ar, ai, br, bi)], lanes, edges)
        cross_i = box_sum([q * r - p * s for p, q, r, s in zip(ar, ai, br, bi)], lanes, edges)
        out = []
        for k in range(half):
            scale = lax.rsqrt(powers[one][k] * powers[two][k])
            off_r, off_i = cross_r[k] * scale, cross_i[k] * scale
            bound = jnp.maximum(jnp.sqrt(off_r * off_r + off_i * off_i), LINK_FLOOR)
            back = 1.0 / bound
            out.append((off_r * back, off_i * back))
        return out

    near, far = unit(0, 1), unit(1, 2)
    for k in range(half):
        (nr, ni), (fr, fi) = near[k], far[k]
        fr = jnp.where(no_second, 1.0, fr)
        fi = jnp.where(no_second, 0.0, fi)
        re = nr * fr - ni * fi
        im = nr * fi + ni * fr
        im = jnp.where(odd_stack, -im, im)
        total_ref[0, k] = re
        total_ref[1, k] = im
        unit_ref[0, k] = jnp.where(odd_stack, re, 1.0)
        unit_ref[1, k] = jnp.where(odd_stack, im, 0.0)


def result_kernel(
    rows, tiles, chosen_ref, outer_ref, inner_ref, rest_ref, datum_ref, out_hbm,
    out_ref, turn, sems,
):
    half = rows // 2
    parts = (outer_ref, inner_ref, rest_ref)
    links = [(ref, k) for ref in parts for k in range(ref.shape[2])]
    dates = outer_ref.shape[1]

    chosen = chosen_ref[0]
    for k, (ref, at) in enumerate(links):
        vr = ref[0, chosen, at] * float(dates)
        vi = ref[1, chosen, at] * float(dates)
        dr, di = datum_ref[0, k], datum_ref[1, k]
        turn[0, k] = dr * vr + di * vi
        turn[1, k] = di * vr - dr * vi

    def copies(t):
        return [
            pltpu.make_async_copy(out_ref.at[part, t], out_hbm.at[part, t], sems.at[part, t])
            for part in range(2)
        ]

    def one_date(t, carry):
        for k in range(half):
            ref, at = links[k]
            lr, li = ref[0, t, at], ref[1, t, at]
            dr, di = turn[0, k], turn[1, k]
            first, second = bases(k, rows, tiles)
            for part, value in enumerate((lr * dr - li * di, lr * di + li * dr)):
                out_ref[part, t, pl.ds(first, tiles, stride=SUB), :] = value[:tiles]
                out_ref[part, t, pl.ds(second, tiles, stride=SUB), :] = value[tiles:]
        for copy in copies(t):
            copy.start()
        return carry

    lax.fori_loop(0, dates, one_date, 0)
    for t in range(dates):
        for copy in copies(t):
            copy.wait()


def swaps(count, bit=None, odd=False):
    if bit is not None:
        return [(i, i ^ bit) for i in range(count)]
    if odd:
        return [(i, (i + 1 if i % 2 else i - 1) % count) for i in range(count)]
    return [(i, i ^ 1) for i in range(count)]


def strides(count):
    return [(i, (i + 2 if i % 2 else i - 2) % count) for i in range(count)]


def times(a, b):
    return jnp.stack([a[0] * b[0] - a[1] * b[1], a[0] * b[1] + a[1] * b[0]])


def linked_phases(amplitude, phase, validity, iterations, reference_date):
    dates, rows, columns = amplitude.shape
    half = rows // 2
    tiles = columns // LANES
    ext = half + HALF_ROWS
    members = lax.axis_size("tm")
    blocks = lax.axis_size("space")
    place = lax.axis_index("tm")
    params = pltpu.CompilerParams(vmem_limit_bytes=VMEM_LIMIT)

    def shape(*dims):
        return jax.ShapeDtypeStruct(dims, jnp.float32)

    def tiled(x):
        lead = x.shape[:-2]
        x = x.reshape(lead + (rows // SUB, SUB, tiles, LANES))
        return jnp.swapaxes(x, -3, -2).reshape(lead + (rows * tiles, LANES))

    def far_memory(x):
        return pltpu.with_memory_space_constraint(x, pltpu.MemorySpace.HBM)

    z, slab_x, slab_y = pl.pallas_call(
        lambda *refs: images_kernel(rows, tiles, *refs),
        out_shape=(
            shape(2, dates, ext, SUB, LANES),
            shape(dates, HALF_ROWS, SUB, LANES),
            shape(dates, HALF_ROWS, SUB, LANES),
        ),
        in_specs=[hbm(), hbm(), hbm()],
        out_specs=(vmem(), vmem(), vmem()),
        scratch_shapes=[
            pltpu.VMEM((dates, rows * tiles, LANES), jnp.float32),
            pltpu.VMEM((dates, rows * tiles, LANES), jnp.float32),
            pltpu.VMEM((rows * tiles, LANES), jnp.int32),
            pltpu.SemaphoreType.DMA((3, dates)),
        ],
        compiler_params=params,
        name="images",
    )(*(far_memory(tiled(x)) for x in (amplitude, phase, validity)))
    pair_x, pair_y = swaps(blocks), swaps(blocks, odd=True)
    got_y = lax.ppermute(slab_y, "space", pair_y)
    got_x = lax.ppermute(slab_x, "space", pair_x)

    count = dates * (dates - 1) // 2
    inner = half - HALF_ROWS
    done = min(INNER_DONE, inner - 1)
    work = [
        pltpu.VMEM((2 * count, SUB, LANES), jnp.float32),
        pltpu.VMEM((3 * count + dates, SUB, LANES), jnp.float32),
        pltpu.VMEM((2 * dates, SUB, LANES), jnp.float32),
    ]

    def window_work(vectors):
        return [
            pltpu.VMEM((2 * LANES, 2 * LANES), jnp.bfloat16),
            pltpu.VMEM((dates // 2 + count, 2 * vectors * SUB, 2 * LANES), jnp.bfloat16),
            pltpu.VMEM((dates, vectors, SUB, LANES), jnp.float32),
        ]

    def cost(vectors):
        return pl.CostEstimate(
            flops=vectors * 2_000_000 * 8, bytes_accessed=1 << 20, transcendentals=0
        )

    nr, ni, part, linked_a, comp_a = pl.pallas_call(
        lambda *refs: inner_kernel(tiles, done, *refs),
        out_shape=(
            shape(count, inner - done, SUB, LANES),
            shape(count, inner - done, SUB, LANES),
            shape(2 * count + dates, HALF_ROWS, SUB, LANES),
            shape(2, dates, done, SUB, LANES),
            shape(2, done, SUB, LANES),
        ),
        in_specs=[smem(), vmem()],
        out_specs=(vmem(),) * 5,
        scratch_shapes=window_work(inner)
        + [pltpu.VMEM((count, done, SUB, LANES), jnp.float32)] * 2
        + work,
        compiler_params=params,
        cost_estimate=cost(4),
        name="inner",
    )(iterations, z)
    linked_b, comp_b, pack_x, pack_y = pl.pallas_call(
        lambda *refs: outer_kernel(tiles, *refs),
        out_shape=(
            shape(2, dates, HALF_ROWS, SUB, LANES),
            shape(2, HALF_ROWS, SUB, LANES),
            shape(HALF_ROWS, SUB, LANES),
            shape(HALF_ROWS, SUB, LANES),
        ),
        in_specs=[smem()] + [vmem()] * 4,
        out_specs=(vmem(),) * 4,
        scratch_shapes=[pltpu.VMEM((2, dates, HALF_ROWS, SUB, LANES), jnp.float32)]
        + window_work(HALF_ROWS)
        + [
            pltpu.VMEM((count, HALF_ROWS, SUB, LANES), jnp.float32),
            pltpu.VMEM((count, HALF_ROWS, SUB, LANES), jnp.float32),
        ]
        + work,
        compiler_params=params,
        cost_estimate=cost(7),
        name="outer",
    )(iterations, z, part, got_x, got_y)
    more_y = lax.ppermute(pack_y, "space", pair_y)
    more_x = lax.ppermute(pack_x, "space", pair_x)

    start = HALF_ROWS + done
    linked_c, comp_c = pl.pallas_call(
        lambda *refs: rest_kernel(start, *refs),
        out_shape=(
            shape(2, dates, half - start, SUB, LANES),
            shape(2, half - start, SUB, LANES),
        ),
        in_specs=[smem()] + [vmem()] * 4,
        out_specs=(vmem(),) * 2,
        scratch_shapes=work,
        compiler_params=params,
        cost_estimate=cost(5),
        name="rest",
    )(iterations, z, nr, ni, pack_x)
    wide = pl.pallas_call(
        extend_kernel,
        out_shape=shape(2, ext, SUB, LANES),
        in_specs=[vmem()] * 5,
        out_specs=vmem(),
        compiler_params=params,
        name="extend",
    )(comp_b, comp_a, comp_c, more_x, more_y)
    other_b = lax.ppermute(wide, "tm", strides(members))
    other_a = lax.ppermute(wide, "tm", swaps(members))
    datum, total = pl.pallas_call(
        lambda *refs: offsets_kernel(tiles, *refs),
        out_shape=(shape(2, half, SUB, LANES), shape(2, half, SUB, LANES)),
        in_specs=[vmem()] * 3,
        out_specs=(vmem(), vmem()),
        compiler_params=params,
        name="offsets",
    )(wide, other_a, other_b)
    bit = 2
    while bit < members:
        other = lax.ppermute(total, "tm", swaps(members, bit=2 * bit - 2))
        datum = jnp.where((place & bit) != 0, times(datum, other), datum)
        total = times(total, other)
        bit *= 2
    out = pl.pallas_call(
        lambda *refs: result_kernel(rows, tiles, *refs),
        out_shape=shape(2, dates, rows * tiles, LANES),
        in_specs=[smem()] + [vmem()] * 4,
        out_specs=hbm(),
        scratch_shapes=[
            pltpu.VMEM((2, dates, rows * tiles, LANES), jnp.float32),
            pltpu.VMEM((2, half, SUB, LANES), jnp.float32),
            pltpu.SemaphoreType.DMA((2, dates)),
        ],
        compiler_params=params,
        name="result",
    )(reference_date, linked_b, linked_a, linked_c, datum)
    out = out.reshape(2, dates, rows // SUB, tiles, SUB, LANES)
    return jnp.swapaxes(out, -3, -2).reshape(2, dates, rows, columns)


def solution(mesh):
    return jax.shard_map(
        linked_phases,
        mesh=mesh,
        in_specs=(
            P("tm", "space", None),
            P("tm", "space", None),
            P("space", None),
            P("tm"),
            P("tm"),
        ),
        out_specs=P(None, "tm", "space", None),
        check_vma=False,
    )
```
